8 devices in a mesh: dp: 1 (over z), tx: 2 (over y), ty: 4 (over x, core).
Axes of the slice: x: 2, y: 2, z: 1, core: 2. Of those that a mesh axis runs over, the one named last changes fastest.
Arguments:
- residual: float32 [512, 2560], P('dp', 'tx')
- norm_w: float32 [2, 2560], P(None, 'tx')
- w_in: bfloat16 [2, 2560, 2, 5120], P(None, 'tx', None, 'ty')
- conv_w: float32 [2, 5120, 4], P(None, 'ty')
- conv_b: float32 [2, 5120], P(None, 'ty')
- w_x: bfloat16 [2, 5120, 192], P(None, 'ty')
- w_dt: bfloat16 [2, 160, 5120], P(None, None, 'ty')
- dt_bias: float32 [2, 5120], P(None, 'ty')
- a_log: float32 [2, 5120, 16], P(None, 'ty')
- d_skip: float32 [2, 5120], P(None, 'ty')
- w_out: bfloat16 [2, 5120, 2560], P(None, 'ty', 'tx')
- conv_state: bfloat16 [2, 512, 5120, 3], P(None, ('dp', 'tx'), 'ty')
- ssm_state: float32 [2, 512, 5120, 16], P(None, ('dp', 'tx'), 'ty')
Outputs:
- output 1: float32 [512, 2560], P('dp', 'tx')
- output 2: bfloat16 [2, 512, 5120, 3], P(None, ('dp', 'tx'), 'ty')
- output 3: float32 [2, 512, 5120, 16], P(None, ('dp', 'tx'), 'ty')
All inputs are finite; a program needn't handle non-finite values.
Results may differ from the reference program's by a relative error of at most 0.0142533.
Values are sent between devices in bfloat16 or wider.
A program may use at most 1 GiB of HBM per device.

```python
import math
import jax
import jax.numpy as jnp
from jax import lax

BATCH_ROWS = 512
D_MODEL = 2560
D_INNER = 5120
D_STATE = 16
DT_RANK = 160
CONV_WIDTH = 4
LAYERS = 2
NORM_EPS = 1e-5
INNER_EPS = 1e-6


def setup_inputs(seed: int = 0, part: int = 0) -> dict:
    keys = jax.random.split(jax.random.key(seed), 10)
    row_keys = jax.random.split(jax.random.fold_in(jax.random.key(seed + 1), part), 3)
    col_pos = jnp.arange(D_MODEL, dtype=jnp.float32) / D_MODEL
    col_scale = jnp.exp(3.0 * col_pos - 1.5)
    residual = jax.random.normal(row_keys[0], (BATCH_ROWS, D_MODEL), jnp.float32) * col_scale
    norm_w = jax.random.uniform(keys[0], (LAYERS, D_MODEL), jnp.float32, 0.5, 1.5)
    w_in = (jax.random.normal(keys[1], (LAYERS, D_MODEL, 2, D_INNER), jnp.float32) * D_MODEL ** -0.5).astype(jnp.bfloat16)
    conv_w = jax.random.normal(keys[2], (LAYERS, D_INNER, CONV_WIDTH), jnp.float32) * CONV_WIDTH ** -0.5
    conv_b = jax.random.normal(keys[3], (LAYERS, D_INNER), jnp.float32) * 0.2
    w_x = (jax.random.normal(keys[4], (LAYERS, D_INNER, DT_RANK + 2 * D_STATE), jnp.float32) * D_INNER ** -0.5).astype(jnp.bfloat16)
    w_dt = (jax.random.normal(keys[5], (LAYERS, DT_RANK, D_INNER), jnp.float32) * DT_RANK ** -0.5).astype(jnp.bfloat16)
    dt_init = jnp.exp(jax.random.uniform(keys[6], (LAYERS, D_INNER), jnp.float32, math.log(0.005), math.log(0.1)))
    dt_bias = dt_init + jnp.log(-jnp.expm1(-dt_init))
    a_log = jnp.log(jax.random.uniform(keys[7], (LAYERS, D_INNER, D_STATE), jnp.float32, 1.0, 16.0))
    d_skip = jax.random.uniform(keys[8], (LAYERS, D_INNER), jnp.float32, 0.5, 2.0)
    w_out = (jax.random.normal(keys[9], (LAYERS, D_INNER, D_MODEL), jnp.float32) * D_INNER ** -0.5).astype(jnp.bfloat16)
    conv_state = jax.random.normal(row_keys[1], (LAYERS, BATCH_ROWS, D_INNER, CONV_WIDTH - 1), jnp.float32).astype(jnp.bfloat16)
    ssm_state = jax.random.normal(row_keys[2], (LAYERS, BATCH_ROWS, D_INNER, D_STATE), jnp.float32) * 0.5
    return {"residual": residual, "norm_w": norm_w, "w_in": w_in, "conv_w": conv_w, "conv_b": conv_b, "w_x": w_x, "w_dt": w_dt, "dt_bias": dt_bias, "a_log": a_log, "d_skip": d_skip, "w_out": w_out, "conv_state": conv_state, "ssm_state": ssm_state}


def unit_rms(vec):
    return vec * lax.rsqrt(jnp.mean(vec * vec, axis=-1, keepdims=True) + INNER_EPS)


def mixer_layer(residual, params):
    norm_w, w_in, conv_w, conv_b, w_x, w_dt, dt_bias, a_log, d_skip, w_out, conv_prev, ssm_prev = params
    variance = jnp.mean(residual * residual, axis=-1, keepdims=True)
    normed = (residual * lax.rsqrt(variance + NORM_EPS) * norm_w).astype(jnp.bfloat16)
    proj_in = jnp.dot(normed, w_in.reshape(D_MODEL, 2 * D_INNER), preferred_element_type=jnp.float32).astype(jnp.bfloat16)
    x_branch = proj_in[:, :D_INNER]
    z_branch = proj_in[:, D_INNER:]
    window = jnp.concatenate([conv_prev, x_branch[:, :, None]], axis=-1)
    conv_val = jnp.sum(window.astype(jnp.float32) * conv_w, axis=-1) + conv_b
    x_conv = jax.nn.silu(conv_val).astype(jnp.bfloat16)
    x_dbl = jnp.dot(x_conv, w_x, preferred_element_type=jnp.float32)
    dt_low = unit_rms(x_dbl[:, :DT_RANK])
    b_mat = unit_rms(x_dbl[:, DT_RANK:DT_RANK + D_STATE])
    c_mat = unit_rms(x_dbl[:, DT_RANK + D_STATE:])
    delta = jax.nn.softplus(jnp.dot(dt_low.astype(jnp.bfloat16), w_dt, preferred_element_type=jnp.float32) + dt_bias)
    x_float = x_conv.astype(jnp.float32)
    decay = jnp.exp(delta[:, :, None] * -jnp.exp(a_log))
    ssm_new = decay * ssm_prev + (delta * x_float)[:, :, None] * b_mat[:, None, :]
    state_val = jnp.sum(ssm_new * c_mat[:, None, :], axis=-1)
    gated = ((state_val + d_skip * x_float) * jax.nn.silu(z_branch.astype(jnp.float32))).astype(jnp.bfloat16)
    out_proj = jnp.dot(gated, w_out, preferred_element_type=jnp.float32)
    return residual + out_proj, (window[:, :, 1:], ssm_new)


def reference(residual, norm_w, w_in, conv_w, conv_b, w_x, w_dt, dt_bias, a_log, d_skip, w_out, conv_state, ssm_state):
    layer_params = (norm_w, w_in, conv_w, conv_b, w_x, w_dt, dt_bias, a_log, d_skip, w_out, conv_state, ssm_state)
    residual_out, caches = lax.scan(mixer_layer, residual, layer_params)
    return residual_out, caches[0], caches[1]
```

```python
import functools
import jax
import jax.numpy as jnp
from jax import lax
from jax.experimental import pallas as pl
from jax.experimental.pallas import tpu as pltpu
from jax.sharding import PartitionSpec as P

NORM_EPS = 1e-5
INNER_EPS = 1e-6
LOG2E = 1.4426950408889634
N_CHUNK = 4
BF = jnp.bfloat16
F32 = jnp.float32
MESH = pl.DeviceIdType.MESH


def step_kernel(dims, res_hbm, norm_w, w_in_hbm, conv_w, conv_b, w_x, w_dt, dt_bias, a_log, d_skip, w_out_hbm, conv_hbm, ssm_hbm,
                r_ref, conv_out, ssm_out,
                w_in, w_out, a_neg, ssm_buf, conv_buf, h_buf, u_own, z_buf, x_buf, dt_buf, dtx_buf, y_buf, b_bc, c_bc, o_buf,
                st_send, st_recv, u_send, u_recv, p_own, p_send, p_recv, g_all, cr_send, cr_recv, xs_send, xs_recv, ag_send, ag_recv,
                in_sem, ssm_in_sem, ssm_out_sem, conv_in_sem, conv_out_sem,
                st_s, st_r, u_s, u_r, p_s, p_r, g_s, g_r, cr_s, cr_r, xs_s, xs_r, ag_s, ag_r):
    n_layer, rows, d_loc, e_loc, n_state, n_rank, d_model = dims
    half = rows // 2
    n_chunk = N_CHUNK
    blk = half // n_chunk
    total = n_layer * n_chunk
    tx = lax.axis_index("tx")
    ty = lax.axis_index("ty")
    core = lax.rem(ty, 2)
    chip = lax.div(ty, 2)
    y_peer = {"tx": 1 - tx, "ty": ty}
    core_peer = {"tx": tx, "ty": chip * 2 + (1 - core)}
    x_peer = {"tx": tx, "ty": (1 - chip) * 2 + core}
    d_peer = {"tx": tx, "ty": (1 - chip) * 2 + (1 - core)}

    def layer_of(i):
        return lax.div(i, n_chunk)

    def chunk_of(i):
        return lax.rem(i, n_chunk)

    def part_rows(i, part):
        side = jnp.where(part == 0, tx, 1 - tx)
        return pl.multiple_of(side * half + chunk_of(i) * blk, blk)

    def remote(src, dst, s_sem, r_sem, dev):
        return pltpu.make_async_remote_copy(src_ref=src, dst_ref=dst, send_sem=s_sem, recv_sem=r_sem, device_id=dev, device_id_type=MESH)

    def st_copy(i):
        return remote(st_send.at[i], st_recv.at[i], st_s.at[i], st_r.at[i], y_peer)

    def u_copy(i, k):
        s = lax.rem(i, 2)
        return remote(u_send.at[s, k], u_recv.at[i, k], u_s.at[s, k], u_r.at[i, k], y_peer)

    def p_copy(i, q):
        s = lax.rem(i, 2)
        dev = (core_peer, x_peer, d_peer)[q]
        return remote(p_send.at[s], p_recv.at[i, q], p_s.at[s, q], p_r.at[i, q], dev)

    def g_copy(i):
        return remote(g_all.at[i, pl.ds(0, blk)], g_all.at[i, pl.ds(blk, blk)], g_s.at[i], g_r.at[i], y_peer)

    def cr_copy(i):
        return remote(cr_send.at[i], cr_recv.at[i], cr_s.at[i], cr_r.at[i], core_peer)

    def xs_copy(i):
        return remote(xs_send.at[i], xs_recv.at[i], xs_s.at[i], xs_r.at[i], x_peer)

    def ag_copy(i):
        return remote(ag_send.at[i], ag_recv.at[i], ag_s.at[i], ag_r.at[i], core_peer)

    def cache_rows(i):
        return pl.ds(pl.multiple_of(chunk_of(i) * blk, blk), blk)

    def ssm_load(i):
        s = lax.rem(i, 2)
        return pltpu.make_async_copy(ssm_hbm.at[layer_of(i), cache_rows(i)], ssm_buf.at[s], ssm_in_sem.at[s])

    def ssm_store(i):
        s = lax.rem(i, 2)
        return pltpu.make_async_copy(ssm_buf.at[s], ssm_out.at[layer_of(i), cache_rows(i)], ssm_out_sem.at[s])

    def conv_load(i):
        s = lax.rem(i, 2)
        return pltpu.make_async_copy(conv_hbm.at[layer_of(i), :, cache_rows(i)], conv_buf.at[s, pl.ds(0, 3)], conv_in_sem.at[s])

    def conv_store(i):
        s = lax.rem(i, 2)
        return pltpu.make_async_copy(conv_buf.at[s, pl.ds(1, 3)], conv_out.at[layer_of(i), :, cache_rows(i)], conv_out_sem.at[s])

    res_load = pltpu.make_async_copy(res_hbm, r_ref, in_sem.at[0])
    w_in_load = [pltpu.make_async_copy(w_in_hbm.at[l], w_in.at[l], in_sem.at[1 + l]) for l in range(n_layer)]
    w_out_load = pltpu.make_async_copy(w_out_hbm, w_out, in_sem.at[1 + n_layer])

    res_load.start()
    w_in_load[0].start()

    barrier = pltpu.get_barrier_semaphore()
    for dev in (y_peer, core_peer, x_peer, d_peer):
        pl.semaphore_signal(barrier, inc=1, device_id=dev, device_id_type=MESH)
    pl.semaphore_wait(barrier, 4)

    def eye():
        n = 2 * blk
        return lax.broadcasted_iota(jnp.int32, (n, n), 0) == lax.broadcasted_iota(jnp.int32, (n, n), 1)

    def phase_a(i):
        sums = []
        for part in range(2):
            val = r_ref[pl.ds(part_rows(i, part), blk), :]
            sums.append(jnp.sum(val * val, axis=1, keepdims=True))
        col = jnp.concatenate(sums, axis=0)
        row = jnp.sum(jnp.where(eye(), col, 0.0), axis=0, keepdims=True)
        st_send[i] = jnp.broadcast_to(row, (8, 2 * blk))
        st_copy(i).start()

    def phase_b(i):
        l = layer_of(i)
        s = lax.rem(i, 2)
        st_copy(i).wait_recv()
        sq = st_send[i] + pltpu.roll(st_recv[i], blk, 1)
        inv = lax.rsqrt(sq / d_model + NORM_EPS)
        col = jnp.sum(jnp.where(eye(), jnp.broadcast_to(inv[0:1], (2 * blk, 2 * blk)), 0.0), axis=1, keepdims=True)
        nw = norm_w[l]
        for part in range(2):
            base = part_rows(i, part)
            for q in range(blk // 16):
                lo = part * blk + q * 16
                val = r_ref[pl.ds(base + q * 16, 16), :]
                h_buf[lo:lo + 16, :] = (val * col[lo:lo + 16] * nw).astype(BF)

        @pl.when(i >= 2)
        def _():
            for k in range(2):
                u_copy(i - 2, k).wait_send()

        for k in range(2):
            def tile(t, carry):
                cols = pl.ds(pl.multiple_of(t * 256, 256), 256)
                u = jnp.dot(h_buf[...], w_in[l, k, :, cols], preferred_element_type=F32)
                u_own[s, k, :, cols] = u[:blk]
                u_send[s, k, :, cols] = u[blk:].astype(BF)
                return carry
            lax.fori_loop(0, e_loc // 256, tile, 0)
            u_copy(i, k).start()

    def phase_c(i):
        l = layer_of(i)
        s = lax.rem(i, 2)

        @pl.when(i >= 1)
        def _():
            conv_store(i - 1).wait()

            @pl.when(i + 1 < total)
            def _():
                conv_load(i + 1).start()

        conv_load(i).wait()
        u_copy(i, 0).wait_recv()
        cb = conv_b[l]

        def rows16(q, carry):
            rws = pl.ds(pl.multiple_of(q * 16, 16), 16)
            xi = (u_own[s, 0, rws, :] + u_recv[i, 0, rws, :].astype(F32)).astype(BF)
            conv_buf[s, 3, rws, :] = xi
            acc = conv_buf[s, 0, rws, :].astype(F32) * conv_w[l, 0:1, :]
            acc = acc + conv_buf[s, 1, rws, :].astype(F32) * conv_w[l, 1:2, :]
            acc = acc + conv_buf[s, 2, rws, :].astype(F32) * conv_w[l, 2:3, :]
            acc = acc + xi.astype(F32) * conv_w[l, 3:4, :]
            acc = acc + cb
            x_buf[rws, :] = (acc * jax.nn.sigmoid(acc)).astype(BF)
            return carry
        lax.fori_loop(0, blk // 16, rows16, 0)
        conv_store(i).start()

        @pl.when(i >= 2)
        def _():
            for q in range(3):
                p_copy(i - 2, q).wait_send()

        pt = lax.dot_general(w_x[l], x_buf[...], (((1,), (1,)), ((), ())), preferred_element_type=F32)
        pt = jnp.concatenate([pt, pt], axis=1)
        p_own[...] = pt
        p_send[s] = pt.astype(BF)
        for q in range(3):
            p_copy(i, q).start()

        u_copy(i, 1).wait_recv()

        def zrows(q, carry):
            rws = pl.ds(pl.multiple_of(q * 16, 16), 16)
            z = (u_own[s, 1, rws, :] + u_recv[i, 1, rws, :].astype(F32)).astype(BF).astype(F32)
            z_buf[rws, :] = z * jax.nn.sigmoid(z)
            return carry
        lax.fori_loop(0, blk // 16, zrows, 0)

    def phase_d(i):
        l = layer_of(i)
        s = lax.rem(i, 2)
        for q in range(3):
            p_copy(i, q).wait_recv()
        pt = p_own[...]
        for q in range(3):
            pt = pt + p_recv[i, q].astype(F32)

        def unit(v):
            return v * lax.rsqrt(jnp.mean(v * v, axis=0, keepdims=True) + INNER_EPS)
        low = unit(pt[:n_rank]).astype(BF)
        bt = unit(pt[n_rank:n_rank + n_state])
        ct = unit(pt[n_rank + n_state:])
        for b in range(blk):
            b_bc[b] = jnp.broadcast_to(bt[:, b:b + 1], (n_state, 128))
            c_bc[b] = jnp.broadcast_to(ct[:, b:b + 1], (n_state, 128))

        def dt_tile(t, carry):
            cols = pl.ds(pl.multiple_of(t * 256, 256), 256)
            v = lax.dot_general(low, w_dt[l, :, cols], (((0,), (0,)), ((), ())), preferred_element_type=F32)[:blk]
            v = v + dt_bias[l, :, cols]
            dt = jnp.maximum(v, 0.0) + jnp.log1p(jnp.exp(-jnp.abs(v)))
            dt_buf[:, cols] = dt
            dtx_buf[:, cols] = dt * x_buf[:, cols].astype(F32)
            return carry
        lax.fori_loop(0, e_loc // 256, dt_tile, 0)
        ssm_load(i).wait()

        def group(g, carry):
            rws = pl.ds(pl.multiple_of(g * 8, 8), 8)
            for j in range(e_loc // 128):
                cols = slice(j * 128, (j + 1) * 128)
                dt8 = dt_buf[rws, cols]
                dx8 = dtx_buf[rws, cols]
                a = a_neg[l, :, cols]
                decay = jnp.exp2(dt8[:, None, :] * a[None])
                new = decay * ssm_buf[s, rws, :, cols] + dx8[:, None, :] * b_bc[rws]
                ssm_buf[s, rws, :, cols] = new
                y_buf[rws, cols] = jnp.sum(new * c_bc[rws], axis=1)
            return carry
        lax.fori_loop(0, blk // 8, group, 0)
        ssm_store(i).start()
        ds = d_skip[l]

        def gate(q, carry):
            rws = pl.ds(pl.multiple_of(q * 16, 16), 16)
            g_all[i, rws, :] = ((y_buf[rws, :] + ds * x_buf[rws, :].astype(F32)) * z_buf[rws, :]).astype(BF)
            return carry
        lax.fori_loop(0, blk // 16, gate, 0)
        g_copy(i).start()

    def phase_e(i):
        l = layer_of(i)
        g_copy(i).wait_recv()

        def tile(t, carry):
            cols = pl.ds(pl.multiple_of(t * 256, 256), 256)
            o_buf[:, cols] = jnp.dot(g_all[i], w_out[l, :, cols], preferred_element_type=F32)
            return carry
        lax.fori_loop(0, d_loc // 256, tile, 0)
        other = pl.multiple_of((1 - core) * blk, blk)
        cr_send[i] = o_buf[pl.ds(other, blk), :].astype(BF)
        cr_copy(i).start()

    def phase_f(i):
        cr_copy(i).wait_recv()
        mine = pl.multiple_of(core * blk, blk)
        xs_send[i] = (o_buf[pl.ds(mine, blk), :] + cr_recv[i].astype(F32)).astype(BF)
        xs_copy(i).start()

    def phase_g(i):
        xs_copy(i).wait_recv()
        tot = (xs_send[i].astype(F32) + xs_recv[i].astype(F32)).astype(BF)
        ag_send[i] = tot
        ag_copy(i).start()
        rws = pl.ds(part_rows(i, core), blk)
        r_ref[rws, :] = r_ref[rws, :] + tot.astype(F32)

    def phase_h(i):
        ag_copy(i).wait_recv()
        rws = pl.ds(part_rows(i, 1 - core), blk)
        r_ref[rws, :] = r_ref[rws, :] + ag_recv[i].astype(F32)

        @pl.when(i + n_chunk < total)
        def _():
            phase_a(i + n_chunk)

    for l in range(n_layer):
        a_neg[l] = jnp.exp(a_log[l]) * (-LOG2E)
    res_load.wait()

    def first_a(i, carry):
        phase_a(i)
        return carry
    lax.fori_loop(0, n_chunk, first_a, 0)
    w_in_load[0].wait()

    def run(phase, i, extra=None):
        ok = (i >= 0) & (i < total)

        @pl.when(ok)
        def _():
            phase(i)

    def step(s, carry):
        @pl.when(s == n_chunk)
        def _():
            w_in_load[1].wait()
        run(phase_b, s)

        @pl.when(s == 0)
        def _():
            conv_load(0).start()
            conv_load(1).start()
            ssm_load(0).start()
            ssm_load(1).start()
            w_out_load.start()
            w_in_load[1].start()

        @pl.when((s >= 2) & (s - 2 < total))
        def _():
            ssm_store(s - 2 - 0).wait()

            @pl.when(s < total)
            def _():
                ssm_load(s).start()
        run(phase_c, s - 1)

        @pl.when(s == 2)
        def _():
            w_out_load.wait()
        run(phase_e, s - 2)
        run(phase_g, s - 3)
        run(phase_f, s - 2)
        run(phase_h, s - 3)
        run(phase_d, s - 1)
        return carry
    lax.fori_loop(0, total + 3, step, 0)

    conv_store(total - 1).wait()
    for i in range(total - 2, total):
        for k in range(2):
            u_copy(i, k).wait_send()
        for q in range(3):
            p_copy(i, q).wait_send()

    def drain(i, carry):
        st_copy(i).wait_send()
        g_copy(i).wait_send()
        cr_copy(i).wait_send()
        xs_copy(i).wait_send()
        ag_copy(i).wait_send()
        return carry
    lax.fori_loop(0, total, drain, 0)


def solution(mesh):
    def local_step(residual, norm_w, w_in, conv_w, conv_b, w_x, w_dt, dt_bias, a_log, d_skip, w_out, conv_state, ssm_state):
        n_layer = norm_w.shape[0]
        rows, d_loc = residual.shape
        e_loc = w_x.shape[1]
        n_state = a_log.shape[-1]
        n_rank = w_dt.shape[1]
        n_proj = w_x.shape[2]
        d_model = d_loc * mesh.shape["tx"]
        total = n_layer * N_CHUNK
        blk = rows // 2 // N_CHUNK
        dims = (n_layer, rows, d_loc, e_loc, n_state, n_rank, d_model)
        w_in_t = jnp.transpose(w_in, (0, 2, 1, 3))
        conv_t = jnp.transpose(conv_state, (0, 3, 1, 2))
        ssm_t = jnp.transpose(ssm_state, (0, 1, 3, 2))
        args = (residual, norm_w[:, None, :], w_in_t, jnp.transpose(conv_w, (0, 2, 1)), conv_b[:, None, :], jnp.transpose(w_x, (0, 2, 1)), w_dt, dt_bias[:, None, :], jnp.transpose(a_log, (0, 2, 1)), d_skip[:, None, :], w_out, conv_t, ssm_t)
        hbm = pl.BlockSpec(memory_space=pl.ANY)
        vmem = pl.BlockSpec(memory_space=pltpu.VMEM)
        in_specs = [hbm, vmem, hbm, vmem, vmem, vmem, vmem, vmem, vmem, vmem, hbm, hbm, hbm]
        dma = pltpu.SemaphoreType.DMA
        scratch = [
            pltpu.VMEM((n_layer, 2, d_loc, e_loc), BF),
            pltpu.VMEM((n_layer, e_loc, d_loc), BF),
            pltpu.VMEM((n_layer, n_state, e_loc), F32),
            pltpu.VMEM((2, blk, n_state, e_loc), F32),
            pltpu.VMEM((2, 4, blk, e_loc), BF),
            pltpu.VMEM((2 * blk, d_loc), BF),
            pltpu.VMEM((2, 2, blk, e_loc), F32),
            pltpu.VMEM((blk, e_loc), F32),
            pltpu.VMEM((blk, e_loc), BF),
            pltpu.VMEM((blk, e_loc), F32),
            pltpu.VMEM((blk, e_loc), F32),
            pltpu.VMEM((blk, e_loc), F32),
            pltpu.VMEM((blk, n_state, 128), F32),
            pltpu.VMEM((blk, n_state, 128), F32),
            pltpu.VMEM((2 * blk, d_loc), F32),
            pltpu.VMEM((total, 8, 2 * blk), F32),
            pltpu.VMEM((total, 8, 2 * blk), F32),
            pltpu.VMEM((2, 2, blk, e_loc), BF),
            pltpu.VMEM((total, 2, blk, e_loc), BF),
            pltpu.VMEM((n_proj, 2 * blk), F32),
            pltpu.VMEM((2, n_proj, 2 * blk), BF),
            pltpu.VMEM((total, 3, n_proj, 2 * blk), BF),
            pltpu.VMEM((total, 2 * blk, e_loc), BF),
        ] + [pltpu.VMEM((total, blk, d_loc), BF)] * 6 + [
            dma((2 + n_layer,)), dma((2,)), dma((2,)), dma((2,)), dma((2,)),
            dma((total,)), dma((total,)), dma((2, 2)), dma((total, 2)), dma((2, 3)), dma((total, 3)),
            dma((total,)), dma((total,)), dma((total,)), dma((total,)), dma((total,)), dma((total,)), dma((total,)), dma((total,)),
        ]
        out = pl.pallas_call(
            functools.partial(step_kernel, dims),
            out_shape=(jax.ShapeDtypeStruct((rows, d_loc), F32), jax.ShapeDtypeStruct(conv_t.shape, BF), jax.ShapeDtypeStruct(ssm_t.shape, F32)),
            in_specs=in_specs,
            out_specs=(vmem, hbm, hbm),
            scratch_shapes=scratch,
            compiler_params=pltpu.CompilerParams(collective_id=0, has_side_effects=True, vmem_limit_bytes=67043328),
            name="mamba_step",
        )(*args)
        return out[0], jnp.transpose(out[1], (0, 2, 3, 1)), jnp.transpose(out[2], (0, 1, 3, 2))

    cache_spec = P(None, ("dp", "tx"), "ty", None)
    in_specs = (P("dp", "tx"), P(None, "tx"), P(None, "tx", None, "ty"), P(None, "ty", None), P(None, "ty"), P(None, "ty", None), P(None, None, "ty"), P(None, "ty"), P(None, "ty", None), P(None, "ty"), P(None, "ty", "tx"), cache_spec, cache_spec)
    out_specs = (P("dp", "tx"), cache_spec, cache_spec)
    return jax.shard_map(local_step, mesh=mesh, in_specs=in_specs, out_specs=out_specs, check_vma=False)
```

```python
import functools
import jax
import jax.numpy as jnp
from jax import lax
from jax.experimental import pallas as pl
from jax.experimental.pallas import tpu as pltpu
from jax.sharding import PartitionSpec as P


NORM_EPS = 1e-5
INNER_EPS = 1e-6
LOG2E = 1.4426950408889634
N_CHUNK = 4
BF = jnp.bfloat16
F32 = jnp.float32
MESH = pl.DeviceIdType.MESH


def step_kernel(dims, res_hbm, norm_w_in, w_in_hbm, conv_w, conv_b_in, w_x, w_dt, dt_bias_in, a_log, d_skip_in, w_out_hbm, conv_hbm, ssm_hbm,
                r_ref, bt_out, g_out, dt_out, x_out, xi_out,
                norm_w, conv_b, dt_bias, d_skip, w_in, w_out, a_neg, ssm_buf, conv_buf, h_buf, u_own, z_buf, x_buf, low_buf, dt_buf, dtx_buf, b_bc, c_bc, o_buf,
                st_send, st_recv, u_send, u_recv, p_own, p_send, p_recv, g_all, cr_send, cr_recv, xs_send, xs_recv, ag_send, ag_recv,
                in_sem, ssm_in_sem, conv_in_sem, dt_sem, x_sem, xi_sem, go_sem,
                st_s, st_r, u_s, u_r, p_s, p_r, g_s, g_r, cr_s, cr_r, xs_s, xs_r, ag_s, ag_r):
    n_layer, rows, d_loc, e_loc, n_state, n_rank, d_model = dims
    half = rows // 2
    n_chunk = N_CHUNK
    blk = half // n_chunk
    total = n_layer * n_chunk
    tx = lax.axis_index("tx")
    ty = lax.axis_index("ty")
    core = lax.rem(ty, 2)
    chip = lax.div(ty, 2)
    y_peer = {"tx": 1 - tx, "ty": ty}
    core_peer = {"tx": tx, "ty": chip * 2 + (1 - core)}
    x_peer = {"tx": tx, "ty": (1 - chip) * 2 + core}
    d_peer = {"tx": tx, "ty": (1 - chip) * 2 + (1 - core)}

    def layer_of(i):
        return lax.div(i, n_chunk)

    def chunk_of(i):
        return lax.rem(i, n_chunk)

    def part_rows(i, part):
        side = jnp.where(part == 0, tx, 1 - tx)
        return pl.multiple_of(side * half + chunk_of(i) * blk, blk)

    def remote(src, dst, s_sem, r_sem, dev):
        return pltpu.make_async_remote_copy(src_ref=src, dst_ref=dst, send_sem=s_sem, recv_sem=r_sem, device_id=dev, device_id_type=MESH)

    def st_copy(i):
        return remote(st_send.at[i], st_recv.at[i], st_s.at[i], st_r.at[i], y_peer)

    def u_copy(i, k):
        s = lax.rem(i, 2)
        return remote(u_send.at[s, k], u_recv.at[i, k], u_s.at[s, k], u_r.at[i, k], y_peer)

    def p_copy(i, q):
        s = lax.rem(i, 2)
        dev = (core_peer, x_peer, d_peer)[q]
        return remote(p_send.at[s], p_recv.at[i, q], p_s.at[s, q], p_r.at[i, q], dev)

    def g_copy(i):
        return remote(g_all.at[i, pl.ds(0, blk)], g_all.at[i, pl.ds(blk, blk)], g_s.at[i], g_r.at[i], y_peer)

    def cr_copy(i):
        return remote(cr_send.at[i], cr_recv.at[i], cr_s.at[i], cr_r.at[i], core_peer)

    def xs_copy(i):
        return remote(xs_send.at[i], xs_recv.at[i], xs_s.at[i], xs_r.at[i], x_peer)

    def ag_copy(i):
        return remote(ag_send.at[i], ag_recv.at[i], ag_s.at[i], ag_r.at[i], core_peer)

    def cache_rows(i):
        return pl.ds(pl.multiple_of(chunk_of(i) * blk, blk), blk)

    def ssm_load(i):
        s = lax.rem(i, 2)
        return pltpu.make_async_copy(ssm_hbm.at[layer_of(i), cache_rows(i)], ssm_buf.at[s], ssm_in_sem.at[s])

    def conv_load(i):
        s = lax.rem(i, 2)
        return pltpu.make_async_copy(conv_hbm.at[layer_of(i), :, cache_rows(i)], conv_buf.at[s, pl.ds(0, 3)], conv_in_sem.at[s])

    def dt_store(i):
        return pltpu.make_async_copy(dt_buf, dt_out.at[layer_of(i), cache_rows(i)], dt_sem)

    def x_store(i):
        return pltpu.make_async_copy(x_buf, x_out.at[layer_of(i), cache_rows(i)], x_sem)

    def xi_store(i):
        s = lax.rem(i, 2)
        return pltpu.make_async_copy(conv_buf.at[s, 3], xi_out.at[layer_of(i), cache_rows(i)], xi_sem.at[s])

    def g_store(i):
        return pltpu.make_async_copy(g_all.at[i, pl.ds(0, blk)], g_out.at[cache_rows(i)], go_sem.at[chunk_of(i)])

    res_load = pltpu.make_async_copy(res_hbm, r_ref, in_sem.at[0])
    w_in_load = [pltpu.make_async_copy(w_in_hbm.at[l], w_in.at[l], in_sem.at[1 + l]) for l in range(n_layer)]
    w_out_load = pltpu.make_async_copy(w_out_hbm, w_out, in_sem.at[1 + n_layer])

    res_load.start()
    w_in_load[0].start()

    barrier = pltpu.get_barrier_semaphore()
    for dev in (y_peer, core_peer, x_peer, d_peer):
        pl.semaphore_signal(barrier, inc=1, device_id=dev, device_id_type=MESH)
    pl.semaphore_wait(barrier, 4)

    def eye():
        n = 2 * blk
        return lax.broadcasted_iota(jnp.int32, (n, n), 0) == lax.broadcasted_iota(jnp.int32, (n, n), 1)

    def phase_a(i):
        sums = []
        for part in range(2):
            val = r_ref[pl.ds(part_rows(i, part), blk), :]
            sums.append(jnp.sum(val * val, axis=1, keepdims=True))
        col = jnp.concatenate(sums, axis=0)
        row = jnp.sum(jnp.where(eye(), col, 0.0), axis=0, keepdims=True)
        st_send[i] = jnp.broadcast_to(row, (8, 2 * blk))
        st_copy(i).start()

    def phase_b(i):
        l = layer_of(i)
        s = lax.rem(i, 2)
        st_copy(i).wait_recv()
        sq = st_send[i] + pltpu.roll(st_recv[i], blk, 1)
        inv = lax.rsqrt(sq / d_model + NORM_EPS)
        col = jnp.sum(jnp.where(eye(), jnp.broadcast_to(inv[0:1], (2 * blk, 2 * blk)), 0.0), axis=1, keepdims=True)
        nw = norm_w[l]
        for part in range(2):
            base = part_rows(i, part)
            for q in range(blk // 16):
                lo = part * blk + q * 16
                val = r_ref[pl.ds(base + q * 16, 16), :]
                h_buf[lo:lo + 16, :] = (val * col[lo:lo + 16] * nw).astype(BF)

        @pl.when(i >= 2)
        def _():
            for k in range(2):
                u_copy(i - 2, k).wait_send()

        for k in range(2):
            def tile(t, carry):
                cols = pl.ds(pl.multiple_of(t * 256, 256), 256)
                u = jnp.dot(h_buf[...], w_in[l, k, :, cols], preferred_element_type=F32)
                u_own[s, k, :, cols] = u[:blk]
                u_send[s, k, :, cols] = u[blk:].astype(BF)
                return carry

            lax.fori_loop(0, e_loc // 256, tile, 0)
            u_copy(i, k).start()

    def phase_c(i):
        l = layer_of(i)
        s = lax.rem(i, 2)

        @pl.when(i >= 1)
        def _():
            xi_store(i - 1).wait()
            x_store(i - 1).wait()

            @pl.when(i + 1 < total)
            def _():
                conv_load(i + 1).start()

        conv_load(i).wait()
        u_copy(i, 0).wait_recv()
        cb = conv_b[l]

        def rows16(q, carry):
            rws = pl.ds(pl.multiple_of(q * 16, 16), 16)
            xi = (u_own[s, 0, rws, :] + u_recv[i, 0, rws, :].astype(F32)).astype(BF)
            conv_buf[s, 3, rws, :] = xi
            acc = conv_buf[s, 0, rws, :].astype(F32) * conv_w[l, 0:1, :]
            acc = acc + conv_buf[s, 1, rws, :].astype(F32) * conv_w[l, 1:2, :]
            acc = acc + conv_buf[s, 2, rws, :].astype(F32) * conv_w[l, 2:3, :]
            acc = acc + xi.astype(F32) * conv_w[l, 3:4, :]
            acc = acc + cb
            x_buf[rws, :] = (acc * jax.nn.sigmoid(acc)).astype(BF)
            return carry

        lax.fori_loop(0, blk // 16, rows16, 0)
        xi_store(i).start()
        x_store(i).start()

        @pl.when(i >= 2)
        def _():
            for q in range(3):
                p_copy(i - 2, q).wait_send()

        pt = lax.dot_general(w_x[l], x_buf[...], (((1,), (1,)), ((), ())), preferred_element_type=F32)
        pt = jnp.concatenate([pt, pt], axis=1)
        p_own[...] = pt
        p_send[s] = pt.astype(BF)
        for q in range(3):
            p_copy(i, q).start()

        u_copy(i, 1).wait_recv()

        def zrows(q, carry):
            rws = pl.ds(pl.multiple_of(q * 16, 16), 16)
            z = (u_own[s, 1, rws, :] + u_recv[i, 1, rws, :].astype(F32)).astype(BF).astype(F32)
            z_buf[rws, :] = z * jax.nn.sigmoid(z)
            return carry

        lax.fori_loop(0, blk // 16, zrows, 0)

    def phase_d(i):
        l = layer_of(i)
        s = lax.rem(i, 2)
        for q in range(3):
            p_copy(i, q).wait_recv()
        pt = p_own[...]
        for q in range(3):
            pt = pt + p_recv[i, q].astype(F32)

        def unit(v):
            return v * lax.rsqrt(jnp.mean(v * v, axis=0, keepdims=True) + INNER_EPS)

        low_buf[...] = jnp.transpose(unit(pt[:n_rank]))[:blk].astype(BF)
        bt = unit(pt[n_rank:n_rank + n_state])
        ct = unit(pt[n_rank + n_state:])
        bt_out[i, 0] = bt
        bt_out[i, 1] = pltpu.roll(bt, 2 * blk - blk // 2, 1)
        for b in range(blk):
            b_bc[b] = jnp.broadcast_to(bt[:, b:b + 1], (n_state, 128))
            c_bc[b] = jnp.broadcast_to(ct[:, b:b + 1], (n_state, 128))

        @pl.when(i >= 1)
        def _():
            dt_store(i - 1).wait()

        def dt_tile(t, carry):
            cols = pl.ds(pl.multiple_of(t * 256, 256), 256)
            v = jnp.dot(low_buf[...], w_dt[l, :, cols], preferred_element_type=F32)
            v = v + dt_bias[l, :, cols]
            dt = jnp.maximum(v, 0.0) + jnp.log1p(jnp.exp(-jnp.abs(v)))
            dt_buf[:, cols] = dt
            dtx_buf[:, cols] = dt * x_buf[:, cols].astype(F32)
            return carry

        lax.fori_loop(0, e_loc // 256, dt_tile, 0)
        dt_store(i).start()
        ssm_load(i).wait()

        def group(g, carry):
            for j in range(e_loc // 128):
                cols = slice(j * 128, (j + 1) * 128)
                a = a_neg[l, :, cols]
                out = []
                for p in range(2):
                    rws = pl.ds(pl.multiple_of(g * 16 + p * 8, 8), 8)
                    decay = jnp.exp2(dt_buf[rws, cols][:, None, :] * a[None])
                    new = decay * ssm_buf[s, rws, :, cols] + dtx_buf[rws, cols][:, None, :] * b_bc[rws]
                    out.append(jnp.sum(new * c_bc[rws], axis=1))
                rws = pl.ds(pl.multiple_of(g * 16, 16), 16)
                y = jnp.concatenate(out, axis=0) + d_skip[l, :, cols] * x_buf[rws, cols].astype(F32)
                g_all[i, rws, cols] = (y * z_buf[rws, cols]).astype(BF)
            return carry

        lax.fori_loop(0, blk // 16, group, 0)

        @pl.when(i < total - n_chunk)
        def _():
            g_copy(i).start()

        @pl.when(i >= total - n_chunk)
        def _():
            g_store(i).start()

    def phase_e(i):
        l = layer_of(i)
        g_copy(i).wait_recv()

        def tile(t, carry):
            cols = pl.ds(pl.multiple_of(t * 256, 256), 256)
            o_buf[:, cols] = jnp.dot(g_all[i], w_out[l, :, cols], preferred_element_type=F32)
            return carry

        lax.fori_loop(0, d_loc // 256, tile, 0)
        other = pl.multiple_of((1 - core) * blk, blk)
        cr_send[i] = o_buf[pl.ds(other, blk), :].astype(BF)
        cr_copy(i).start()

    def phase_f(i):
        cr_copy(i).wait_recv()
        mine = pl.multiple_of(core * blk, blk)
        xs_send[i] = (o_buf[pl.ds(mine, blk), :] + cr_recv[i].astype(F32)).astype(BF)
        xs_copy(i).start()

    def phase_g(i):
        xs_copy(i).wait_recv()
        tot = (xs_send[i].astype(F32) + xs_recv[i].astype(F32)).astype(BF)
        ag_send[i] = tot
        ag_copy(i).start()
        rws = pl.ds(part_rows(i, core), blk)
        r_ref[rws, :] = r_ref[rws, :] + tot.astype(F32)

    def phase_h(i):
        ag_copy(i).wait_recv()
        rws = pl.ds(part_rows(i, 1 - core), blk)
        r_ref[rws, :] = r_ref[rws, :] + ag_recv[i].astype(F32)

        @pl.when(i + n_chunk < total)
        def _():
            phase_a(i + n_chunk)

    for l in range(n_layer):
        for vec, src in ((norm_w, norm_w_in), (conv_b, conv_b_in), (dt_bias, dt_bias_in), (d_skip, d_skip_in)):
            vec[l] = src[l:l + 1, :]
        a_neg[l] = jnp.exp(a_log[l]) * (-LOG2E)
    res_load.wait()

    def first_a(i, carry):
        phase_a(i)
        return carry

    lax.fori_loop(0, n_chunk, first_a, 0)
    w_in_load[0].wait()

    def run(phase, i, stop=total):
        ok = (i >= 0) & (i < stop)

        @pl.when(ok)
        def _():
            phase(i)

    def step(s, carry):
        @pl.when(s == n_chunk)
        def _():
            w_in_load[1].wait()

        run(phase_b, s)

        @pl.when(s == 0)
        def _():
            conv_load(0).start()
            conv_load(1).start()
            ssm_load(0).start()
            ssm_load(1).start()
            w_out_load.start()
            w_in_load[1].start()

        @pl.when((s >= 2) & (s < total))
        def _():
            ssm_load(s).start()

        run(phase_c, s - 1)

        @pl.when(s == 2)
        def _():
            w_out_load.wait()

        run(phase_e, s - 2, total - n_chunk)
        run(phase_g, s - 3, total - n_chunk)
        run(phase_f, s - 2, total - n_chunk)
        run(phase_h, s - 3, total - n_chunk)
        run(phase_d, s - 1)
        return carry

    lax.fori_loop(0, total + 1, step, 0)

    xi_store(total - 1).wait()
    x_store(total - 1).wait()
    dt_store(total - 1).wait()
    for i in range(total - 2, total):
        for k in range(2):
            u_copy(i, k).wait_send()
        for q in range(3):
            p_copy(i, q).wait_send()

    def drain(i, carry):
        st_copy(i).wait_send()
        st_copy(i + n_chunk).wait_send()
        g_copy(i).wait_send()
        cr_copy(i).wait_send()
        xs_copy(i).wait_send()
        ag_copy(i).wait_send()
        g_store(i + total - n_chunk).wait()
        return carry

    lax.fori_loop(0, n_chunk, drain, 0)


def state_kernel(n_carry, blk, ssm_in, dt, x, bt, a_log, conv_in, xi, *refs):
    ssm_out, conv_out, a_neg, b_bc = refs[n_carry:]
    n_state, e_loc = a_log.shape[1:]

    @pl.when(pl.program_id(0) == 0)
    def _():
        a_neg[...] = jnp.exp(a_log[0]) * (-LOG2E)

    for b in range(blk):
        b_bc[b] = jnp.broadcast_to(bt[0, 0, :, b:b + 1], (n_state, 128))
    conv_out[0, 0] = conv_in[0, 1]
    conv_out[0, 1] = conv_in[0, 2]
    conv_out[0, 2] = xi[0]

    def group(g, carry):
        rws16 = pl.ds(pl.multiple_of(g * 16, 16), 16)
        for j in range(e_loc // 128):
            cols = slice(j * 128, (j + 1) * 128)
            a = a_neg[:, cols]
            dtx = dt[0, rws16, cols] * x[0, rws16, cols].astype(F32)
            for p in range(2):
                rws = pl.ds(pl.multiple_of(g * 16 + p * 8, 8), 8)
                decay = jnp.exp2(dt[0, rws, cols][:, None, :] * a[None])
                ssm_out[0, rws, :, cols] = decay * ssm_in[0, rws, :, cols] + dtx[p * 8:p * 8 + 8][:, None, :] * b_bc[rws]
        return carry

    lax.fori_loop(0, blk // 16, group, 0)


def state_pass(l, ssm_t, dt, x, bt, a_log_t, conv_t, xi, carried):
    _, half, n_state, e_loc = ssm_t.shape
    blk = 32
    per = half // N_CHUNK // blk

    def rows_spec(*tail):
        return pl.BlockSpec((1, blk) + tail, lambda g: (l, g) + (0,) * len(tail))

    conv_spec = pl.BlockSpec((1, 3, blk, e_loc), lambda g: (l, 0, g, 0))
    in_specs = [rows_spec(n_state, e_loc), rows_spec(e_loc), rows_spec(e_loc),
                pl.BlockSpec((1, 1, n_state, 128), lambda g: (l * N_CHUNK + g // per, g % per, 0, 0)),
                pl.BlockSpec((1, n_state, e_loc), lambda g: (l, 0, 0)), conv_spec, rows_spec(e_loc)]
    in_specs += [pl.BlockSpec(memory_space=pl.ANY)] * len(carried)
    n_elem = half * n_state * e_loc
    return pl.pallas_call(
        functools.partial(state_kernel, len(carried), blk),
        grid=(half // blk,),
        out_shape=(jax.ShapeDtypeStruct(ssm_t.shape, F32), jax.ShapeDtypeStruct(conv_t.shape, BF)),
        in_specs=in_specs,
        out_specs=(rows_spec(n_state, e_loc), conv_spec),
        scratch_shapes=[pltpu.VMEM((n_state, e_loc), F32), pltpu.VMEM((blk, n_state, 128), F32)],
        input_output_aliases={7 + k: k for k in range(len(carried))},
        compiler_params=pltpu.CompilerParams(vmem_limit_bytes=67043328),
        cost_estimate=pl.CostEstimate(flops=n_elem * 1000, bytes_accessed=n_elem * 8, transcendentals=n_elem),
    )(ssm_t, dt, x, bt, a_log_t, conv_t, xi, *carried)


def out_kernel(g_ref, w_ref, o_ref):
    def tile(t, carry):
        cols = pl.ds(pl.multiple_of(t * 256, 256), 256)
        o_ref[:, cols] = jnp.dot(g_ref[...], w_ref[0, :, cols], preferred_element_type=F32)
        return carry

    lax.fori_loop(0, w_ref.shape[2] // 256, tile, 0)


def out_proj(g, w_out, l):
    return pl.pallas_call(
        out_kernel,
        grid=(1,),
        out_shape=jax.ShapeDtypeStruct((g.shape[0], w_out.shape[2]), F32),
        in_specs=[pl.BlockSpec(g.shape, lambda q: (0, 0)), pl.BlockSpec((1,) + w_out.shape[1:], lambda q: (l, 0, 0))],
        out_specs=pl.BlockSpec((g.shape[0], w_out.shape[2]), lambda q: (0, 0)),
        compiler_params=pltpu.CompilerParams(vmem_limit_bytes=67043328),
        name="out_proj",
    )(g, w_out)


def solution(mesh):
    def local_step(residual, norm_w, w_in, conv_w, conv_b, w_x, w_dt, dt_bias, a_log, d_skip, w_out, conv_state, ssm_state):
        n_layer = norm_w.shape[0]
        rows, d_loc = residual.shape
        e_loc = w_x.shape[1]
        n_state = a_log.shape[-1]
        n_rank = w_dt.shape[1]
        n_proj = w_x.shape[2]
        d_model = d_loc * mesh.shape["tx"]
        total = n_layer * N_CHUNK
        blk = rows // 2 // N_CHUNK
        dims = (n_layer, rows, d_loc, e_loc, n_state, n_rank, d_model)
        w_in_t = jnp.transpose(w_in, (0, 2, 1, 3))
        conv_t = jnp.transpose(conv_state, (0, 3, 1, 2))
        ssm_t = jnp.transpose(ssm_state, (0, 1, 3, 2))
        a_log_t = jnp.transpose(a_log, (0, 2, 1))
        args = (residual, norm_w, w_in_t, jnp.transpose(conv_w, (0, 2, 1)), conv_b, jnp.transpose(w_x, (0, 2, 1)), w_dt, dt_bias, a_log_t, d_skip, w_out, conv_t, ssm_t)
        hbm = pl.BlockSpec(memory_space=pl.ANY)
        vmem = pl.BlockSpec(memory_space=pltpu.VMEM)
        in_specs = [hbm, vmem, hbm, vmem, vmem, vmem, vmem, vmem, vmem, vmem, hbm, hbm, hbm]
        dma = pltpu.SemaphoreType.DMA
        scratch = [pltpu.VMEM((n_layer, 1, d_loc), F32)] + [pltpu.VMEM((n_layer, 1, e_loc), F32)] * 3 + [
            pltpu.VMEM((n_layer, 2, d_loc, e_loc), BF),
            pltpu.VMEM((n_layer, e_loc, d_loc), BF),
            pltpu.VMEM((n_layer, n_state, e_loc), F32),
            pltpu.VMEM((2, blk, n_state, e_loc), F32),
            pltpu.VMEM((2, 4, blk, e_loc), BF),
            pltpu.VMEM((2 * blk, d_loc), BF),
            pltpu.VMEM((2, 2, blk, e_loc), F32),
            pltpu.VMEM((blk, e_loc), F32),
            pltpu.VMEM((blk, e_loc), BF),
            pltpu.VMEM((blk, n_rank), BF),
            pltpu.VMEM((blk, e_loc), F32),
            pltpu.VMEM((blk, e_loc), F32),
            pltpu.VMEM((blk, n_state, 128), F32),
            pltpu.VMEM((blk, n_state, 128), F32),
            pltpu.VMEM((2 * blk, d_loc), F32),
            pltpu.VMEM((total, 8, 2 * blk), F32),
            pltpu.VMEM((total, 8, 2 * blk), F32),
            pltpu.VMEM((2, 2, blk, e_loc), BF),
            pltpu.VMEM((total, 2, blk, e_loc), BF),
            pltpu.VMEM((n_proj, 2 * blk), F32),
            pltpu.VMEM((2, n_proj, 2 * blk), BF),
            pltpu.VMEM((total, 3, n_proj, 2 * blk), BF),
            pltpu.VMEM((total, 2 * blk, e_loc), BF),
        ] + [pltpu.VMEM((total, blk, d_loc), BF)] * 6 + [
            dma((2 + n_layer,)), dma((2,)), dma((2,)), dma(()), dma(()), dma((2,)), dma((N_CHUNK,)),
            dma((total,)), dma((total,)), dma((2, 2)), dma((total, 2)), dma((2, 3)), dma((total, 3)),
            dma((total,)), dma((total,)), dma((total,)), dma((total,)), dma((total,)), dma((total,)), dma((total,)), dma((total,)),
        ]
        half = rows // 2
        r_mid, bt, g_own, dt, x_act, xi = pl.pallas_call(
            functools.partial(step_kernel, dims),
            out_shape=(jax.ShapeDtypeStruct((rows, d_loc), F32), jax.ShapeDtypeStruct((total, 2, n_state, 128), F32), jax.ShapeDtypeStruct((half, e_loc), BF),
                       jax.ShapeDtypeStruct((n_layer, half, e_loc), F32), jax.ShapeDtypeStruct((n_layer, half, e_loc), BF), jax.ShapeDtypeStruct((n_layer, half, e_loc), BF)),
            in_specs=in_specs,
            out_specs=(vmem, vmem, hbm, hbm, hbm, hbm),
            scratch_shapes=scratch,
            compiler_params=pltpu.CompilerParams(collective_id=0, has_side_effects=True, vmem_limit_bytes=67043328),
            name="mamba_step",
        )(*args)

        core = lax.rem(lax.axis_index("ty"), 2)
        tx = lax.axis_index("tx")
        core_swap = [(0, 1), (1, 0), (2, 3), (3, 2)]
        g_peer = lax.ppermute(g_own, "tx", [(0, 1), (1, 0)])
        caches = state_pass(0, ssm_t, dt, x_act, bt, a_log_t, conv_t, xi, ())
        o_own = out_proj(g_own, w_out, n_layer - 1)
        o_peer = out_proj(g_peer, w_out, n_layer - 1)
        kept = jnp.where(core == 0, o_own, o_peer)
        sent = jnp.where(core == 0, o_peer, o_own).astype(BF)
        part = (kept + lax.ppermute(sent, "ty", core_swap).astype(F32)).astype(BF)
        other = lax.ppermute(part, "ty", [(0, 2), (2, 0), (1, 3), (3, 1)])
        caches = state_pass(1, ssm_t, dt, x_act, bt, a_log_t, conv_t, xi, caches)
        tot = (part.astype(F32) + other.astype(F32)).astype(BF)
        tot_peer = lax.ppermute(tot, "ty", core_swap)
        first = jnp.where(core == tx, tot, tot_peer)
        second = jnp.where(core == tx, tot_peer, tot)
        r_out = r_mid + jnp.concatenate([first, second], axis=0).astype(F32)
        return r_out, jnp.transpose(caches[1], (0, 2, 3, 1)), jnp.transpose(caches[0], (0, 1, 3, 2))

    cache_spec = P(None, ("dp", "tx"), "ty", None)
    in_specs = (P("dp", "tx"), P(None, "tx"), P(None, "tx", None, "ty"), P(None, "ty", None), P(None, "ty"), P(None, "ty", None), P(None, None, "ty"), P(None, "ty"), P(None, "ty", None), P(None, "ty"), P(None, "ty", "tx"), cache_spec, cache_spec)
    out_specs = (P("dp", "tx"), cache_spec, cache_spec)
    return jax.shard_map(local_step, mesh=mesh, in_specs=in_specs, out_specs=out_specs, check_vma=False)
```

```python
import functools
import jax
import jax.numpy as jnp
from jax import lax
from jax.experimental import pallas as pl
from jax.experimental.pallas import tpu as pltpu
from jax.sharding import PartitionSpec as P


NORM_EPS = 1e-5
INNER_EPS = 1e-6
LOG2E = 1.4426950408889634
N_CHUNK = 4
BF = jnp.bfloat16
F32 = jnp.float32
MESH = pl.DeviceIdType.MESH


def step_kernel(dims, res_hbm, norm_w_in, w_in_hbm, conv_w, conv_b_in, w_x, w_dt, dt_bias_in, a_log, d_skip_in, w_out_hbm, conv_hbm, ssm_hbm,
                r_ref, bt_out, g_out, o_out, dt_out, x_out, xi_out,
                norm_w, conv_b, dt_bias, d_skip, w_in, w_out, a_neg, ssm_buf, conv_buf, h_buf, u_own, z_buf, x_buf, low_buf, dt_buf, dtx_buf, b_bc, c_bc, o_buf, hx_buf,
                st_send, st_recv, u_send, u_recv, p_own, p_send, p_recv, g_all, cr_send, cr_recv, xs_send, xs_recv,
                in_sem, ssm_in_sem, conv_in_sem, dt_sem, x_sem, xi_sem, go_sem, o_sem,
                st_s, st_r, u_s, u_r, p_s, p_r, g_s, g_r, cr_s, cr_r, xs_s, xs_r):
    n_layer, rows, d_loc, e_loc, n_state, n_rank, d_model = dims
    half = rows // 2
    n_chunk = N_CHUNK
    blk = half // n_chunk
    total = n_layer * n_chunk
    n_tile = e_loc // 256
    tx = lax.axis_index("tx")
    ty = lax.axis_index("ty")
    core = lax.rem(ty, 2)
    chip = lax.div(ty, 2)
    y_peer = {"tx": 1 - tx, "ty": ty}
    core_peer = {"tx": tx, "ty": chip * 2 + (1 - core)}
    x_peer = {"tx": tx, "ty": (1 - chip) * 2 + core}
    d_peer = {"tx": tx, "ty": (1 - chip) * 2 + (1 - core)}

    def layer_of(i):
        return lax.div(i, n_chunk)

    def chunk_of(i):
        return lax.rem(i, n_chunk)

    def part_rows(i, part):
        side = jnp.where(part == 0, tx, 1 - tx)
        return pl.multiple_of(side * half + chunk_of(i) * blk, blk)

    def remote(src, dst, s_sem, r_sem, dev):
        return pltpu.make_async_remote_copy(src_ref=src, dst_ref=dst, send_sem=s_sem, recv_sem=r_sem, device_id=dev, device_id_type=MESH)

    def st_copy(i):
        return remote(st_send.at[i], st_recv.at[i], st_s.at[i], st_r.at[i], y_peer)

    def u_copy(i, k):
        s = lax.rem(i, 2)
        return remote(u_send.at[s, k], u_recv.at[i, k], u_s.at[s, k], u_r.at[i, k], y_peer)

    def p_copy(i, q):
        s = lax.rem(i, 2)
        dev = (core_peer, x_peer, d_peer)[q]
        return remote(p_send.at[s], p_recv.at[i, q], p_s.at[s, q], p_r.at[i, q], dev)

    def g_copy(i):
        return remote(g_all.at[i, pl.ds(0, blk)], g_all.at[i, pl.ds(blk, blk)], g_s.at[i], g_r.at[i], y_peer)

    def cr_copy(i):
        return remote(cr_send.at[i], cr_recv.at[i], cr_s.at[i], cr_r.at[i], core_peer)

    def half_rows(h):
        return pl.ds(pl.multiple_of(h * blk, blk), blk)

    def xs_copy(i, q, h):
        return remote(xs_send.at[i, half_rows(h)], xs_recv.at[i, half_rows(h)], xs_s.at[i, q], xs_r.at[i, h], (x_peer, d_peer)[q])

    def cache_rows(i):
        return pl.ds(pl.multiple_of(chunk_of(i) * blk, blk), blk)

    def ssm_load(i):
        s = lax.rem(i, 2)
        return pltpu.make_async_copy(ssm_hbm.at[layer_of(i), cache_rows(i)], ssm_buf.at[s], ssm_in_sem.at[s])

    def conv_load(i):
        s = lax.rem(i, 2)
        return pltpu.make_async_copy(conv_hbm.at[layer_of(i), :, cache_rows(i)], conv_buf.at[s, pl.ds(0, 3)], conv_in_sem.at[s])

    def dt_store(i):
        return pltpu.make_async_copy(dt_buf, dt_out.at[layer_of(i), cache_rows(i)], dt_sem)

    def x_store(i):
        return pltpu.make_async_copy(x_buf, x_out.at[layer_of(i), cache_rows(i)], x_sem)

    def xi_store(i):
        s = lax.rem(i, 2)
        return pltpu.make_async_copy(conv_buf.at[s, 3], xi_out.at[layer_of(i), cache_rows(i)], xi_sem.at[s])

    def o_store(i):
        return pltpu.make_async_copy(o_buf, o_out.at[cache_rows(i)], o_sem)

    def g_store(i):
        return pltpu.make_async_copy(g_all.at[i, pl.ds(0, blk)], g_out.at[cache_rows(i)], go_sem.at[chunk_of(i)])

    res_load = pltpu.make_async_copy(res_hbm, r_ref, in_sem.at[0])
    w_in_load = [pltpu.make_async_copy(w_in_hbm.at[l], w_in.at[l], in_sem.at[1 + l]) for l in range(n_layer)]
    w_out_load = pltpu.make_async_copy(w_out_hbm, w_out, in_sem.at[1 + n_layer])

    res_load.start()
    w_in_load[0].start()

    barrier = pltpu.get_barrier_semaphore()
    for dev in (y_peer, core_peer, x_peer, d_peer):
        pl.semaphore_signal(barrier, inc=1, device_id=dev, device_id_type=MESH)
    pl.semaphore_wait(barrier, 4)

    def eye():
        n = 2 * blk
        return lax.broadcasted_iota(jnp.int32, (n, n), 0) == lax.broadcasted_iota(jnp.int32, (n, n), 1)

    def phase_a(i):
        sums = []
        for part in range(2):
            val = r_ref[pl.ds(part_rows(i, part), blk), :]
            sums.append(jnp.sum(val * val, axis=1, keepdims=True))
        col = jnp.concatenate(sums, axis=0)
        row = jnp.sum(jnp.where(eye(), col, 0.0), axis=0, keepdims=True)
        st_send[i] = jnp.broadcast_to(row, (8, 2 * blk))
        st_copy(i).start()

    def phase_b(i):
        l = layer_of(i)
        s = lax.rem(i, 2)
        st_copy(i).wait_recv()
        sq = st_send[i] + pltpu.roll(st_recv[i], blk, 1)
        inv = lax.rsqrt(sq / d_model + NORM_EPS)
        col = jnp.sum(jnp.where(eye(), jnp.broadcast_to(inv[0:1], (2 * blk, 2 * blk)), 0.0), axis=1, keepdims=True)
        nw = norm_w[l]
        for part in range(2):
            base = part_rows(i, part)
            for q in range(blk // 16):
                lo = part * blk + q * 16
                val = r_ref[pl.ds(base + q * 16, 16), :]
                h_buf[lo:lo + 16, :] = (val * col[lo:lo + 16] * nw).astype(BF)

        src = lax.broadcasted_iota(jnp.int32, (128, 256), 0)
        dst = lax.broadcasted_iota(jnp.int32, (128, 256), 1)
        for k in range(2):
            spread = jnp.where(dst == 2 * src + k, 1.0, 0.0).astype(BF)
            for t in range(d_loc // 128):
                wide = jnp.dot(h_buf[:, t * 128:(t + 1) * 128], spread, preferred_element_type=F32)
                hx_buf[k * 2 * blk:(k + 1) * 2 * blk, t * 256:(t + 1) * 256] = wide.astype(BF)

        @pl.when(i >= 2)
        def _():
            def done(k, carry):
                u_copy(i - 2, k).wait_send()
                return carry

            lax.fori_loop(0, 2 * n_tile, done, 0)

        w_rows = w_in.at[l].reshape(2 * d_loc, e_loc)

        def tile(t, carry):
            cols = pl.ds(pl.multiple_of(t * 256, 256), 256)
            u = jnp.dot(hx_buf[...], w_rows[:, cols], preferred_element_type=F32)
            for k in range(2):
                u_own[s, k, :, cols] = u[2 * k * blk:(2 * k + 1) * blk]
                u_send[s, k * n_tile + t] = u[(2 * k + 1) * blk:(2 * k + 2) * blk].astype(BF)
            u_copy(i, t).start()
            return carry

        lax.fori_loop(0, n_tile, tile, 0)

        def send_z(t, carry):
            u_copy(i, n_tile + t).start()
            return carry

        lax.fori_loop(0, n_tile, send_z, 0)

    def phase_c(i):
        l = layer_of(i)
        s = lax.rem(i, 2)

        @pl.when(i >= 1)
        def _():
            xi_store(i - 1).wait()
            x_store(i - 1).wait()

            @pl.when(i + 1 < total)
            def _():
                conv_load(i + 1).start()

        conv_load(i).wait()

        def conv_tile(t, carry):
            u_copy(i, t).wait_recv()
            cols = pl.ds(pl.multiple_of(t * 256, 256), 256)
            xi = (u_own[s, 0, :, cols] + u_recv[i, t].astype(F32)).astype(BF)
            conv_buf[s, 3, :, cols] = xi
            acc = conv_buf[s, 0, :, cols].astype(F32) * conv_w[l, 0:1, cols]
            acc = acc + conv_buf[s, 1, :, cols].astype(F32) * conv_w[l, 1:2, cols]
            acc = acc + conv_buf[s, 2, :, cols].astype(F32) * conv_w[l, 2:3, cols]
            acc = acc + xi.astype(F32) * conv_w[l, 3:4, cols]
            acc = acc + conv_b[l, :, cols]
            x_buf[:, cols] = (acc * jax.nn.sigmoid(acc)).astype(BF)
            return carry

        lax.fori_loop(0, n_tile, conv_tile, 0)
        xi_store(i).start()
        x_store(i).start()

        @pl.when(i >= 2)
        def _():
            for q in range(3):
                p_copy(i - 2, q).wait_send()

        pt = lax.dot_general(w_x[l], x_buf[...], (((1,), (1,)), ((), ())), preferred_element_type=F32)
        pt = jnp.concatenate([pt, pt], axis=1)
        p_own[...] = pt
        p_send[s] = pt.astype(BF)
        for q in range(3):
            p_copy(i, q).start()

    def phase_d(i):
        l = layer_of(i)
        s = lax.rem(i, 2)

        def z_tile(t, carry):
            u_copy(i, n_tile + t).wait_recv()
            cols = pl.ds(pl.multiple_of(t * 256, 256), 256)
            z = (u_own[s, 1, :, cols] + u_recv[i, n_tile + t].astype(F32)).astype(BF).astype(F32)
            z_buf[:, cols] = z * jax.nn.sigmoid(z)
            return carry

        lax.fori_loop(0, n_tile, z_tile, 0)
        for q in range(3):
            p_copy(i, q).wait_recv()
        pt = p_own[...]
        for q in range(3):
            pt = pt + p_recv[i, q].astype(F32)

        def unit(v):
            return v * lax.rsqrt(jnp.mean(v * v, axis=0, keepdims=True) + INNER_EPS)

        low_buf[...] = jnp.transpose(unit(pt[:n_rank]))[:blk].astype(BF)
        bt = unit(pt[n_rank:n_rank + n_state])
        ct = unit(pt[n_rank + n_state:])
        bt_out[i] = bt
        for b in range(blk):
            b_bc[b] = jnp.broadcast_to(bt[:, b:b + 1], (n_state, 128))
            c_bc[b] = jnp.broadcast_to(ct[:, b:b + 1], (n_state, 128))

        @pl.when(i >= 1)
        def _():
            dt_store(i - 1).wait()

        def dt_tile(t, carry):
            cols = pl.ds(pl.multiple_of(t * 256, 256), 256)
            v = jnp.dot(low_buf[...], w_dt[l, :, cols], preferred_element_type=F32)
            v = v + dt_bias[l, :, cols]
            dt = jnp.maximum(v, 0.0) + jnp.log1p(jnp.exp(-jnp.abs(v)))
            dt_buf[:, cols] = dt
            dtx_buf[:, cols] = dt * x_buf[:, cols].astype(F32)
            return carry

        lax.fori_loop(0, e_loc // 256, dt_tile, 0)
        dt_store(i).start()
        ssm_load(i).wait()

        def group(g, carry):
            for j in range(e_loc // 128):
                cols = slice(j * 128, (j + 1) * 128)
                a = a_neg[l, :, cols]
                out = []
                for p in range(2):
                    rws = pl.ds(pl.multiple_of(g * 16 + p * 8, 8), 8)
                    decay = jnp.exp2(dt_buf[rws, cols][:, None, :] * a[None])
                    new = decay * ssm_buf[s, rws, :, cols] + dtx_buf[rws, cols][:, None, :] * b_bc[rws]
                    out.append(jnp.sum(new * c_bc[rws], axis=1))
                rws = pl.ds(pl.multiple_of(g * 16, 16), 16)
                y = jnp.concatenate(out, axis=0) + d_skip[l, :, cols] * x_buf[rws, cols].astype(F32)
                g_all[i, rws, cols] = (y * z_buf[rws, cols]).astype(BF)
            return carry

        lax.fori_loop(0, blk // 16, group, 0)

        @pl.when(i < total - n_chunk)
        def _():
            g_copy(i).start()

        @pl.when(i >= total - n_chunk)
        def _():
            g_store(i).start()

            @pl.when(i > total - n_chunk)
            def _():
                o_store(i - 1).wait()

            def o_tile(t, carry):
                cols = pl.ds(pl.multiple_of(t * 256, 256), 256)
                o_buf[:, cols] = jnp.dot(g_all[i, pl.ds(0, blk)], w_out[l, :, cols], preferred_element_type=F32)
                return carry

            lax.fori_loop(0, d_loc // 256, o_tile, 0)
            o_store(i).start()

    def phase_e(i):
        l = layer_of(i)
        g_copy(i).wait_recv()

        def tile(t, carry):
            cols = pl.ds(pl.multiple_of(t * 256, 256), 256)
            cr_send[i, :, cols] = jnp.dot(g_all[i], w_out[l, :, cols], preferred_element_type=F32).astype(BF)
            return carry

        lax.fori_loop(0, d_loc // 256, tile, 0)
        cr_copy(i).start()

    def phase_f(i):
        cr_copy(i).wait_recv()
        xs_send[i] = (cr_send[i].astype(F32) + cr_recv[i].astype(F32)).astype(BF)
        for q in range(2):
            xs_copy(i, q, core).start()

    def phase_g(i):
        for h in range(2):
            xs_copy(i, 0, h).wait_recv()
            rws = pl.ds(part_rows(i, h), blk)
            r_ref[rws, :] = r_ref[rws, :] + (xs_send[i, h * blk:(h + 1) * blk].astype(F32) + xs_recv[i, h * blk:(h + 1) * blk].astype(F32))
        phase_a(i + n_chunk)

    for l in range(n_layer):
        for vec, src in ((norm_w, norm_w_in), (conv_b, conv_b_in), (dt_bias, dt_bias_in), (d_skip, d_skip_in)):
            vec[l] = src[l:l + 1, :]
        a_neg[l] = jnp.exp(a_log[l]) * (-LOG2E)
    res_load.wait()

    def first_a(i, carry):
        phase_a(i)
        return carry

    lax.fori_loop(0, n_chunk, first_a, 0)
    w_in_load[0].wait()

    def run(phase, i, stop=total):
        ok = (i >= 0) & (i < stop)

        @pl.when(ok)
        def _():
            phase(i)

    def step(s, carry):
        last = total - n_chunk
        run(phase_g, s - 4, last)

        @pl.when((s >= 2) & (s < total))
        def _():
            ssm_load(s).start()

        run(phase_c, s - 1)
        run(phase_f, s - 3, last)

        @pl.when(s == n_chunk)
        def _():
            w_in_load[1].wait()

        run(phase_b, s)

        @pl.when(s == 0)
        def _():
            conv_load(0).start()
            conv_load(1).start()
            ssm_load(0).start()
            ssm_load(1).start()
            w_out_load.start()
            w_in_load[1].start()

        run(phase_d, s - 1)

        @pl.when(s == 2)
        def _():
            w_out_load.wait()

        run(phase_e, s - 2, last)
        return carry

    lax.fori_loop(0, total + 1, step, 0)

    xi_store(total - 1).wait()
    x_store(total - 1).wait()
    dt_store(total - 1).wait()
    o_store(total - 1).wait()
    for i in range(total - 2, total):
        for k in range(2 * n_tile):
            u_copy(i, k).wait_send()
        for q in range(3):
            p_copy(i, q).wait_send()

    def drain(i, carry):
        st_copy(i).wait_send()
        st_copy(i + n_chunk).wait_send()
        g_copy(i).wait_send()
        cr_copy(i).wait_send()
        for q in range(2):
            xs_copy(i, q, core).wait_send()
        g_store(i + total - n_chunk).wait()
        return carry

    lax.fori_loop(0, n_chunk, drain, 0)


def state_kernel(n_carry, blk, ssm_in, dt, x, bt, a_log, conv_in, xi, *refs):
    ssm_out, conv_out, a_neg, b_bc = refs[n_carry:]
    n_state, e_loc = a_log.shape[1:]

    @pl.when(pl.program_id(0) == 0)
    def _():
        a_neg[...] = jnp.exp(a_log[0]) * (-LOG2E)

    for b in range(blk):
        b_bc[b] = jnp.broadcast_to(bt[0, :, b:b + 1], (n_state, 128))
    conv_out[0, 0] = conv_in[0, 1]
    conv_out[0, 1] = conv_in[0, 2]
    conv_out[0, 2] = xi[0]

    def group(g, carry):
        rws16 = pl.ds(pl.multiple_of(g * 16, 16), 16)
        for j in range(e_loc // 128):
            cols = slice(j * 128, (j + 1) * 128)
            a = a_neg[:, cols]
            dtx = dt[0, rws16, cols] * x[0, rws16, cols].astype(F32)
            for p in range(2):
                rws = pl.ds(pl.multiple_of(g * 16 + p * 8, 8), 8)
                decay = jnp.exp2(dt[0, rws, cols][:, None, :] * a[None])
                ssm_out[0, rws, :, cols] = decay * ssm_in[0, rws, :, cols] + dtx[p * 8:p * 8 + 8][:, None, :] * b_bc[rws]
        return carry

    lax.fori_loop(0, blk // 16, group, 0)


def state_pass(l, ssm_t, dt, x, bt, a_log_t, conv_t, xi, carried):
    _, half, n_state, e_loc = ssm_t.shape
    blk = half // N_CHUNK

    def rows_spec(*tail):
        return pl.BlockSpec((1, blk) + tail, lambda g: (l, g) + (0,) * len(tail))

    conv_spec = pl.BlockSpec((1, 3, blk, e_loc), lambda g: (l, 0, g, 0))
    in_specs = [rows_spec(n_state, e_loc), rows_spec(e_loc), rows_spec(e_loc),
                pl.BlockSpec((1, n_state, 128), lambda g: (l * N_CHUNK + g, 0, 0)),
                pl.BlockSpec((1, n_state, e_loc), lambda g: (l, 0, 0)), conv_spec, rows_spec(e_loc)]
    in_specs += [pl.BlockSpec(memory_space=pl.ANY)] * len(carried)
    n_elem = half * n_state * e_loc
    return pl.pallas_call(
        functools.partial(state_kernel, len(carried), blk),
        grid=(half // blk,),
        out_shape=(jax.ShapeDtypeStruct(ssm_t.shape, F32), jax.ShapeDtypeStruct(conv_t.shape, BF)),
        in_specs=in_specs,
        out_specs=(rows_spec(n_state, e_loc), conv_spec),
        scratch_shapes=[pltpu.VMEM((n_state, e_loc), F32), pltpu.VMEM((blk, n_state, 128), F32)],
        input_output_aliases={7 + k: k for k in range(len(carried))},
        compiler_params=pltpu.CompilerParams(vmem_limit_bytes=67043328),
        cost_estimate=pl.CostEstimate(flops=n_elem * 1000, bytes_accessed=n_elem * 8, transcendentals=n_elem),
    )(ssm_t, dt, x, bt, a_log_t, conv_t, xi, *carried)


def out_kernel(g_ref, w_ref, o_ref):
    def tile(t, carry):
        cols = pl.ds(pl.multiple_of(t * 256, 256), 256)
        o_ref[:, cols] = jnp.dot(g_ref[...], w_ref[0, :, cols], preferred_element_type=F32)
        return carry

    lax.fori_loop(0, w_ref.shape[2] // 256, tile, 0)


def out_proj(g, w_out, l):
    return pl.pallas_call(
        out_kernel,
        grid=(1,),
        out_shape=jax.ShapeDtypeStruct((g.shape[0], w_out.shape[2]), F32),
        in_specs=[pl.BlockSpec(g.shape, lambda q: (0, 0)), pl.BlockSpec((1,) + w_out.shape[1:], lambda q: (l, 0, 0))],
        out_specs=pl.BlockSpec((g.shape[0], w_out.shape[2]), lambda q: (0, 0)),
        compiler_params=pltpu.CompilerParams(vmem_limit_bytes=67043328),
        name="out_proj",
    )(g, w_out)


def solution(mesh):
    def local_step(residual, norm_w, w_in, conv_w, conv_b, w_x, w_dt, dt_bias, a_log, d_skip, w_out, conv_state, ssm_state):
        n_layer = norm_w.shape[0]
        rows, d_loc = residual.shape
        e_loc = w_x.shape[1]
        n_state = a_log.shape[-1]
        n_rank = w_dt.shape[1]
        n_proj = w_x.shape[2]
        d_model = d_loc * mesh.shape["tx"]
        total = n_layer * N_CHUNK
        blk = rows // 2 // N_CHUNK
        dims = (n_layer, rows, d_loc, e_loc, n_state, n_rank, d_model)
        conv_t = jnp.transpose(conv_state, (0, 3, 1, 2))
        ssm_t = jnp.transpose(ssm_state, (0, 1, 3, 2))
        a_log_t = jnp.transpose(a_log, (0, 2, 1))
        args = (residual, norm_w, w_in, jnp.transpose(conv_w, (0, 2, 1)), conv_b, jnp.transpose(w_x, (0, 2, 1)), w_dt, dt_bias, a_log_t, d_skip, w_out, conv_t, ssm_t)
        hbm = pl.BlockSpec(memory_space=pl.ANY)
        vmem = pl.BlockSpec(memory_space=pltpu.VMEM)
        in_specs = [hbm, vmem, hbm, vmem, vmem, vmem, vmem, vmem, vmem, vmem, hbm, hbm, hbm]
        dma = pltpu.SemaphoreType.DMA
        scratch = [pltpu.VMEM((n_layer, 1, d_loc), F32)] + [pltpu.VMEM((n_layer, 1, e_loc), F32)] * 3 + [
            pltpu.VMEM((n_layer, d_loc, 2, e_loc), BF),
            pltpu.VMEM((n_layer, e_loc, d_loc), BF),
            pltpu.VMEM((n_layer, n_state, e_loc), F32),
            pltpu.VMEM((2, blk, n_state, e_loc), F32),
            pltpu.VMEM((2, 4, blk, e_loc), BF),
            pltpu.VMEM((2 * blk, d_loc), BF),
            pltpu.VMEM((2, 2, blk, e_loc), F32),
            pltpu.VMEM((blk, e_loc), F32),
            pltpu.VMEM((blk, e_loc), BF),
            pltpu.VMEM((blk, n_rank), BF),
            pltpu.VMEM((blk, e_loc), F32),
            pltpu.VMEM((blk, e_loc), F32),
            pltpu.VMEM((blk, n_state, 128), F32),
            pltpu.VMEM((blk, n_state, 128), F32),
            pltpu.VMEM((blk, d_loc), F32),
            pltpu.VMEM((4 * blk, 2 * d_loc), BF),
            pltpu.VMEM((total, 8, 2 * blk), F32),
            pltpu.VMEM((total, 8, 2 * blk), F32),
            pltpu.VMEM((2, 2 * (e_loc // 256), blk, 256), BF),
            pltpu.VMEM((total, 2 * (e_loc // 256), blk, 256), BF),
            pltpu.VMEM((n_proj, 2 * blk), F32),
            pltpu.VMEM((2, n_proj, 2 * blk), BF),
            pltpu.VMEM((total, 3, n_proj, 2 * blk), BF),
            pltpu.VMEM((total, 2 * blk, e_loc), BF),
        ] + [pltpu.VMEM((N_CHUNK, 2 * blk, d_loc), BF)] * 4 + [
            dma((2 + n_layer,)), dma((2,)), dma((2,)), dma(()), dma(()), dma((2,)), dma((N_CHUNK,)), dma(()),
            dma((total,)), dma((total,)), dma((2, 2 * (e_loc // 256))), dma((total, 2 * (e_loc // 256))), dma((2, 3)), dma((total, 3)),
            dma((total,)), dma((total,)), dma((N_CHUNK,)), dma((N_CHUNK,)), dma((N_CHUNK, 2)), dma((N_CHUNK, 2)),
        ]
        half = rows // 2
        r_mid, bt, g_own, o_own, dt, x_act, xi = pl.pallas_call(
            functools.partial(step_kernel, dims),
            out_shape=(jax.ShapeDtypeStruct((rows, d_loc), F32), jax.ShapeDtypeStruct((total, n_state, 128), F32), jax.ShapeDtypeStruct((half, e_loc), BF), jax.ShapeDtypeStruct((half, d_loc), F32),
                       jax.ShapeDtypeStruct((n_layer, half, e_loc), F32), jax.ShapeDtypeStruct((n_layer, half, e_loc), BF), jax.ShapeDtypeStruct((n_layer, half, e_loc), BF)),
            in_specs=in_specs,
            out_specs=(vmem, vmem, hbm, hbm, hbm, hbm, hbm),
            scratch_shapes=scratch,
            compiler_params=pltpu.CompilerParams(collective_id=0, has_side_effects=True, vmem_limit_bytes=67043328),
            name="mamba_step",
        )(*args)

        core = lax.rem(lax.axis_index("ty"), 2)
        tx = lax.axis_index("tx")
        core_swap = [(0, 1), (1, 0), (2, 3), (3, 2)]
        g_peer = lax.ppermute(g_own, "tx", [(0, 1), (1, 0)])
        caches = state_pass(0, ssm_t, dt, x_act, bt, a_log_t, conv_t, xi, ())
        o_peer = out_proj(g_peer, w_out, n_layer - 1)
        kept = jnp.where(core == 0, o_own, o_peer)
        sent = jnp.where(core == 0, o_peer, o_own).astype(BF)
        part = (kept + lax.ppermute(sent, "ty", core_swap).astype(F32)).astype(BF)
        other = lax.ppermute(part, "ty", [(0, 2), (2, 0), (1, 3), (3, 1)])
        caches = state_pass(1, ssm_t, dt, x_act, bt, a_log_t, conv_t, xi, caches)
        tot = (part.astype(F32) + other.astype(F32)).astype(BF)
        tot_peer = lax.ppermute(tot, "ty", core_swap)
        first = jnp.where(core == tx, tot, tot_peer)
        second = jnp.where(core == tx, tot_peer, tot)
        r_out = r_mid + jnp.concatenate([first, second], axis=0).astype(F32)
        return r_out, jnp.transpose(caches[1], (0, 2, 3, 1)), jnp.transpose(caches[0], (0, 1, 3, 2))

    cache_spec = P(None, ("dp", "tx"), "ty", None)
    in_specs = (P("dp", "tx"), P(None, "tx"), P(None, "tx", None, "ty"), P(None, "ty", None), P(None, "ty"), P(None, "ty", None), P(None, None, "ty"), P(None, "ty"), P(None, "ty", None), P(None, "ty"), P(None, "ty", "tx"), cache_spec, cache_spec)
    out_specs = (P("dp", "tx"), cache_spec, cache_spec)
    return jax.shard_map(local_step, mesh=mesh, in_specs=in_specs, out_specs=out_specs, check_vma=False)
```

```python
import functools
import jax
import jax.numpy as jnp
from jax import lax
from jax.experimental import pallas as pl
from jax.experimental.pallas import tpu as pltpu
from jax.sharding import PartitionSpec as P


NORM_EPS = 1e-5
INNER_EPS = 1e-6
LOG2E = 1.4426950408889634
N_CHUNK = 4
BF = jnp.bfloat16
F32 = jnp.float32
MESH = pl.DeviceIdType.MESH


def fold_rows(parts):
    sub = lax.broadcasted_iota(jnp.int32, (8, 128), 0)

    def pair(a, b, shift):
        low = (sub & shift) == 0
        p = jnp.where(low, a, b)
        q = jnp.where(low, b, a)
        if shift == 4:
            return p + pltpu.roll(q, 4, 0)
        return p + jnp.where(low, pltpu.roll(q, 8 - shift, 0), pltpu.roll(q, shift, 0))

    for shift in (4, 2, 1):
        parts = [pair(parts[b], parts[b + shift], shift) for b in range(shift)]
    return parts[0]


def step_kernel(dims, res_hbm, norm_w_in, w_in_hbm, conv_w, conv_b_in, w_x, w_dt, dt_bias_in, a_log, d_skip_in, w_out_hbm, conv_hbm, ssm_hbm,
                r_ref, bt_out, g_out, o_out, dt_out, x_out, xi_out,
                norm_w, conv_b, dt_bias, d_skip, w_in, w_out, a_neg, ssm_buf, conv_buf, h_buf, u_own, z_buf, x_buf, low_buf, dt_buf, dtx_buf, b_bc, c_bc, o_buf, hx_buf,
                st_send, st_recv, u_send, u_recv, p_own, p_send, p_recv, g_all, cr_send, cr_recv, xs_send, xs_recv,
                in_sem, ssm_in_sem, conv_in_sem, dt_sem, x_sem, xi_sem, go_sem, o_sem,
                st_s, st_r, u_s, u_r, p_s, p_r, g_s, g_r, cr_s, cr_r, xs_s, xs_r, fw_s, fw_r):
    n_layer, rows, d_loc, e_loc, n_state, n_rank, d_model = dims
    half = rows // 2
    n_chunk = N_CHUNK
    blk = half // n_chunk
    total = n_layer * n_chunk
    n_tile = e_loc // 256
    tx = lax.axis_index("tx")
    ty = lax.axis_index("ty")
    core = lax.rem(ty, 2)
    chip = lax.div(ty, 2)
    y_peer = {"tx": 1 - tx, "ty": ty}
    core_peer = {"tx": tx, "ty": chip * 2 + (1 - core)}
    x_peer = {"tx": tx, "ty": (1 - chip) * 2 + core}
    d_peer = {"tx": tx, "ty": (1 - chip) * 2 + (1 - core)}
    st_peer = {"tx": 1 - tx, "ty": (1 - chip) * 2 + core}

    def layer_of(i):
        return lax.div(i, n_chunk)

    def chunk_of(i):
        return lax.rem(i, n_chunk)

    def part_rows(i, part):
        side = jnp.where(part == 0, tx, 1 - tx)
        return pl.multiple_of(side * half + chunk_of(i) * blk, blk)

    def remote(src, dst, s_sem, r_sem, dev):
        return pltpu.make_async_remote_copy(src_ref=src, dst_ref=dst, send_sem=s_sem, recv_sem=r_sem, device_id=dev, device_id_type=MESH)

    def st_copy(i):
        return remote(st_send.at[i], st_recv.at[i], st_s.at[i], st_r.at[i], st_peer)

    def u_copy(i, k):
        s = lax.rem(i, 2)
        return remote(u_send.at[s, k], u_recv.at[i, k], u_s.at[s, k], u_r.at[i, k], y_peer)

    def p_copy(i, q):
        s = lax.rem(i, 2)
        dev = (core_peer, x_peer, d_peer)[q]
        return remote(p_send.at[s], p_recv.at[i, q], p_s.at[s, q], p_r.at[i, q], dev)

    def g_copy(i):
        return remote(g_all.at[i, pl.ds(0, blk)], g_all.at[i, pl.ds(blk, blk)], g_s.at[i], g_r.at[i], y_peer)

    def cr_copy(i):
        return remote(cr_send.at[i], cr_recv.at[i], cr_s.at[i], cr_r.at[i], core_peer)

    def half_rows(h):
        return pl.ds(pl.multiple_of(h * blk, blk), blk)

    def xs_copy(i):
        return remote(xs_send.at[i, half_rows(core)], xs_recv.at[i, half_rows(core)], xs_s.at[i], xs_r.at[i], x_peer)

    def fw_copy(i):
        return remote(xs_recv.at[i, half_rows(core)], xs_recv.at[i, half_rows(core)], fw_s.at[i], fw_r.at[i], core_peer)

    def cache_rows(i):
        return pl.ds(pl.multiple_of(chunk_of(i) * blk, blk), blk)

    def ssm_load(i):
        s = lax.rem(i, 2)
        return pltpu.make_async_copy(ssm_hbm.at[layer_of(i), cache_rows(i)], ssm_buf.at[s], ssm_in_sem.at[s])

    def conv_load(i):
        s = lax.rem(i, 2)
        return pltpu.make_async_copy(conv_hbm.at[layer_of(i), :, cache_rows(i)], conv_buf.at[s, pl.ds(0, 3)], conv_in_sem.at[s])

    def dt_store(i):
        n = blk // 8
        return pltpu.make_async_copy(dt_buf, dt_out.at[layer_of(i), pl.ds(chunk_of(i) * n, n)], dt_sem)

    def x_store(i):
        return pltpu.make_async_copy(x_buf, x_out.at[layer_of(i), cache_rows(i)], x_sem)

    def xi_store(i):
        s = lax.rem(i, 2)
        return pltpu.make_async_copy(conv_buf.at[s, 3], xi_out.at[layer_of(i), cache_rows(i)], xi_sem.at[s])

    def o_store(i):
        return pltpu.make_async_copy(o_buf, o_out.at[cache_rows(i)], o_sem)

    def g_store(i):
        return pltpu.make_async_copy(g_all.at[i, pl.ds(0, blk)], g_out.at[cache_rows(i)], go_sem.at[chunk_of(i)])

    res_load = pltpu.make_async_copy(res_hbm, r_ref, in_sem.at[0])
    w_in_load = [pltpu.make_async_copy(w_in_hbm.at[l], w_in.at[l], in_sem.at[1 + l]) for l in range(n_layer)]
    w_out_load = pltpu.make_async_copy(w_out_hbm, w_out, in_sem.at[1 + n_layer])

    res_load.start()
    w_in_load[0].start()

    barrier = pltpu.get_barrier_semaphore()
    for dev in (y_peer, core_peer, x_peer, d_peer, st_peer):
        pl.semaphore_signal(barrier, inc=1, device_id=dev, device_id_type=MESH)
    pl.semaphore_wait(barrier, 5)

    def eye():
        n = 2 * blk
        return lax.broadcasted_iota(jnp.int32, (n, n), 0) == lax.broadcasted_iota(jnp.int32, (n, n), 1)

    def phase_a(i):
        sums = []
        for part in range(2):
            val = r_ref[pl.ds(part_rows(i, part), blk), :]
            sums.append(jnp.sum(val * val, axis=1, keepdims=True))
        col = jnp.concatenate(sums, axis=0)
        row = jnp.sum(jnp.where(eye(), col, 0.0), axis=0, keepdims=True)
        st_send[i] = jnp.broadcast_to(row, (8, 2 * blk))
        st_copy(i).start()

    def phase_b(i):
        l = layer_of(i)
        s = lax.rem(i, 2)
        st_copy(i).wait_recv()
        sq = st_send[i] + pltpu.roll(st_recv[i], blk, 1)
        inv = lax.rsqrt(sq / d_model + NORM_EPS)
        col = jnp.sum(jnp.where(eye(), jnp.broadcast_to(inv[0:1], (2 * blk, 2 * blk)), 0.0), axis=1, keepdims=True)
        nw = norm_w[l]
        for part in range(2):
            base = part_rows(i, part)
            for q in range(blk // 16):
                lo = part * blk + q * 16
                val = r_ref[pl.ds(base + q * 16, 16), :]
                h_buf[lo:lo + 16, :] = (val * col[lo:lo + 16] * nw).astype(BF)

        src = lax.broadcasted_iota(jnp.int32, (128, 256), 0)
        dst = lax.broadcasted_iota(jnp.int32, (128, 256), 1)
        for k in range(2):
            spread = jnp.where(dst == 2 * src + k, 1.0, 0.0).astype(BF)
            for t in range(d_loc // 128):
                wide = jnp.dot(h_buf[:, t * 128:(t + 1) * 128], spread, preferred_element_type=F32)
                hx_buf[k * 2 * blk:(k + 1) * 2 * blk, t * 256:(t + 1) * 256] = wide.astype(BF)

        @pl.when(i >= 2)
        def _():
            def done(k, carry):
                u_copy(i - 2, k).wait_send()
                return carry

            lax.fori_loop(0, 2 * n_tile, done, 0)

        w_rows = w_in.at[l].reshape(2 * d_loc, e_loc)

        def tile(t, carry):
            cols = pl.ds(pl.multiple_of(t * 256, 256), 256)
            u = jnp.dot(hx_buf[...], w_rows[:, cols], preferred_element_type=F32)
            for k in range(2):
                u_own[s, k, :, cols] = u[2 * k * blk:(2 * k + 1) * blk]
                u_send[s, k * n_tile + t] = u[(2 * k + 1) * blk:(2 * k + 2) * blk].astype(BF)
            u_copy(i, t).start()
            return carry

        lax.fori_loop(0, n_tile, tile, 0, unroll=True)

        def send_z(t, carry):
            u_copy(i, n_tile + t).start()
            return carry

        lax.fori_loop(0, n_tile, send_z, 0)

    def phase_c(i):
        l = layer_of(i)
        s = lax.rem(i, 2)

        @pl.when(i >= 1)
        def _():
            xi_store(i - 1).wait()
            x_store(i - 1).wait()

            @pl.when(i + 1 < total)
            def _():
                conv_load(i + 1).start()

        conv_load(i).wait()

        def conv_tile(t, carry):
            u_copy(i, t).wait_recv()
            cols = pl.ds(pl.multiple_of(t * 256, 256), 256)
            xi = (u_own[s, 0, :, cols] + u_recv[i, t].astype(F32)).astype(BF)
            conv_buf[s, 3, :, cols] = xi
            acc = conv_buf[s, 0, :, cols].astype(F32) * conv_w[l, 0:1, cols]
            acc = acc + conv_buf[s, 1, :, cols].astype(F32) * conv_w[l, 1:2, cols]
            acc = acc + conv_buf[s, 2, :, cols].astype(F32) * conv_w[l, 2:3, cols]
            acc = acc + xi.astype(F32) * conv_w[l, 3:4, cols]
            acc = acc + conv_b[l, :, cols]
            x_buf[:, cols] = (acc * jax.nn.sigmoid(acc)).astype(BF)
            return carry

        lax.fori_loop(0, n_tile, conv_tile, 0, unroll=True)
        xi_store(i).start()
        x_store(i).start()

        @pl.when(i >= 2)
        def _():
            for q in range(3):
                p_copy(i - 2, q).wait_send()

        pt = lax.dot_general(w_x[l], x_buf[...], (((1,), (1,)), ((), ())), preferred_element_type=F32)
        pt = jnp.concatenate([pt[:pt.shape[0] // 2], pt[pt.shape[0] // 2:]], axis=1)
        p_own[...] = pt
        p_send[s] = pt.astype(BF)
        for q in range(3):
            p_copy(i, q).start()

    def phase_d(i):
        l = layer_of(i)
        s = lax.rem(i, 2)

        def z_tile(t, carry):
            u_copy(i, n_tile + t).wait_recv()
            cols = pl.ds(pl.multiple_of(t * 256, 256), 256)
            z = (u_own[s, 1, :, cols] + u_recv[i, n_tile + t].astype(F32)).astype(BF).astype(F32)
            z_buf[:, cols] = z * jax.nn.sigmoid(z)
            return carry

        lax.fori_loop(0, n_tile, z_tile, 0, unroll=True)
        for q in range(3):
            p_copy(i, q).wait_recv()
        pt = p_own[...]
        for q in range(3):
            pt = pt + p_recv[i, q].astype(F32)
        pt = jnp.concatenate([pt, pltpu.roll(pt, blk, 1)], axis=0)

        def unit(v):
            return v * lax.rsqrt(jnp.mean(v * v, axis=0, keepdims=True) + INNER_EPS)

        low_buf[...] = jnp.transpose(unit(pt[:n_rank]))[:blk].astype(BF)
        bt = unit(pt[n_rank:n_rank + n_state])
        ct = unit(pt[n_rank + n_state:])
        bt_out[i] = bt
        for b in range(blk):
            b_bc[b] = jnp.broadcast_to(bt[:, b:b + 1], (n_state, 128))
            c_bc[b] = jnp.broadcast_to(ct[:, b:b + 1], (n_state, 128))

        @pl.when(i >= 1)
        def _():
            dt_store(i - 1).wait()

        def dt_tile(t, carry):
            cols = pl.ds(pl.multiple_of(t * 256, 256), 256)
            v = jnp.dot(low_buf[...], w_dt[l, :, cols], preferred_element_type=F32)
            v = v + dt_bias[l, :, cols]
            dt = jnp.maximum(v, 0.0) + jnp.log1p(jnp.exp(-jnp.abs(v)))
            dt_buf[:, :, cols] = dt.reshape(blk // 8, 8, 256)
            dtx_buf[:, :, cols] = (dt * x_buf[:, cols].astype(F32)).reshape(blk // 8, 8, 256)
            return carry

        lax.fori_loop(0, e_loc // 256, dt_tile, 0, unroll=True)
        dt_store(i).start()
        ssm_load(i).wait()

        def group(g, carry):
            for j in range(e_loc // 128):
                cols = slice(j * 128, (j + 1) * 128)
                a = a_neg[l, :, cols]
                out = []
                for p in range(2):
                    parts = []
                    for b in range(8):
                        row = g * 16 + p * 8 + b
                        decay = jnp.exp2(jnp.broadcast_to(dt_buf[g * 2 + p, b:b + 1, cols], (n_state, 128)) * a)
                        new = decay * ssm_buf[s, row, :, cols] + jnp.broadcast_to(dtx_buf[g * 2 + p, b:b + 1, cols], (n_state, 128)) * b_bc[row]
                        term = new * c_bc[row]
                        parts.append(term[:8] + term[8:])
                    out.append(fold_rows(parts))
                rws = pl.ds(pl.multiple_of(g * 16, 16), 16)
                y = jnp.concatenate(out, axis=0) + d_skip[l, :, cols] * x_buf[rws, cols].astype(F32)
                g_all[i, rws, cols] = (y * z_buf[rws, cols]).astype(BF)
            return carry

        lax.fori_loop(0, blk // 16, group, 0)

        @pl.when(i < total - n_chunk)
        def _():
            g_copy(i).start()

        @pl.when(i >= total - n_chunk)
        def _():
            g_store(i).start()

            @pl.when(i > total - n_chunk)
            def _():
                o_store(i - 1).wait()

            def o_tile(t, carry):
                cols = pl.ds(pl.multiple_of(t * 256, 256), 256)
                o_buf[:, cols] = jnp.dot(g_all[i, pl.ds(0, blk)], w_out[l, :, cols], preferred_element_type=F32)
                return carry

            lax.fori_loop(0, d_loc // 256, o_tile, 0, unroll=True)
            o_store(i).start()

    def phase_e(i):
        l = layer_of(i)
        g_copy(i).wait_recv()

        def tile(t, carry):
            cols = pl.ds(pl.multiple_of(t * 256, 256), 256)
            cr_send[i, :, cols] = jnp.dot(g_all[i], w_out[l, :, cols], preferred_element_type=F32).astype(BF)
            return carry

        lax.fori_loop(0, d_loc // 256, tile, 0, unroll=True)
        cr_copy(i).start()

    def phase_f(i):
        cr_copy(i).wait_recv()
        xs_send[i] = (cr_send[i].astype(F32) + cr_recv[i].astype(F32)).astype(BF)
        xs_copy(i).start()

    def phase_g(i):
        def add(h):
            rws = pl.ds(part_rows(i, h), blk)
            r_ref[rws, :] = r_ref[rws, :] + (xs_send[i, half_rows(h), :].astype(F32) + xs_recv[i, half_rows(h), :].astype(F32))

        xs_copy(i).wait_recv()
        fw_copy(i).start()
        add(core)
        fw_copy(i).wait_recv()
        add(1 - core)
        phase_a(i + n_chunk)

    for l in range(n_layer):
        for vec, src in ((norm_w, norm_w_in), (conv_b, conv_b_in), (dt_bias, dt_bias_in), (d_skip, d_skip_in)):
            vec[l] = src[l:l + 1, :]
        a_neg[l] = jnp.exp(a_log[l]) * (-LOG2E)
    res_load.wait()

    def first_a(i, carry):
        phase_a(i)
        return carry

    lax.fori_loop(0, n_chunk, first_a, 0)
    w_in_load[0].wait()

    def run(phase, i, stop=total):
        ok = (i >= 0) & (i < stop)

        @pl.when(ok)
        def _():
            phase(i)

    def step(s, carry):
        last = total - n_chunk

        @pl.when((s >= 2) & (s < total))
        def _():
            ssm_load(s).start()

        run(phase_c, s - 1)
        run(phase_f, s - 3, last)

        @pl.when(s == n_chunk)
        def _():
            w_in_load[1].wait()

        run(phase_b, s)

        @pl.when(s == 0)
        def _():
            conv_load(0).start()
            conv_load(1).start()
            ssm_load(0).start()
            ssm_load(1).start()
            w_out_load.start()
            w_in_load[1].start()

        run(phase_d, s - 1)

        @pl.when(s == 2)
        def _():
            w_out_load.wait()

        run(phase_g, s - 3, last)
        run(phase_e, s - 2, last)
        return carry

    lax.fori_loop(0, total + 1, step, 0)

    xi_store(total - 1).wait()
    x_store(total - 1).wait()
    dt_store(total - 1).wait()
    o_store(total - 1).wait()
    for i in range(total - 2, total):
        for k in range(2 * n_tile):
            u_copy(i, k).wait_send()
        for q in range(3):
            p_copy(i, q).wait_send()

    def drain(i, carry):
        st_copy(i).wait_send()
        st_copy(i + n_chunk).wait_send()
        g_copy(i).wait_send()
        cr_copy(i).wait_send()
        xs_copy(i).wait_send()
        fw_copy(i).wait_send()
        g_store(i + total - n_chunk).wait()
        return carry

    lax.fori_loop(0, n_chunk, drain, 0)


def state_kernel(n_carry, blk, ssm_in, dt, x, bt, a_log, conv_in, xi, *refs):
    ssm_out, conv_out, a_neg, b_bc = refs[n_carry:]
    n_state, e_loc = a_log.shape[1:]

    @pl.when(pl.program_id(0) == 0)
    def _():
        a_neg[...] = jnp.exp(a_log[0]) * (-LOG2E)

    for b in range(blk):
        b_bc[b] = jnp.broadcast_to(bt[0, :, b:b + 1], (n_state, 128))
    conv_out[0, 0] = conv_in[0, 1]
    conv_out[0, 1] = conv_in[0, 2]
    conv_out[0, 2] = xi[0]

    def group(g, carry):
        rws16 = pl.ds(pl.multiple_of(g * 16, 16), 16)
        for j in range(e_loc // 128):
            cols = slice(j * 128, (j + 1) * 128)
            a = a_neg[:, cols]
            x16 = x[0, rws16, cols].astype(F32)
            for p in range(2):
                dt8 = dt[0, g * 2 + p, :, cols]
                dtx = dt8 * x16[p * 8:p * 8 + 8]
                rws = pl.ds(pl.multiple_of(g * 16 + p * 8, 8), 8)
                decay = jnp.exp2(dt8[:, None, :] * a[None])
                ssm_out[0, rws, :, cols] = decay * ssm_in[0, rws, :, cols] + dtx[:, None, :] * b_bc[rws]
        return carry

    lax.fori_loop(0, blk // 16, group, 0)


def state_pass(l, ssm_t, dt, x, bt, a_log_t, conv_t, xi, carried):
    _, half, n_state, e_loc = ssm_t.shape
    blk = half // N_CHUNK

    def rows_spec(*tail):
        return pl.BlockSpec((1, blk) + tail, lambda g: (l, g) + (0,) * len(tail))

    conv_spec = pl.BlockSpec((1, 3, blk, e_loc), lambda g: (l, 0, g, 0))
    in_specs = [rows_spec(n_state, e_loc), pl.BlockSpec((1, blk // 8, 8, e_loc), lambda g: (l, g, 0, 0)), rows_spec(e_loc),
                pl.BlockSpec((1, n_state, 128), lambda g: (l * N_CHUNK + g, 0, 0)),
                pl.BlockSpec((1, n_state, e_loc), lambda g: (l, 0, 0)), conv_spec, rows_spec(e_loc)]
    in_specs += [pl.BlockSpec(memory_space=pl.ANY)] * len(carried)
    n_elem = half * n_state * e_loc
    return pl.pallas_call(
        functools.partial(state_kernel, len(carried), blk),
        grid=(half // blk,),
        out_shape=(jax.ShapeDtypeStruct(ssm_t.shape, F32), jax.ShapeDtypeStruct(conv_t.shape, BF)),
        in_specs=in_specs,
        out_specs=(rows_spec(n_state, e_loc), conv_spec),
        scratch_shapes=[pltpu.VMEM((n_state, e_loc), F32), pltpu.VMEM((blk, n_state, 128), F32)],
        input_output_aliases={7 + k: k for k in range(len(carried))},
        compiler_params=pltpu.CompilerParams(vmem_limit_bytes=67043328),
        cost_estimate=pl.CostEstimate(flops=n_elem * 1000, bytes_accessed=n_elem * 8, transcendentals=n_elem),
    )(ssm_t, dt, x, bt, a_log_t, conv_t, xi, *carried)


def out_kernel(g_ref, w_ref, o_ref):
    def tile(t, carry):
        cols = pl.ds(pl.multiple_of(t * 256, 256), 256)
        o_ref[:, cols] = jnp.dot(g_ref[...], w_ref[0, :, cols], preferred_element_type=F32)
        return carry

    lax.fori_loop(0, w_ref.shape[2] // 256, tile, 0)


def out_proj(g, w_out, l):
    return pl.pallas_call(
        out_kernel,
        grid=(1,),
        out_shape=jax.ShapeDtypeStruct((g.shape[0], w_out.shape[2]), F32),
        in_specs=[pl.BlockSpec(g.shape, lambda q: (0, 0)), pl.BlockSpec((1,) + w_out.shape[1:], lambda q: (l, 0, 0))],
        out_specs=pl.BlockSpec((g.shape[0], w_out.shape[2]), lambda q: (0, 0)),
        compiler_params=pltpu.CompilerParams(vmem_limit_bytes=67043328),
        name="out_proj",
    )(g, w_out)


def solution(mesh):
    def local_step(residual, norm_w, w_in, conv_w, conv_b, w_x, w_dt, dt_bias, a_log, d_skip, w_out, conv_state, ssm_state):
        n_layer = norm_w.shape[0]
        rows, d_loc = residual.shape
        e_loc = w_x.shape[1]
        n_state = a_log.shape[-1]
        n_rank = w_dt.shape[1]
        n_proj = w_x.shape[2]
        d_model = d_loc * mesh.shape["tx"]
        total = n_layer * N_CHUNK
        blk = rows // 2 // N_CHUNK
        dims = (n_layer, rows, d_loc, e_loc, n_state, n_rank, d_model)
        conv_t = jnp.transpose(conv_state, (0, 3, 1, 2))
        ssm_t = jnp.transpose(ssm_state, (0, 1, 3, 2))
        a_log_t = jnp.transpose(a_log, (0, 2, 1))
        args = (residual, norm_w, w_in, jnp.transpose(conv_w, (0, 2, 1)), conv_b, jnp.transpose(w_x, (0, 2, 1)), w_dt, dt_bias, a_log_t, d_skip, w_out, conv_t, ssm_t)
        hbm = pl.BlockSpec(memory_space=pl.ANY)
        vmem = pl.BlockSpec(memory_space=pltpu.VMEM)
        in_specs = [hbm, vmem, hbm, vmem, vmem, vmem, vmem, vmem, vmem, vmem, hbm, hbm, hbm]
        dma = pltpu.SemaphoreType.DMA
        scratch = [pltpu.VMEM((n_layer, 1, d_loc), F32)] + [pltpu.VMEM((n_layer, 1, e_loc), F32)] * 3 + [
            pltpu.VMEM((n_layer, d_loc, 2, e_loc), BF),
            pltpu.VMEM((n_layer, e_loc, d_loc), BF),
            pltpu.VMEM((n_layer, n_state, e_loc), F32),
            pltpu.VMEM((2, blk, n_state, e_loc), F32),
            pltpu.VMEM((2, 4, blk, e_loc), BF),
            pltpu.VMEM((2 * blk, d_loc), BF),
            pltpu.VMEM((2, 2, blk, e_loc), F32),
            pltpu.VMEM((blk, e_loc), F32),
            pltpu.VMEM((blk, e_loc), BF),
            pltpu.VMEM((blk, n_rank), BF),
            pltpu.VMEM((blk // 8, 8, e_loc), F32),
            pltpu.VMEM((blk // 8, 8, e_loc), F32),
            pltpu.VMEM((blk, n_state, 128), F32),
            pltpu.VMEM((blk, n_state, 128), F32),
            pltpu.VMEM((blk, d_loc), F32),
            pltpu.VMEM((4 * blk, 2 * d_loc), BF),
            pltpu.VMEM((total, 8, 2 * blk), F32),
            pltpu.VMEM((total, 8, 2 * blk), F32),
            pltpu.VMEM((2, 2 * (e_loc // 256), blk, 256), BF),
            pltpu.VMEM((total, 2 * (e_loc // 256), blk, 256), BF),
            pltpu.VMEM((n_proj // 2, 2 * blk), F32),
            pltpu.VMEM((2, n_proj // 2, 2 * blk), BF),
            pltpu.VMEM((total, 3, n_proj // 2, 2 * blk), BF),
            pltpu.VMEM((total, 2 * blk, e_loc), BF),
        ] + [pltpu.VMEM((N_CHUNK, 2 * blk, d_loc), BF)] * 4 + [
            dma((2 + n_layer,)), dma((2,)), dma((2,)), dma(()), dma(()), dma((2,)), dma((N_CHUNK,)), dma(()),
            dma((total,)), dma((total,)), dma((2, 2 * (e_loc // 256))), dma((total, 2 * (e_loc // 256))), dma((2, 3)), dma((total, 3)),
            dma((total,)), dma((total,)), dma((N_CHUNK,)), dma((N_CHUNK,)), dma((N_CHUNK,)), dma((N_CHUNK,)), dma((N_CHUNK,)), dma((N_CHUNK,)),
        ]
        half = rows // 2
        r_mid, bt, g_own, o_own, dt, x_act, xi = pl.pallas_call(
            functools.partial(step_kernel, dims),
            out_shape=(jax.ShapeDtypeStruct((rows, d_loc), F32), jax.ShapeDtypeStruct((total, n_state, 128), F32), jax.ShapeDtypeStruct((half, e_loc), BF), jax.ShapeDtypeStruct((half, d_loc), F32),
                       jax.ShapeDtypeStruct((n_layer, half // 8, 8, e_loc), F32), jax.ShapeDtypeStruct((n_layer, half, e_loc), BF), jax.ShapeDtypeStruct((n_layer, half, e_loc), BF)),
            in_specs=in_specs,
            out_specs=(vmem, vmem, hbm, hbm, hbm, hbm, hbm),
            scratch_shapes=scratch,
            compiler_params=pltpu.CompilerParams(collective_id=0, has_side_effects=True, vmem_limit_bytes=67043328),
            name="mamba_step",
        )(*args)

        core = lax.rem(lax.axis_index("ty"), 2)
        tx = lax.axis_index("tx")
        core_swap = [(0, 1), (1, 0), (2, 3), (3, 2)]
        g_peer = lax.ppermute(g_own, "tx", [(0, 1), (1, 0)])
        caches = state_pass(0, ssm_t, dt, x_act, bt, a_log_t, conv_t, xi, ())
        o_peer = out_proj(g_peer, w_out, n_layer - 1)
        kept = jnp.where(core == 0, o_own, o_peer)
        sent = jnp.where(core == 0, o_peer, o_own).astype(BF)
        part = (kept + lax.ppermute(sent, "ty", core_swap).astype(F32)).astype(BF)
        other = lax.ppermute(part, "ty", [(0, 2), (2, 0), (1, 3), (3, 1)])
        caches = state_pass(1, ssm_t, dt, x_act, bt, a_log_t, conv_t, xi, caches)
        tot = (part.astype(F32) + other.astype(F32)).astype(BF)
        tot_peer = lax.ppermute(tot, "ty", core_swap)
        first = jnp.where(core == tx, tot, tot_peer)
        second = jnp.where(core == tx, tot_peer, tot)
        r_out = r_mid + jnp.concatenate([first, second], axis=0).astype(F32)
        return r_out, jnp.transpose(caches[1], (0, 2, 3, 1)), jnp.transpose(caches[0], (0, 1, 3, 2))

    cache_spec = P(None, ("dp", "tx"), "ty", None)
    in_specs = (P("dp", "tx"), P(None, "tx"), P(None, "tx", None, "ty"), P(None, "ty", None), P(None, "ty"), P(None, "ty", None), P(None, None, "ty"), P(None, "ty"), P(None, "ty", None), P(None, "ty"), P(None, "ty", "tx"), cache_spec, cache_spec)
    out_specs = (P("dp", "tx"), cache_spec, cache_spec)
    return jax.shard_map(local_step, mesh=mesh, in_specs=in_specs, out_specs=out_specs, check_vma=False)
```

```python
import functools
import jax
import jax.numpy as jnp
from jax import lax
from jax.experimental import pallas as pl
from jax.experimental.pallas import tpu as pltpu
from jax.sharding import PartitionSpec as P


NORM_EPS = 1e-5
INNER_EPS = 1e-6
LOG2E = 1.4426950408889634
N_CHUNK = 4
U_PARTS = ((0, 3), (3, 5), (5, 10))
BF = jnp.bfloat16
F32 = jnp.float32
MESH = pl.DeviceIdType.MESH


def fold_rows(parts):
    sub = lax.broadcasted_iota(jnp.int32, (8, 128), 0)

    def pair(a, b, shift):
        low = (sub & shift) == 0
        p = jnp.where(low, a, b)
        q = jnp.where(low, b, a)
        if shift == 4:
            return p + pltpu.roll(q, 4, 0)
        return p + jnp.where(low, pltpu.roll(q, 8 - shift, 0), pltpu.roll(q, shift, 0))

    for shift in (4, 2, 1):
        parts = [pair(parts[b], parts[b + shift], shift) for b in range(shift)]
    return parts[0]


def step_kernel(dims, res_hbm, norm_w_in, w_in_hbm, conv_w, conv_b_in, w_x_hbm, w_dt_hbm, dt_bias_in, a_log, d_skip_in, w_out_hbm, conv_hbm, ssm_hbm,
                r_out, bt_out, g_out, o_out, dt_out, x_out, xi_out,
                r_ref, w_x, w_dt, norm_w, conv_b, dt_bias, d_skip, w_in, w_out, a_neg, ssm_buf, conv_buf, h_buf, u_own, z_buf, x_buf, low_buf, dt_buf, dtx_buf, b_bc, c_bc, o_buf, hx_buf,
                st_send, st_recv, u_send, u_recv, p_own, p_send, p_recv, g_all, cr_send, cr_recv, xs_send, xs_recv,
                in_sem, ssm_in_sem, conv_in_sem, dt_sem, x_sem, xi_sem, go_sem, o_sem,
                st_s, st_r, u_s, u_r, p_s, p_r, g_s, g_r, cr_s, cr_r, xs_s, xs_r, fw_s, fw_r):
    n_layer, rows, d_loc, e_loc, n_state, n_rank, d_model = dims
    half = rows // 2
    n_chunk = N_CHUNK
    blk = half // n_chunk
    total = n_layer * n_chunk
    n_tile = e_loc // 256
    tx = lax.axis_index("tx")
    ty = lax.axis_index("ty")
    core = lax.rem(ty, 2)
    chip = lax.div(ty, 2)
    y_peer = {"tx": 1 - tx, "ty": ty}
    core_peer = {"tx": tx, "ty": chip * 2 + (1 - core)}
    x_peer = {"tx": tx, "ty": (1 - chip) * 2 + core}
    d_peer = {"tx": tx, "ty": (1 - chip) * 2 + (1 - core)}
    st_peer = {"tx": 1 - tx, "ty": (1 - chip) * 2 + core}

    def layer_of(i):
        return lax.div(i, n_chunk)

    def chunk_of(i):
        return lax.rem(i, n_chunk)

    def part_rows(i, part):
        side = jnp.where(part == 0, tx, 1 - tx)
        return pl.multiple_of(side * half + chunk_of(i) * blk, blk)

    def remote(src, dst, s_sem, r_sem, dev):
        return pltpu.make_async_remote_copy(src_ref=src, dst_ref=dst, send_sem=s_sem, recv_sem=r_sem, device_id=dev, device_id_type=MESH)

    def st_copy(i):
        return remote(st_send.at[i], st_recv.at[i], st_s.at[i], st_r.at[i], st_peer)

    def u_copy(i, k):
        s = lax.rem(i, 2)
        part = pl.ds(U_PARTS[k][0], U_PARTS[k][1] - U_PARTS[k][0])
        return remote(u_send.at[s, part], u_recv.at[i, part], u_s.at[s, k], u_r.at[i, k], y_peer)

    def p_copy(i, q):
        s = lax.rem(i, 2)
        dev = (core_peer, x_peer, d_peer)[q]
        return remote(p_send.at[s], p_recv.at[i, q], p_s.at[s, q], p_r.at[i, q], dev)

    def g_copy(i):
        return remote(g_all.at[i, pl.ds(0, blk)], g_all.at[i, pl.ds(blk, blk)], g_s.at[i], g_r.at[i], y_peer)

    def cr_copy(i):
        return remote(cr_send.at[i], cr_recv.at[i], cr_s.at[i], cr_r.at[i], core_peer)

    def half_rows(h):
        return pl.ds(pl.multiple_of(h * blk, blk), blk)

    def xs_copy(i):
        return remote(xs_send.at[i, half_rows(core)], xs_recv.at[i, half_rows(core)], xs_s.at[i], xs_r.at[i], x_peer)

    def fw_copy(i):
        return remote(xs_recv.at[i, half_rows(core)], xs_recv.at[i, half_rows(core)], fw_s.at[i], fw_r.at[i], core_peer)

    def cache_rows(i):
        return pl.ds(pl.multiple_of(chunk_of(i) * blk, blk), blk)

    def ssm_load(i):
        s = lax.rem(i, 2)
        return pltpu.make_async_copy(ssm_hbm.at[layer_of(i), cache_rows(i)], ssm_buf.at[s], ssm_in_sem.at[s])

    def conv_load(i):
        s = lax.rem(i, 2)
        return pltpu.make_async_copy(conv_hbm.at[layer_of(i), :, cache_rows(i)], conv_buf.at[s, pl.ds(0, 3)], conv_in_sem.at[s])

    def dt_store(i):
        n = blk // 8
        return pltpu.make_async_copy(dt_buf, dt_out.at[layer_of(i), pl.ds(chunk_of(i) * n, n)], dt_sem)

    def x_store(i):
        return pltpu.make_async_copy(x_buf, x_out.at[layer_of(i), cache_rows(i)], x_sem)

    def xi_store(i):
        s = lax.rem(i, 2)
        return pltpu.make_async_copy(conv_buf.at[s, 3], xi_out.at[layer_of(i), cache_rows(i)], xi_sem.at[s])

    def o_store(i):
        return pltpu.make_async_copy(o_buf, o_out.at[cache_rows(i)], o_sem)

    def g_store(i):
        return pltpu.make_async_copy(g_all.at[i, pl.ds(0, blk)], g_out.at[cache_rows(i)], go_sem.at[chunk_of(i)])

    res_load = pltpu.make_async_copy(res_hbm, r_ref, in_sem.at[0])
    w_in_load = [pltpu.make_async_copy(w_in_hbm.at[l], w_in.at[l], in_sem.at[1 + l]) for l in range(n_layer)]
    w_out_load = pltpu.make_async_copy(w_out_hbm, w_out, in_sem.at[1 + n_layer])
    w_x_load = pltpu.make_async_copy(w_x_hbm, w_x, in_sem.at[2 + n_layer])
    w_dt_load = pltpu.make_async_copy(w_dt_hbm, w_dt, in_sem.at[3 + n_layer])
    r_store = pltpu.make_async_copy(r_ref, r_out, in_sem.at[4 + n_layer])

    res_load.start()
    w_in_load[0].start()

    barrier = pltpu.get_barrier_semaphore()
    for dev in (y_peer, core_peer, x_peer, d_peer, st_peer):
        pl.semaphore_signal(barrier, inc=1, device_id=dev, device_id_type=MESH)
    pl.semaphore_wait(barrier, 5)

    def eye():
        n = 2 * blk
        return lax.broadcasted_iota(jnp.int32, (n, n), 0) == lax.broadcasted_iota(jnp.int32, (n, n), 1)

    def phase_a(i):
        sums = []
        for part in range(2):
            val = r_ref[pl.ds(part_rows(i, part), blk), :]
            sums.append(jnp.sum(val * val, axis=1, keepdims=True))
        col = jnp.concatenate(sums, axis=0)
        row = jnp.sum(jnp.where(eye(), col, 0.0), axis=0, keepdims=True)
        st_send[i] = jnp.broadcast_to(row, (8, 2 * blk))
        st_copy(i).start()

    def phase_b(i):
        l = layer_of(i)
        s = lax.rem(i, 2)
        st_copy(i).wait_recv()
        sq = st_send[i] + pltpu.roll(st_recv[i], blk, 1)
        inv = lax.rsqrt(sq / d_model + NORM_EPS)
        col = jnp.sum(jnp.where(eye(), jnp.broadcast_to(inv[0:1], (2 * blk, 2 * blk)), 0.0), axis=1, keepdims=True)
        nw = norm_w[l]
        for part in range(2):
            base = part_rows(i, part)
            for q in range(blk // 16):
                lo = part * blk + q * 16
                val = r_ref[pl.ds(base + q * 16, 16), :]
                h_buf[lo:lo + 16, :] = (val * col[lo:lo + 16] * nw).astype(BF)

        src = lax.broadcasted_iota(jnp.int32, (128, 256), 0)
        dst = lax.broadcasted_iota(jnp.int32, (128, 256), 1)
        for k in range(2):
            spread = jnp.where(dst == 2 * src + k, 1.0, 0.0).astype(BF)
            for t in range(d_loc // 128):
                wide = jnp.dot(h_buf[:, t * 128:(t + 1) * 128], spread, preferred_element_type=F32)
                hx_buf[k * 2 * blk:(k + 1) * 2 * blk, t * 256:(t + 1) * 256] = wide.astype(BF)

        @pl.when(i >= 2)
        def _():
            for k in range(len(U_PARTS)):
                u_copy(i - 2, k).wait_send()

        w_rows = w_in.at[l].reshape(2 * d_loc, e_loc)

        for t in range(n_tile):
            cols = slice(t * 256, (t + 1) * 256)
            u = jnp.dot(hx_buf[...], w_rows[:, cols], preferred_element_type=F32)
            for k in range(2):
                u_own[s, k, :, cols] = u[2 * k * blk:(2 * k + 1) * blk]
                u_send[s, k * n_tile + t] = u[(2 * k + 1) * blk:(2 * k + 2) * blk].astype(BF)
            for k, (lo, hi) in enumerate(U_PARTS):
                if (hi - 1 if hi <= n_tile else n_tile - 1) == t:
                    u_copy(i, k).start()

    def phase_c(i):
        l = layer_of(i)
        s = lax.rem(i, 2)

        @pl.when(i >= 1)
        def _():
            xi_store(i - 1).wait()
            x_store(i - 1).wait()

            @pl.when(i + 1 < total)
            def _():
                conv_load(i + 1).start()

        conv_load(i).wait()

        for t in range(n_tile):
            for k, (lo, hi) in enumerate(U_PARTS):
                if lo == t:
                    u_copy(i, k).wait_recv()
            cols = slice(t * 256, (t + 1) * 256)
            xi = (u_own[s, 0, :, cols] + u_recv[i, t].astype(F32)).astype(BF)
            conv_buf[s, 3, :, cols] = xi
            acc = conv_buf[s, 0, :, cols].astype(F32) * conv_w[l, 0:1, cols]
            acc = acc + conv_buf[s, 1, :, cols].astype(F32) * conv_w[l, 1:2, cols]
            acc = acc + conv_buf[s, 2, :, cols].astype(F32) * conv_w[l, 2:3, cols]
            acc = acc + xi.astype(F32) * conv_w[l, 3:4, cols]
            acc = acc + conv_b[l, :, cols]
            x_buf[:, cols] = (acc * jax.nn.sigmoid(acc)).astype(BF)
        xi_store(i).start()
        x_store(i).start()

        @pl.when(i >= 2)
        def _():
            for q in range(3):
                p_copy(i - 2, q).wait_send()

        pt = lax.dot_general(w_x[l], x_buf[...], (((1,), (1,)), ((), ())), preferred_element_type=F32)
        pt = jnp.concatenate([pt[:pt.shape[0] // 2], pt[pt.shape[0] // 2:]], axis=1)
        p_own[...] = pt
        p_send[s] = pt.astype(BF)
        for q in range(3):
            p_copy(i, q).start()

    def phase_d(i):
        l = layer_of(i)
        s = lax.rem(i, 2)

        for t in range(n_tile):
            for k, (lo, hi) in enumerate(U_PARTS):
                if lo == n_tile + t:
                    u_copy(i, k).wait_recv()
            cols = slice(t * 256, (t + 1) * 256)
            z = (u_own[s, 1, :, cols] + u_recv[i, n_tile + t].astype(F32)).astype(BF).astype(F32)
            z_buf[:, cols] = z * jax.nn.sigmoid(z)
        for q in range(3):
            p_copy(i, q).wait_recv()
        pt = p_own[...]
        for q in range(3):
            pt = pt + p_recv[i, q].astype(F32)
        pt = jnp.concatenate([pt, pltpu.roll(pt, blk, 1)], axis=0)

        def unit(v):
            return v * lax.rsqrt(jnp.mean(v * v, axis=0, keepdims=True) + INNER_EPS)

        low_buf[...] = jnp.transpose(unit(pt[:n_rank]))[:blk].astype(BF)
        bt = unit(pt[n_rank:n_rank + n_state])
        ct = unit(pt[n_rank + n_state:])
        bt_out[i] = bt
        for b in range(blk):
            b_bc[b] = jnp.broadcast_to(bt[:, b:b + 1], (n_state, 128))
            c_bc[b] = jnp.broadcast_to(ct[:, b:b + 1], (n_state, 128))

        @pl.when(i >= 1)
        def _():
            dt_store(i - 1).wait()

        def dt_tile(t, carry):
            cols = pl.ds(pl.multiple_of(t * 256, 256), 256)
            v = jnp.dot(low_buf[...], w_dt[l, :, cols], preferred_element_type=F32)
            v = v + dt_bias[l, :, cols]
            dt = jnp.maximum(v, 0.0) + jnp.log1p(jnp.exp(-jnp.abs(v)))
            dt_buf[:, :, cols] = dt.reshape(blk // 8, 8, 256)
            dtx_buf[:, :, cols] = (dt * x_buf[:, cols].astype(F32)).reshape(blk // 8, 8, 256)
            return carry

        lax.fori_loop(0, e_loc // 256, dt_tile, 0, unroll=True)
        dt_store(i).start()
        ssm_load(i).wait()

        def group(g, carry):
            for j in range(e_loc // 128):
                cols = slice(j * 128, (j + 1) * 128)
                a = a_neg[l, :, cols]
                out = []
                for p in range(2):
                    parts = []
                    for b in range(8):
                        row = g * 16 + p * 8 + b
                        decay = jnp.exp2(jnp.broadcast_to(dt_buf[g * 2 + p, b:b + 1, cols], (n_state, 128)) * a)
                        new = decay * ssm_buf[s, row, :, cols] + jnp.broadcast_to(dtx_buf[g * 2 + p, b:b + 1, cols], (n_state, 128)) * b_bc[row]
                        term = new * c_bc[row]
                        parts.append(term[:8] + term[8:])
                    out.append(fold_rows(parts))
                rws = pl.ds(pl.multiple_of(g * 16, 16), 16)
                y = jnp.concatenate(out, axis=0) + d_skip[l, :, cols] * x_buf[rws, cols].astype(F32)
                g_all[i, rws, cols] = (y * z_buf[rws, cols]).astype(BF)
            return carry

        lax.fori_loop(0, blk // 16, group, 0)

        @pl.when(i < total - n_chunk)
        def _():
            g_copy(i).start()

        @pl.when(i >= total - n_chunk)
        def _():
            g_store(i).start()

            @pl.when(i > total - n_chunk)
            def _():
                o_store(i - 1).wait()

            def o_tile(t, carry):
                cols = pl.ds(pl.multiple_of(t * 256, 256), 256)
                o_buf[:, cols] = jnp.dot(g_all[i, pl.ds(0, blk)], w_out[l, :, cols], preferred_element_type=F32)
                return carry

            lax.fori_loop(0, d_loc // 256, o_tile, 0, unroll=True)
            o_store(i).start()

    def phase_e(i):
        l = layer_of(i)
        g_copy(i).wait_recv()

        def tile(t, carry):
            cols = pl.ds(pl.multiple_of(t * 256, 256), 256)
            cr_send[i, :, cols] = jnp.dot(g_all[i], w_out[l, :, cols], preferred_element_type=F32).astype(BF)
            return carry

        lax.fori_loop(0, d_loc // 256, tile, 0, unroll=True)
        cr_copy(i).start()

    def phase_f(i):
        cr_copy(i).wait_recv()
        xs_send[i] = (cr_send[i].astype(F32) + cr_recv[i].astype(F32)).astype(BF)
        xs_copy(i).start()

    def phase_g(i):
        def add(h):
            rws = pl.ds(part_rows(i, h), blk)
            r_ref[rws, :] = r_ref[rws, :] + (xs_send[i, half_rows(h), :].astype(F32) + xs_recv[i, half_rows(h), :].astype(F32))

        xs_copy(i).wait_recv()
        fw_copy(i).start()
        add(core)
        fw_copy(i).wait_recv()
        add(1 - core)
        phase_a(i + n_chunk)

    for l in range(n_layer):
        for vec, src in ((norm_w, norm_w_in), (conv_b, conv_b_in), (dt_bias, dt_bias_in), (d_skip, d_skip_in)):
            vec[l] = src[l:l + 1, :]
        a_neg[l] = jnp.exp(a_log[l]) * (-LOG2E)
    res_load.wait()

    def first_a(i, carry):
        phase_a(i)
        return carry

    lax.fori_loop(0, n_chunk, first_a, 0)
    w_in_load[0].wait()

    def run(phase, i, stop=total):
        ok = (i >= 0) & (i < stop)

        @pl.when(ok)
        def _():
            phase(i)

    def step(s, carry):
        last = total - n_chunk

        @pl.when((s >= 2) & (s < total))
        def _():
            ssm_load(s).start()

        @pl.when(s == 1)
        def _():
            w_x_load.wait()
            w_dt_load.wait()

        run(phase_c, s - 1)
        run(phase_f, s - 3, last)

        @pl.when(s == n_chunk)
        def _():
            w_in_load[1].wait()

        run(phase_b, s)

        @pl.when(s == 0)
        def _():
            conv_load(0).start()
            w_x_load.start()
            w_dt_load.start()
            conv_load(1).start()
            ssm_load(0).start()
            ssm_load(1).start()
            w_out_load.start()
            w_in_load[1].start()

        run(phase_d, s - 1)
        run(phase_g, s - 3, last)

        @pl.when(s == n_chunk + 2)
        def _():
            r_store.start()

        @pl.when(s == 2)
        def _():
            w_out_load.wait()

        run(phase_e, s - 2, last)
        return carry

    lax.fori_loop(0, total + 1, step, 0)

    r_store.wait()
    xi_store(total - 1).wait()
    x_store(total - 1).wait()
    dt_store(total - 1).wait()
    o_store(total - 1).wait()
    for i in range(total - 2, total):
        for k in range(len(U_PARTS)):
            u_copy(i, k).wait_send()
        for q in range(3):
            p_copy(i, q).wait_send()

    def drain(i, carry):
        st_copy(i).wait_send()
        st_copy(i + n_chunk).wait_send()
        g_copy(i).wait_send()
        cr_copy(i).wait_send()
        xs_copy(i).wait_send()
        fw_copy(i).wait_send()
        g_store(i + total - n_chunk).wait()
        return carry

    lax.fori_loop(0, n_chunk, drain, 0)


def state_kernel(n_carry, blk, ssm_in, dt, x, bt, a_log, conv_in, xi, *refs):
    ssm_out, conv_out, a_neg, b_bc = refs[n_carry:]
    n_state, e_loc = a_log.shape[1:]

    @pl.when(pl.program_id(0) == 0)
    def _():
        a_neg[...] = jnp.exp(a_log[0]) * (-LOG2E)

    for b in range(blk):
        b_bc[b] = jnp.broadcast_to(bt[0, :, b:b + 1], (n_state, 128))
    conv_out[0, 0] = conv_in[0, 1]
    conv_out[0, 1] = conv_in[0, 2]
    conv_out[0, 2] = xi[0]

    def group(g, carry):
        rws16 = pl.ds(pl.multiple_of(g * 16, 16), 16)
        for j in range(e_loc // 128):
            cols = slice(j * 128, (j + 1) * 128)
            a = a_neg[:, cols]
            x16 = x[0, rws16, cols].astype(F32)
            for p in range(2):
                dt8 = dt[0, g * 2 + p, :, cols]
                dtx = dt8 * x16[p * 8:p * 8 + 8]
                rws = pl.ds(pl.multiple_of(g * 16 + p * 8, 8), 8)
                decay = jnp.exp2(dt8[:, None, :] * a[None])
                ssm_out[0, rws, :, cols] = decay * ssm_in[0, rws, :, cols] + dtx[:, None, :] * b_bc[rws]
        return carry

    lax.fori_loop(0, blk // 16, group, 0)


def state_pass(l, ssm_t, dt, x, bt, a_log_t, conv_t, xi, carried):
    _, half, n_state, e_loc = ssm_t.shape
    blk = half // N_CHUNK

    def rows_spec(*tail):
        return pl.BlockSpec((1, blk) + tail, lambda g: (l, g) + (0,) * len(tail))

    conv_spec = pl.BlockSpec((1, 3, blk, e_loc), lambda g: (l, 0, g, 0))
    in_specs = [rows_spec(n_state, e_loc), pl.BlockSpec((1, blk // 8, 8, e_loc), lambda g: (l, g, 0, 0)), rows_spec(e_loc),
                pl.BlockSpec((1, n_state, 128), lambda g: (l * N_CHUNK + g, 0, 0)),
                pl.BlockSpec((1, n_state, e_loc), lambda g: (l, 0, 0)), conv_spec, rows_spec(e_loc)]
    in_specs += [pl.BlockSpec(memory_space=pl.ANY)] * len(carried)
    n_elem = half * n_state * e_loc
    return pl.pallas_call(
        functools.partial(state_kernel, len(carried), blk),
        grid=(half // blk,),
        out_shape=(jax.ShapeDtypeStruct(ssm_t.shape, F32), jax.ShapeDtypeStruct(conv_t.shape, BF)),
        in_specs=in_specs,
        out_specs=(rows_spec(n_state, e_loc), conv_spec),
        scratch_shapes=[pltpu.VMEM((n_state, e_loc), F32), pltpu.VMEM((blk, n_state, 128), F32)],
        input_output_aliases={7 + k: k for k in range(len(carried))},
        compiler_params=pltpu.CompilerParams(vmem_limit_bytes=67043328),
        cost_estimate=pl.CostEstimate(flops=n_elem * 1000, bytes_accessed=n_elem * 8, transcendentals=n_elem),
    )(ssm_t, dt, x, bt, a_log_t, conv_t, xi, *carried)


def out_kernel(l, g_ref, w_hbm, own_ref, kept_ref, sent_ref, w_buf, sem):
    first = lax.rem(lax.axis_index("ty"), 2) == 0
    n_tile = own_ref.shape[1] // 256
    loads = [pltpu.make_async_copy(w_hbm.at[l, :, pl.ds(t * 256, 256)], w_buf.at[t], sem.at[t]) for t in range(n_tile)]
    for load in loads:
        load.start()
    for t in range(n_tile):
        loads[t].wait()
        cols = slice(t * 256, (t + 1) * 256)
        peer = jnp.dot(g_ref[...], w_buf[t], preferred_element_type=F32)
        own = own_ref[:, cols]
        kept_ref[:, cols] = jnp.where(first, own, peer)
        sent_ref[:, cols] = jnp.where(first, peer, own).astype(BF)


def out_proj(g, w_out, own, l):
    vmem = pl.BlockSpec(memory_space=pltpu.VMEM)
    n_tile = own.shape[1] // 256
    return pl.pallas_call(
        functools.partial(out_kernel, l),
        out_shape=(jax.ShapeDtypeStruct(own.shape, F32), jax.ShapeDtypeStruct(own.shape, BF)),
        in_specs=[vmem, pl.BlockSpec(memory_space=pl.ANY), vmem],
        out_specs=(vmem, vmem),
        scratch_shapes=[pltpu.VMEM((n_tile, w_out.shape[1], 256), BF), pltpu.SemaphoreType.DMA((n_tile,))],
        compiler_params=pltpu.CompilerParams(vmem_limit_bytes=67043328),
        name="out_proj",
    )(g, w_out, own)


def solution(mesh):
    def local_step(residual, norm_w, w_in, conv_w, conv_b, w_x, w_dt, dt_bias, a_log, d_skip, w_out, conv_state, ssm_state):
        n_layer = norm_w.shape[0]
        rows, d_loc = residual.shape
        e_loc = w_x.shape[1]
        n_state = a_log.shape[-1]
        n_rank = w_dt.shape[1]
        n_proj = w_x.shape[2]
        d_model = d_loc * mesh.shape["tx"]
        total = n_layer * N_CHUNK
        blk = rows // 2 // N_CHUNK
        dims = (n_layer, rows, d_loc, e_loc, n_state, n_rank, d_model)
        conv_t = jnp.transpose(conv_state, (0, 3, 1, 2))
        ssm_t = jnp.transpose(ssm_state, (0, 1, 3, 2))
        a_log_t = jnp.transpose(a_log, (0, 2, 1))
        args = (residual, norm_w, w_in, jnp.transpose(conv_w, (0, 2, 1)), conv_b, jnp.transpose(w_x, (0, 2, 1)), w_dt, dt_bias, a_log_t, d_skip, w_out, conv_t, ssm_t)
        hbm = pl.BlockSpec(memory_space=pl.ANY)
        vmem = pl.BlockSpec(memory_space=pltpu.VMEM)
        in_specs = [hbm, vmem, hbm, vmem, vmem, hbm, hbm, vmem, vmem, vmem, hbm, hbm, hbm]
        dma = pltpu.SemaphoreType.DMA
        scratch = [pltpu.VMEM((rows, d_loc), F32), pltpu.VMEM((n_layer, n_proj, e_loc), BF), pltpu.VMEM((n_layer, n_rank, e_loc), BF), pltpu.VMEM((n_layer, 1, d_loc), F32)] + [pltpu.VMEM((n_layer, 1, e_loc), F32)] * 3 + [
            pltpu.VMEM((n_layer, d_loc, 2, e_loc), BF),
            pltpu.VMEM((n_layer, e_loc, d_loc), BF),
            pltpu.VMEM((n_layer, n_state, e_loc), F32),
            pltpu.VMEM((2, blk, n_state, e_loc), F32),
            pltpu.VMEM((2, 4, blk, e_loc), BF),
            pltpu.VMEM((2 * blk, d_loc), BF),
            pltpu.VMEM((2, 2, blk, e_loc), F32),
            pltpu.VMEM((blk, e_loc), F32),
            pltpu.VMEM((blk, e_loc), BF),
            pltpu.VMEM((blk, n_rank), BF),
            pltpu.VMEM((blk // 8, 8, e_loc), F32),
            pltpu.VMEM((blk // 8, 8, e_loc), F32),
            pltpu.VMEM((blk, n_state, 128), F32),
            pltpu.VMEM((blk, n_state, 128), F32),
            pltpu.VMEM((blk, d_loc), F32),
            pltpu.VMEM((4 * blk, 2 * d_loc), BF),
            pltpu.VMEM((total, 8, 2 * blk), F32),
            pltpu.VMEM((total, 8, 2 * blk), F32),
            pltpu.VMEM((2, 2 * (e_loc // 256), blk, 256), BF),
            pltpu.VMEM((total, 2 * (e_loc // 256), blk, 256), BF),
            pltpu.VMEM((n_proj // 2, 2 * blk), F32),
            pltpu.VMEM((2, n_proj // 2, 2 * blk), BF),
            pltpu.VMEM((total, 3, n_proj // 2, 2 * blk), BF),
            pltpu.VMEM((total, 2 * blk, e_loc), BF),
        ] + [pltpu.VMEM((N_CHUNK, 2 * blk, d_loc), BF)] * 4 + [
            dma((5 + n_layer,)), dma((2,)), dma((2,)), dma(()), dma(()), dma((2,)), dma((N_CHUNK,)), dma(()),
            dma((total,)), dma((total,)), dma((2, len(U_PARTS))), dma((total, len(U_PARTS))), dma((2, 3)), dma((total, 3)),
            dma((total,)), dma((total,)), dma((N_CHUNK,)), dma((N_CHUNK,)), dma((N_CHUNK,)), dma((N_CHUNK,)), dma((N_CHUNK,)), dma((N_CHUNK,)),
        ]
        half = rows // 2
        r_mid, bt, g_own, o_own, dt, x_act, xi = pl.pallas_call(
            functools.partial(step_kernel, dims),
            out_shape=(jax.ShapeDtypeStruct((rows, d_loc), F32), jax.ShapeDtypeStruct((total, n_state, 128), F32), jax.ShapeDtypeStruct((half, e_loc), BF), jax.ShapeDtypeStruct((half, d_loc), F32),
                       jax.ShapeDtypeStruct((n_layer, half // 8, 8, e_loc), F32), jax.ShapeDtypeStruct((n_layer, half, e_loc), BF), jax.ShapeDtypeStruct((n_layer, half, e_loc), BF)),
            in_specs=in_specs,
            out_specs=(hbm, vmem, hbm, hbm, hbm, hbm, hbm),
            scratch_shapes=scratch,
            compiler_params=pltpu.CompilerParams(collective_id=0, has_side_effects=True, vmem_limit_bytes=67043328),
            name="mamba_step",
        )(*args)

        core = lax.rem(lax.axis_index("ty"), 2)
        tx = lax.axis_index("tx")
        core_swap = [(0, 1), (1, 0), (2, 3), (3, 2)]
        g_peer = lax.ppermute(g_own, "tx", [(0, 1), (1, 0)])
        caches = state_pass(0, ssm_t, dt, x_act, bt, a_log_t, conv_t, xi, ())
        kept, sent = out_proj(g_peer, w_out, o_own, n_layer - 1)
        part = (kept + lax.ppermute(sent, "ty", core_swap).astype(F32)).astype(BF)
        other = lax.ppermute(part, "ty", [(0, 2), (2, 0), (1, 3), (3, 1)])
        part_peer = lax.ppermute(part, "ty", core_swap)
        caches = state_pass(1, ssm_t, dt, x_act, bt, a_log_t, conv_t, xi, caches)
        other_peer = lax.ppermute(other, "ty", core_swap)
        mine = part.astype(F32) + other.astype(F32)
        theirs = part_peer.astype(F32) + other_peer.astype(F32)
        same = core == tx
        r_out = r_mid + jnp.concatenate([jnp.where(same, mine, theirs), jnp.where(same, theirs, mine)], axis=0)
        return r_out, jnp.transpose(caches[1], (0, 2, 3, 1)), jnp.transpose(caches[0], (0, 1, 3, 2))

    cache_spec = P(None, ("dp", "tx"), "ty", None)
    in_specs = (P("dp", "tx"), P(None, "tx"), P(None, "tx", None, "ty"), P(None, "ty", None), P(None, "ty"), P(None, "ty", None), P(None, None, "ty"), P(None, "ty"), P(None, "ty", None), P(None, "ty"), P(None, "ty", "tx"), cache_spec, cache_spec)
    out_specs = (P("dp", "tx"), cache_spec, cache_spec)
    return jax.shard_map(local_step, mesh=mesh, in_specs=in_specs, out_specs=out_specs, check_vma=False)
```

```python
import functools
import jax
import jax.numpy as jnp
from jax import lax
from jax.experimental import pallas as pl
from jax.experimental.pallas import tpu as pltpu
from jax.sharding import PartitionSpec as P


NORM_EPS = 1e-5
INNER_EPS = 1e-6
LOG2E = 1.4426950408889634
N_CHUNK = 4
U_PARTS = ((0, 3), (3, 5), (5, 10))
BF = jnp.bfloat16
F32 = jnp.float32
MESH = pl.DeviceIdType.MESH


def fold_rows(parts):
    sub = lax.broadcasted_iota(jnp.int32, (8, 128), 0)

    def pair(a, b, shift):
        low = (sub & shift) == 0
        p = jnp.where(low, a, b)
        q = jnp.where(low, b, a)
        if shift == 4:
            return p + pltpu.roll(q, 4, 0)
        return p + jnp.where(low, pltpu.roll(q, 8 - shift, 0), pltpu.roll(q, shift, 0))

    for shift in (4, 2, 1):
        parts = [pair(parts[b], parts[b + shift], shift) for b in range(shift)]
    return parts[0]


def step_kernel(dims, res_hbm, norm_w_in, w_in_hbm, conv_w, conv_b_in, w_x_hbm, w_dt_hbm, dt_bias_in, a_log, d_skip_in, w_out_hbm, conv_hbm, ssm_hbm,
                r_out, bt_out, g_out, o_out, dt_out, x_out, xi_out,
                r_ref, w_x, w_dt, norm_w, conv_b, dt_bias, d_skip, w_in, w_out, a_neg, ssm_buf, conv_buf, h_buf, u_own, z_buf, x_buf, low_buf, dt_buf, dtx_buf, b_bc, c_bc, o_buf, hx_buf,
                st_send, st_recv, u_send, u_recv, p_own, p_send, p_recv, g_all, cr_send, cr_recv, xs_send, xs_recv,
                in_sem, ssm_in_sem, conv_in_sem, dt_sem, x_sem, xi_sem, go_sem, o_sem,
                st_s, st_r, u_s, u_r, p_s, p_r, g_s, g_r, cr_s, cr_r, xs_s, xs_r, fw_s, fw_r):
    n_layer, rows, d_loc, e_loc, n_state, n_rank, d_model = dims
    half = rows // 2
    n_chunk = N_CHUNK
    blk = half // n_chunk
    total = n_layer * n_chunk
    n_tile = e_loc // 256
    tx = lax.axis_index("tx")
    ty = lax.axis_index("ty")
    core = lax.rem(ty, 2)
    chip = lax.div(ty, 2)
    y_peer = {"tx": 1 - tx, "ty": ty}
    core_peer = {"tx": tx, "ty": chip * 2 + (1 - core)}
    x_peer = {"tx": tx, "ty": (1 - chip) * 2 + core}
    d_peer = {"tx": tx, "ty": (1 - chip) * 2 + (1 - core)}
    st_peer = {"tx": 1 - tx, "ty": (1 - chip) * 2 + core}

    def layer_of(i):
        return lax.div(i, n_chunk)

    def chunk_of(i):
        return lax.rem(i, n_chunk)

    def part_rows(i, part):
        side = jnp.where(part == 0, tx, 1 - tx)
        return pl.multiple_of(side * half + chunk_of(i) * blk, blk)

    def remote(src, dst, s_sem, r_sem, dev):
        return pltpu.make_async_remote_copy(src_ref=src, dst_ref=dst, send_sem=s_sem, recv_sem=r_sem, device_id=dev, device_id_type=MESH)

    def st_copy(i):
        return remote(st_send.at[i], st_recv.at[i], st_s.at[i], st_r.at[i], st_peer)

    def u_copy(i, k):
        s = lax.rem(i, 2)
        part = pl.ds(U_PARTS[k][0], U_PARTS[k][1] - U_PARTS[k][0])
        return remote(u_send.at[s, part], u_recv.at[i, part], u_s.at[s, k], u_r.at[i, k], y_peer)

    def p_copy(i, q):
        s = lax.rem(i, 2)
        dev = (core_peer, x_peer, d_peer)[q]
        return remote(p_send.at[s], p_recv.at[i, q], p_s.at[s, q], p_r.at[i, q], dev)

    def g_copy(i):
        return remote(g_all.at[i, pl.ds(0, blk)], g_all.at[i, pl.ds(blk, blk)], g_s.at[i], g_r.at[i], y_peer)

    def cr_copy(i):
        return remote(cr_send.at[i], cr_recv.at[i], cr_s.at[i], cr_r.at[i], core_peer)

    def half_rows(h):
        return pl.ds(pl.multiple_of(h * blk, blk), blk)

    def xs_copy(i):
        return remote(xs_send.at[i, half_rows(core)], xs_recv.at[i, half_rows(core)], xs_s.at[i], xs_r.at[i], x_peer)

    def fw_copy(i):
        return remote(xs_recv.at[i, half_rows(core)], xs_recv.at[i, half_rows(core)], fw_s.at[i], fw_r.at[i], core_peer)

    def cache_rows(i):
        return pl.ds(pl.multiple_of(chunk_of(i) * blk, blk), blk)

    def ssm_load(i):
        s = lax.rem(i, 2)
        return pltpu.make_async_copy(ssm_hbm.at[layer_of(i), cache_rows(i)], ssm_buf.at[s], ssm_in_sem.at[s])

    def conv_load(i):
        s = lax.rem(i, 2)
        return pltpu.make_async_copy(conv_hbm.at[layer_of(i), :, cache_rows(i)], conv_buf.at[s, pl.ds(0, 3)], conv_in_sem.at[s])

    def dt_store(i):
        n = blk // 8
        return pltpu.make_async_copy(dt_buf, dt_out.at[layer_of(i), pl.ds(chunk_of(i) * n, n)], dt_sem)

    def x_store(i):
        return pltpu.make_async_copy(x_buf, x_out.at[layer_of(i), cache_rows(i)], x_sem)

    def xi_store(i):
        s = lax.rem(i, 2)
        return pltpu.make_async_copy(conv_buf.at[s, 3], xi_out.at[layer_of(i), cache_rows(i)], xi_sem.at[s])

    def o_store(i):
        return pltpu.make_async_copy(o_buf, o_out.at[cache_rows(i)], o_sem)

    def g_store(i):
        return pltpu.make_async_copy(g_all.at[i, pl.ds(0, blk)], g_out.at[cache_rows(i)], go_sem.at[chunk_of(i)])

    res_load = pltpu.make_async_copy(res_hbm, r_ref, in_sem.at[0])
    w_in_load = [pltpu.make_async_copy(w_in_hbm.at[l], w_in.at[l], in_sem.at[1 + l]) for l in range(n_layer)]
    w_out_load = pltpu.make_async_copy(w_out_hbm, w_out, in_sem.at[1 + n_layer])
    w_x_load = pltpu.make_async_copy(w_x_hbm, w_x, in_sem.at[2 + n_layer])
    w_dt_load = pltpu.make_async_copy(w_dt_hbm, w_dt, in_sem.at[3 + n_layer])
    r_store = pltpu.make_async_copy(r_ref, r_out, in_sem.at[4 + n_layer])

    res_load.start()
    w_in_load[0].start()

    barrier = pltpu.get_barrier_semaphore()
    for dev in (y_peer, core_peer, x_peer, d_peer, st_peer):
        pl.semaphore_signal(barrier, inc=1, device_id=dev, device_id_type=MESH)
    pl.semaphore_wait(barrier, 5)

    def eye():
        n = 2 * blk
        return lax.broadcasted_iota(jnp.int32, (n, n), 0) == lax.broadcasted_iota(jnp.int32, (n, n), 1)

    def phase_a(i):
        sums = []
        for part in range(2):
            val = r_ref[pl.ds(part_rows(i, part), blk), :]
            sums.append(jnp.sum(val * val, axis=1, keepdims=True))
        col = jnp.concatenate(sums, axis=0)
        row = jnp.sum(jnp.where(eye(), col, 0.0), axis=0, keepdims=True)
        st_send[i] = jnp.broadcast_to(row, (8, 2 * blk))
        st_copy(i).start()

    def phase_b(i):
        l = layer_of(i)
        s = lax.rem(i, 2)
        st_copy(i).wait_recv()
        sq = st_send[i] + pltpu.roll(st_recv[i], blk, 1)
        inv = lax.rsqrt(sq / d_model + NORM_EPS)
        col = jnp.sum(jnp.where(eye(), jnp.broadcast_to(inv[0:1], (2 * blk, 2 * blk)), 0.0), axis=1, keepdims=True)
        nw = norm_w[l]
        for part in range(2):
            base = part_rows(i, part)
            for q in range(blk // 16):
                lo = part * blk + q * 16
                val = r_ref[pl.ds(base + q * 16, 16), :]
                h_buf[lo:lo + 16, :] = (val * col[lo:lo + 16] * nw).astype(BF)

        src = lax.broadcasted_iota(jnp.int32, (128, 256), 0)
        dst = lax.broadcasted_iota(jnp.int32, (128, 256), 1)
        for k in range(2):
            spread = jnp.where(dst == 2 * src + k, 1.0, 0.0).astype(BF)
            for t in range(d_loc // 128):
                wide = jnp.dot(h_buf[:, t * 128:(t + 1) * 128], spread, preferred_element_type=F32)
                hx_buf[k * 2 * blk:(k + 1) * 2 * blk, t * 256:(t + 1) * 256] = wide.astype(BF)

        @pl.when(i >= 2)
        def _():
            for k in range(len(U_PARTS)):
                u_copy(i - 2, k).wait_send()

        w_rows = w_in.at[l].reshape(2 * d_loc, e_loc)

        for t in range(n_tile):
            cols = slice(t * 256, (t + 1) * 256)
            u = jnp.dot(hx_buf[...], w_rows[:, cols], preferred_element_type=F32)
            for k in range(2):
                u_own[s, k, :, cols] = u[2 * k * blk:(2 * k + 1) * blk]
                u_send[s, k * n_tile + t] = u[(2 * k + 1) * blk:(2 * k + 2) * blk].astype(BF)
            for k, (lo, hi) in enumerate(U_PARTS):
                if (hi - 1 if hi <= n_tile else n_tile - 1) == t:
                    u_copy(i, k).start()

    def phase_c(i):
        l = layer_of(i)
        s = lax.rem(i, 2)

        @pl.when(i >= 1)
        def _():
            xi_store(i - 1).wait()
            x_store(i - 1).wait()

            @pl.when(i + 1 < total)
            def _():
                conv_load(i + 1).start()

        conv_load(i).wait()

        for t in range(n_tile):
            for k, (lo, hi) in enumerate(U_PARTS):
                if lo == t:
                    u_copy(i, k).wait_recv()
            cols = slice(t * 256, (t + 1) * 256)
            xi = (u_own[s, 0, :, cols] + u_recv[i, t].astype(F32)).astype(BF)
            conv_buf[s, 3, :, cols] = xi
            acc = conv_buf[s, 0, :, cols].astype(F32) * conv_w[l, 0:1, cols]
            acc = acc + conv_buf[s, 1, :, cols].astype(F32) * conv_w[l, 1:2, cols]
            acc = acc + conv_buf[s, 2, :, cols].astype(F32) * conv_w[l, 2:3, cols]
            acc = acc + xi.astype(F32) * conv_w[l, 3:4, cols]
            acc = acc + conv_b[l, :, cols]
            x_buf[:, cols] = (acc * jax.nn.sigmoid(acc)).astype(BF)
        xi_store(i).start()
        x_store(i).start()

        @pl.when(i >= 2)
        def _():
            for q in range(3):
                p_copy(i - 2, q).wait_send()

        pt = lax.dot_general(w_x[l], x_buf[...], (((1,), (1,)), ((), ())), preferred_element_type=F32)
        pt = jnp.concatenate([pt[:pt.shape[0] // 2], pt[pt.shape[0] // 2:]], axis=1)
        p_own[...] = pt
        p_send[s] = pt.astype(BF)
        for q in range(3):
            p_copy(i, q).start()

    def phase_d(i):
        l = layer_of(i)
        s = lax.rem(i, 2)

        for t in range(n_tile):
            for k, (lo, hi) in enumerate(U_PARTS):
                if lo == n_tile + t:
                    u_copy(i, k).wait_recv()
            cols = slice(t * 256, (t + 1) * 256)
            z = (u_own[s, 1, :, cols] + u_recv[i, n_tile + t].astype(F32)).astype(BF).astype(F32)
            z_buf[:, cols] = z * jax.nn.sigmoid(z)
        for q in range(3):
            p_copy(i, q).wait_recv()
        pt = p_own[...]
        for q in range(3):
            pt = pt + p_recv[i, q].astype(F32)
        pt = jnp.concatenate([pt, pltpu.roll(pt, blk, 1)], axis=0)

        def unit(v):
            return v * lax.rsqrt(jnp.mean(v * v, axis=0, keepdims=True) + INNER_EPS)

        low_buf[...] = jnp.transpose(unit(pt[:n_rank]))[:blk].astype(BF)
        bt = unit(pt[n_rank:n_rank + n_state])
        ct = unit(pt[n_rank + n_state:])
        bt_out[i] = bt
        for b in range(blk):
            b_bc[b] = jnp.broadcast_to(bt[:, b:b + 1], (n_state, 128))
            c_bc[b] = jnp.broadcast_to(ct[:, b:b + 1], (n_state, 128))

        @pl.when(i >= 1)
        def _():
            dt_store(i - 1).wait()

        def dt_tile(t, carry):
            cols = pl.ds(pl.multiple_of(t * 256, 256), 256)
            v = jnp.dot(low_buf[...], w_dt[l, :, cols], preferred_element_type=F32)
            v = v + dt_bias[l, :, cols]
            dt = jnp.maximum(v, 0.0) + jnp.log1p(jnp.exp(-jnp.abs(v)))
            dt_buf[:, :, cols] = dt.reshape(blk // 8, 8, 256)
            dtx_buf[:, :, cols] = (dt * x_buf[:, cols].astype(F32)).reshape(blk // 8, 8, 256)
            return carry

        lax.fori_loop(0, e_loc // 256, dt_tile, 0, unroll=True)
        dt_store(i).start()
        ssm_load(i).wait()

        def group(g, carry):
            for j in range(e_loc // 128):
                cols = slice(j * 128, (j + 1) * 128)
                a = a_neg[l, :, cols]
                out = []
                for p in range(2):
                    parts = []
                    for b in range(8):
                        row = g * 16 + p * 8 + b
                        decay = jnp.exp2(jnp.broadcast_to(dt_buf[g * 2 + p, b:b + 1, cols], (n_state, 128)) * a)
                        new = decay * ssm_buf[s, row, :, cols] + jnp.broadcast_to(dtx_buf[g * 2 + p, b:b + 1, cols], (n_state, 128)) * b_bc[row]
                        term = new * c_bc[row]
                        parts.append(term[:8] + term[8:])
                    out.append(fold_rows(parts))
                rws = pl.ds(pl.multiple_of(g * 16, 16), 16)
                y = jnp.concatenate(out, axis=0) + d_skip[l, :, cols] * x_buf[rws, cols].astype(F32)
                g_all[i, rws, cols] = (y * z_buf[rws, cols]).astype(BF)
            return carry

        lax.fori_loop(0, blk // 16, group, 0)

        @pl.when(i < total - n_chunk)
        def _():
            g_copy(i).start()

        @pl.when(i >= total - n_chunk)
        def _():
            g_store(i).start()

            @pl.when(i > total - n_chunk)
            def _():
                o_store(i - 1).wait()

            def o_tile(t, carry):
                cols = pl.ds(pl.multiple_of(t * 256, 256), 256)
                o_buf[:, cols] = jnp.dot(g_all[i, pl.ds(0, blk)], w_out[l, :, cols], preferred_element_type=F32)
                return carry

            lax.fori_loop(0, d_loc // 256, o_tile, 0, unroll=True)
            o_store(i).start()

    def phase_e(i):
        l = layer_of(i)
        g_copy(i).wait_recv()

        def tile(t, carry):
            cols = pl.ds(pl.multiple_of(t * 256, 256), 256)
            cr_send[i, :, cols] = jnp.dot(g_all[i], w_out[l, :, cols], preferred_element_type=F32).astype(BF)
            return carry

        lax.fori_loop(0, d_loc // 256, tile, 0, unroll=True)
        cr_copy(i).start()

    def phase_f(i):
        cr_copy(i).wait_recv()
        xs_send[i] = (cr_send[i].astype(F32) + cr_recv[i].astype(F32)).astype(BF)
        xs_copy(i).start()

    def phase_g(i):
        def add(h):
            rws = pl.ds(part_rows(i, h), blk)
            r_ref[rws, :] = r_ref[rws, :] + (xs_send[i, half_rows(h), :].astype(F32) + xs_recv[i, half_rows(h), :].astype(F32))

        xs_copy(i).wait_recv()
        fw_copy(i).start()
        add(core)
        fw_copy(i).wait_recv()
        add(1 - core)
        phase_a(i + n_chunk)

    for l in range(n_layer):
        for vec, src in ((norm_w, norm_w_in), (conv_b, conv_b_in), (dt_bias, dt_bias_in), (d_skip, d_skip_in)):
            vec[l] = src[l:l + 1, :]
        a_neg[l] = jnp.exp(a_log[l]) * (-LOG2E)
    res_load.wait()

    def first_a(i, carry):
        phase_a(i)
        return carry

    lax.fori_loop(0, n_chunk, first_a, 0)
    w_in_load[0].wait()

    def run(phase, i, stop=total):
        ok = (i >= 0) & (i < stop)

        @pl.when(ok)
        def _():
            phase(i)

    def step(s, carry):
        last = total - n_chunk

        @pl.when((s >= 2) & (s < total))
        def _():
            ssm_load(s).start()

        @pl.when(s == 1)
        def _():
            w_x_load.wait()
            w_dt_load.wait()

        run(phase_c, s - 1)
        run(phase_f, s - 3, last)

        @pl.when(s == n_chunk)
        def _():
            w_in_load[1].wait()

        run(phase_b, s)

        @pl.when(s == 0)
        def _():
            conv_load(0).start()
            w_x_load.start()
            w_dt_load.start()
            conv_load(1).start()
            ssm_load(0).start()
            ssm_load(1).start()
            w_out_load.start()
            w_in_load[1].start()

        run(phase_d, s - 1)
        run(phase_g, s - 3, last)

        @pl.when(s == n_chunk + 2)
        def _():
            r_store.start()

        @pl.when(s == 2)
        def _():
            w_out_load.wait()

        run(phase_e, s - 2, last)
        return carry

    lax.fori_loop(0, total + 1, step, 0)

    r_store.wait()
    xi_store(total - 1).wait()
    x_store(total - 1).wait()
    dt_store(total - 1).wait()
    o_store(total - 1).wait()
    for i in range(total - 2, total):
        for k in range(len(U_PARTS)):
            u_copy(i, k).wait_send()
        for q in range(3):
            p_copy(i, q).wait_send()

    def drain(i, carry):
        st_copy(i).wait_send()
        st_copy(i + n_chunk).wait_send()
        g_copy(i).wait_send()
        cr_copy(i).wait_send()
        xs_copy(i).wait_send()
        fw_copy(i).wait_send()
        g_store(i + total - n_chunk).wait()
        return carry

    lax.fori_loop(0, n_chunk, drain, 0)


def state_kernel(n_carry, blk, ssm_in, dt, x, bt, a_log, conv_in, xi, *refs):
    ssm_out, conv_out, a_neg, b_bc = refs[n_carry:]
    n_state, e_loc = a_log.shape[1:]

    @pl.when(pl.program_id(0) == 0)
    def _():
        a_neg[...] = jnp.exp(a_log[0]) * (-LOG2E)

    for b in range(blk):
        b_bc[b] = jnp.broadcast_to(bt[0, :, b:b + 1], (n_state, 128))
    conv_out[0, 0] = conv_in[0, 1]
    conv_out[0, 1] = conv_in[0, 2]
    conv_out[0, 2] = xi[0]

    def group(g, carry):
        rws16 = pl.ds(pl.multiple_of(g * 16, 16), 16)
        for j in range(e_loc // 128):
            cols = slice(j * 128, (j + 1) * 128)
            a = a_neg[:, cols]
            x16 = x[0, rws16, cols].astype(F32)
            for p in range(2):
                dt8 = dt[0, g * 2 + p, :, cols]
                dtx = dt8 * x16[p * 8:p * 8 + 8]
                rws = pl.ds(pl.multiple_of(g * 16 + p * 8, 8), 8)
                decay = jnp.exp2(dt8[:, None, :] * a[None])
                ssm_out[0, rws, :, cols] = decay * ssm_in[0, rws, :, cols] + dtx[:, None, :] * b_bc[rws]
        return carry

    lax.fori_loop(0, blk // 16, group, 0)


def state_pass(l, ssm_t, dt, x, bt, a_log_t, conv_t, xi, carried):
    _, half, n_state, e_loc = ssm_t.shape
    blk = half // N_CHUNK

    def rows_spec(*tail):
        return pl.BlockSpec((1, blk) + tail, lambda g: (l, g) + (0,) * len(tail))

    conv_spec = pl.BlockSpec((1, 3, blk, e_loc), lambda g: (l, 0, g, 0))
    in_specs = [rows_spec(n_state, e_loc), pl.BlockSpec((1, blk // 8, 8, e_loc), lambda g: (l, g, 0, 0)), rows_spec(e_loc),
                pl.BlockSpec((1, n_state, 128), lambda g: (l * N_CHUNK + g, 0, 0)),
                pl.BlockSpec((1, n_state, e_loc), lambda g: (l, 0, 0)), conv_spec, rows_spec(e_loc)]
    in_specs += [pl.BlockSpec(memory_space=pl.ANY)] * len(carried)
    n_elem = half * n_state * e_loc
    return pl.pallas_call(
        functools.partial(state_kernel, len(carried), blk),
        grid=(half // blk,),
        out_shape=(jax.ShapeDtypeStruct(ssm_t.shape, F32), jax.ShapeDtypeStruct(conv_t.shape, BF)),
        in_specs=in_specs,
        out_specs=(rows_spec(n_state, e_loc), conv_spec),
        scratch_shapes=[pltpu.VMEM((n_state, e_loc), F32), pltpu.VMEM((blk, n_state, 128), F32)],
        input_output_aliases={7 + k: k for k in range(len(carried))},
        compiler_params=pltpu.CompilerParams(vmem_limit_bytes=67043328),
        cost_estimate=pl.CostEstimate(flops=n_elem * 1000, bytes_accessed=n_elem * 8, transcendentals=n_elem),
    )(ssm_t, dt, x, bt, a_log_t, conv_t, xi, *carried)


def out_kernel(l, g_ref, w_hbm, own_hbm, kept_ref, sent_ref, w_buf, own_buf, sem, own_sem):
    first = lax.rem(lax.axis_index("ty"), 2) == 0
    n_tile = kept_ref.shape[1] // 256
    loads = [pltpu.make_async_copy(w_hbm.at[l, :, pl.ds(t * 256, 256)], w_buf.at[t], sem.at[t]) for t in range(n_tile)]
    own_loads = [pltpu.make_async_copy(own_hbm.at[:, pl.ds(t * 256, 256)], own_buf.at[t], own_sem.at[t]) for t in range(n_tile)]
    for t in range(n_tile):
        loads[t].start()
        own_loads[t].start()
    for t in range(n_tile):
        loads[t].wait()
        cols = slice(t * 256, (t + 1) * 256)
        peer = jnp.dot(g_ref[...], w_buf[t], preferred_element_type=F32)
        own_loads[t].wait()
        own = own_buf[t]
        kept_ref[:, cols] = jnp.where(first, own, peer)
        sent_ref[:, cols] = jnp.where(first, peer, own).astype(BF)


def out_proj(g, w_out, own, l):
    vmem = pl.BlockSpec(memory_space=pltpu.VMEM)
    n_tile = own.shape[1] // 256
    return pl.pallas_call(
        functools.partial(out_kernel, l),
        out_shape=(jax.ShapeDtypeStruct(own.shape, F32), jax.ShapeDtypeStruct(own.shape, BF)),
        in_specs=[vmem, pl.BlockSpec(memory_space=pltpu.HBM), pl.BlockSpec(memory_space=pltpu.HBM)],
        out_specs=(vmem, vmem),
        scratch_shapes=[pltpu.VMEM((n_tile, w_out.shape[1], 256), BF), pltpu.VMEM((n_tile, own.shape[0], 256), F32), pltpu.SemaphoreType.DMA((n_tile,)), pltpu.SemaphoreType.DMA((n_tile,))],
        compiler_params=pltpu.CompilerParams(vmem_limit_bytes=24 * 2 ** 20),
        name="out_proj",
    )(g, w_out, own)


def solution(mesh):
    def local_step(residual, norm_w, w_in, conv_w, conv_b, w_x, w_dt, dt_bias, a_log, d_skip, w_out, conv_state, ssm_state):
        n_layer = norm_w.shape[0]
        rows, d_loc = residual.shape
        e_loc = w_x.shape[1]
        n_state = a_log.shape[-1]
        n_rank = w_dt.shape[1]
        n_proj = w_x.shape[2]
        d_model = d_loc * mesh.shape["tx"]
        total = n_layer * N_CHUNK
        blk = rows // 2 // N_CHUNK
        dims = (n_layer, rows, d_loc, e_loc, n_state, n_rank, d_model)
        conv_t = jnp.transpose(conv_state, (0, 3, 1, 2))
        ssm_t = jnp.transpose(ssm_state, (0, 1, 3, 2))
        a_log_t = jnp.transpose(a_log, (0, 2, 1))
        args = (residual, norm_w, w_in, jnp.transpose(conv_w, (0, 2, 1)), conv_b, jnp.transpose(w_x, (0, 2, 1)), w_dt, dt_bias, a_log_t, d_skip, w_out, conv_t, ssm_t)
        hbm = pl.BlockSpec(memory_space=pl.ANY)
        vmem = pl.BlockSpec(memory_space=pltpu.VMEM)
        in_specs = [hbm, vmem, hbm, vmem, vmem, hbm, hbm, vmem, vmem, vmem, hbm, hbm, hbm]
        dma = pltpu.SemaphoreType.DMA
        scratch = [pltpu.VMEM((rows, d_loc), F32), pltpu.VMEM((n_layer, n_proj, e_loc), BF), pltpu.VMEM((n_layer, n_rank, e_loc), BF), pltpu.VMEM((n_layer, 1, d_loc), F32)] + [pltpu.VMEM((n_layer, 1, e_loc), F32)] * 3 + [
            pltpu.VMEM((n_layer, d_loc, 2, e_loc), BF),
            pltpu.VMEM((n_layer, e_loc, d_loc), BF),
            pltpu.VMEM((n_layer, n_state, e_loc), F32),
            pltpu.VMEM((2, blk, n_state, e_loc), F32),
            pltpu.VMEM((2, 4, blk, e_loc), BF),
            pltpu.VMEM((2 * blk, d_loc), BF),
            pltpu.VMEM((2, 2, blk, e_loc), F32),
            pltpu.VMEM((blk, e_loc), F32),
            pltpu.VMEM((blk, e_loc), BF),
            pltpu.VMEM((blk, n_rank), BF),
            pltpu.VMEM((blk // 8, 8, e_loc), F32),
            pltpu.VMEM((blk // 8, 8, e_loc), F32),
            pltpu.VMEM((blk, n_state, 128), F32),
            pltpu.VMEM((blk, n_state, 128), F32),
            pltpu.VMEM((blk, d_loc), F32),
            pltpu.VMEM((4 * blk, 2 * d_loc), BF),
            pltpu.VMEM((total, 8, 2 * blk), F32),
            pltpu.VMEM((total, 8, 2 * blk), F32),
            pltpu.VMEM((2, 2 * (e_loc // 256), blk, 256), BF),
            pltpu.VMEM((total, 2 * (e_loc // 256), blk, 256), BF),
            pltpu.VMEM((n_proj // 2, 2 * blk), F32),
            pltpu.VMEM((2, n_proj // 2, 2 * blk), BF),
            pltpu.VMEM((total, 3, n_proj // 2, 2 * blk), BF),
            pltpu.VMEM((total, 2 * blk, e_loc), BF),
        ] + [pltpu.VMEM((N_CHUNK, 2 * blk, d_loc), BF)] * 4 + [
            dma((5 + n_layer,)), dma((2,)), dma((2,)), dma(()), dma(()), dma((2,)), dma((N_CHUNK,)), dma(()),
            dma((total,)), dma((total,)), dma((2, len(U_PARTS))), dma((total, len(U_PARTS))), dma((2, 3)), dma((total, 3)),
            dma((total,)), dma((total,)), dma((N_CHUNK,)), dma((N_CHUNK,)), dma((N_CHUNK,)), dma((N_CHUNK,)), dma((N_CHUNK,)), dma((N_CHUNK,)),
        ]
        half = rows // 2
        r_mid, bt, g_own, o_own, dt, x_act, xi = pl.pallas_call(
            functools.partial(step_kernel, dims),
            out_shape=(jax.ShapeDtypeStruct((rows, d_loc), F32), jax.ShapeDtypeStruct((total, n_state, 128), F32), jax.ShapeDtypeStruct((half, e_loc), BF), jax.ShapeDtypeStruct((half, d_loc), F32),
                       jax.ShapeDtypeStruct((n_layer, half // 8, 8, e_loc), F32), jax.ShapeDtypeStruct((n_layer, half, e_loc), BF), jax.ShapeDtypeStruct((n_layer, half, e_loc), BF)),
            in_specs=in_specs,
            out_specs=(hbm, vmem, hbm, hbm, hbm, hbm, hbm),
            scratch_shapes=scratch,
            compiler_params=pltpu.CompilerParams(collective_id=0, has_side_effects=True, vmem_limit_bytes=67043328),
            name="mamba_step",
        )(*args)

        core = lax.rem(lax.axis_index("ty"), 2)
        tx = lax.axis_index("tx")
        core_swap = [(0, 1), (1, 0), (2, 3), (3, 2)]
        g_peer = lax.ppermute(g_own, "tx", [(0, 1), (1, 0)])
        caches = state_pass(0, ssm_t, dt, x_act, bt, a_log_t, conv_t, xi, ())
        kept, sent = out_proj(g_peer, pltpu.with_memory_space_constraint(w_out, pltpu.HBM), pltpu.with_memory_space_constraint(o_own, pltpu.HBM), n_layer - 1)
        part = (kept + lax.ppermute(sent, "ty", core_swap).astype(F32)).astype(BF)
        other = lax.ppermute(part, "ty", [(0, 2), (2, 0), (1, 3), (3, 1)])
        part_peer = lax.ppermute(part, "ty", core_swap)
        caches = state_pass(1, ssm_t, dt, x_act, bt, a_log_t, conv_t, xi, caches)
        other_peer = lax.ppermute(other, "ty", core_swap)
        mine = part.astype(F32) + other.astype(F32)
        theirs = part_peer.astype(F32) + other_peer.astype(F32)
        same = core == tx
        r_out = r_mid + jnp.concatenate([jnp.where(same, mine, theirs), jnp.where(same, theirs, mine)], axis=0)
        return r_out, jnp.transpose(caches[1], (0, 2, 3, 1)), jnp.transpose(caches[0], (0, 1, 3, 2))

    cache_spec = P(None, ("dp", "tx"), "ty", None)
    in_specs = (P("dp", "tx"), P(None, "tx"), P(None, "tx", None, "ty"), P(None, "ty", None), P(None, "ty"), P(None, "ty", None), P(None, None, "ty"), P(None, "ty"), P(None, "ty", None), P(None, "ty"), P(None, "ty", "tx"), cache_spec, cache_spec)
    out_specs = (P("dp", "tx"), cache_spec, cache_spec)
    return jax.shard_map(local_step, mesh=mesh, in_specs=in_specs, out_specs=out_specs, check_vma=False)
```

```python
import functools
import jax
import jax.numpy as jnp
from jax import lax
from jax.experimental import pallas as pl
from jax.experimental.pallas import tpu as pltpu
from jax.sharding import PartitionSpec as P


NORM_EPS = 1e-5
INNER_EPS = 1e-6
LOG2E = 1.4426950408889634
N_CHUNK = 4
U_PARTS = ((0, 3), (3, 5), (5, 10))
BF = jnp.bfloat16
F32 = jnp.float32
MESH = pl.DeviceIdType.MESH


def fold_rows(parts):
    sub = lax.broadcasted_iota(jnp.int32, (8, 128), 0)

    def pair(a, b, shift):
        low = (sub & shift) == 0
        p = jnp.where(low, a, b)
        q = jnp.where(low, b, a)
        if shift == 4:
            return p + pltpu.roll(q, 4, 0)
        return p + jnp.where(low, pltpu.roll(q, 8 - shift, 0), pltpu.roll(q, shift, 0))

    for shift in (4, 2, 1):
        parts = [pair(parts[b], parts[b + shift], shift) for b in range(shift)]
    return parts[0]


def step_kernel(dims, res_hbm, norm_w_in, w_in_hbm, conv_w, conv_b_in, w_x_hbm, w_dt_hbm, dt_bias_in, a_log, d_skip_in, w_out_hbm, conv_hbm, ssm_hbm,
                r_out, bt_out, g_out, dt_out, x_out, xi_out,
                r_ref, w_x, w_dt, norm_w, conv_b, dt_bias, d_skip, w_in, w_out, a_neg, ssm_buf, conv_buf, h_buf, u_own, z_buf, x_buf, low_buf, dt_buf, dtx_buf, b_bc, c_bc, hx_buf,
                st_send, st_recv, u_send, u_recv, p_own, p_send, p_recv, g_all, cr_send, cr_recv, xs_send, xs_recv,
                in_sem, ssm_in_sem, conv_in_sem, dt_sem, x_sem, xi_sem, go_sem,
                st_s, st_r, u_s, u_r, p_s, p_r, g_s, g_r, cr_s, cr_r, xs_s, xs_r, fw_s, fw_r):
    n_layer, rows, d_loc, e_loc, n_state, n_rank, d_model = dims
    half = rows // 2
    n_chunk = N_CHUNK
    blk = half // n_chunk
    total = n_layer * n_chunk
    n_tile = e_loc // 256
    tx = lax.axis_index("tx")
    ty = lax.axis_index("ty")
    core = lax.rem(ty, 2)
    chip = lax.div(ty, 2)
    y_peer = {"tx": 1 - tx, "ty": ty}
    core_peer = {"tx": tx, "ty": chip * 2 + (1 - core)}
    x_peer = {"tx": tx, "ty": (1 - chip) * 2 + core}
    d_peer = {"tx": tx, "ty": (1 - chip) * 2 + (1 - core)}
    st_peer = {"tx": 1 - tx, "ty": (1 - chip) * 2 + core}

    def layer_of(i):
        return lax.div(i, n_chunk)

    def chunk_of(i):
        return lax.rem(i, n_chunk)

    def part_rows(i, part):
        side = jnp.where(part == 0, tx, 1 - tx)
        return pl.multiple_of(side * half + chunk_of(i) * blk, blk)

    def remote(src, dst, s_sem, r_sem, dev):
        return pltpu.make_async_remote_copy(src_ref=src, dst_ref=dst, send_sem=s_sem, recv_sem=r_sem, device_id=dev, device_id_type=MESH)

    def st_copy(i):
        return remote(st_send.at[i], st_recv.at[i], st_s.at[i], st_r.at[i], st_peer)

    def u_copy(i, k):
        s = lax.rem(i, 2)
        part = pl.ds(U_PARTS[k][0], U_PARTS[k][1] - U_PARTS[k][0])
        return remote(u_send.at[s, part], u_recv.at[i, part], u_s.at[s, k], u_r.at[i, k], y_peer)

    def p_copy(i, q):
        s = lax.rem(i, 2)
        dev = (core_peer, x_peer, d_peer)[q]
        return remote(p_send.at[s], p_recv.at[i, q], p_s.at[s, q], p_r.at[i, q], dev)

    def g_copy(i):
        return remote(g_all.at[i, pl.ds(0, blk)], g_all.at[i, pl.ds(blk, blk)], g_s.at[i], g_r.at[i], y_peer)

    def cr_copy(i):
        return remote(cr_send.at[i], cr_recv.at[i], cr_s.at[i], cr_r.at[i], core_peer)

    def half_rows(h):
        return pl.ds(pl.multiple_of(h * blk, blk), blk)

    def xs_copy(i):
        return remote(xs_send.at[i, half_rows(core)], xs_recv.at[i, half_rows(core)], xs_s.at[i], xs_r.at[i], x_peer)

    def fw_copy(i):
        return remote(xs_recv.at[i, half_rows(core)], xs_recv.at[i, half_rows(core)], fw_s.at[i], fw_r.at[i], core_peer)

    def cache_rows(i):
        return pl.ds(pl.multiple_of(chunk_of(i) * blk, blk), blk)

    def ssm_load(i):
        s = lax.rem(i, 2)
        return pltpu.make_async_copy(ssm_hbm.at[layer_of(i), cache_rows(i)], ssm_buf.at[s], ssm_in_sem.at[s])

    def conv_load(i):
        s = lax.rem(i, 2)
        return pltpu.make_async_copy(conv_hbm.at[layer_of(i), :, cache_rows(i)], conv_buf.at[s, pl.ds(0, 3)], conv_in_sem.at[s])

    def dt_store(i):
        n = blk // 8
        return pltpu.make_async_copy(dt_buf, dt_out.at[layer_of(i), pl.ds(chunk_of(i) * n, n)], dt_sem)

    def x_store(i):
        return pltpu.make_async_copy(x_buf, x_out.at[layer_of(i), cache_rows(i)], x_sem)

    def xi_store(i):
        s = lax.rem(i, 2)
        return pltpu.make_async_copy(conv_buf.at[s, 3], xi_out.at[layer_of(i), cache_rows(i)], xi_sem.at[s])

    def g_store(i):
        return pltpu.make_async_copy(g_all.at[i, pl.ds(0, blk)], g_out.at[cache_rows(i)], go_sem.at[chunk_of(i)])

    res_load = pltpu.make_async_copy(res_hbm, r_ref, in_sem.at[0])
    w_in_load = [pltpu.make_async_copy(w_in_hbm.at[l], w_in.at[l], in_sem.at[1 + l]) for l in range(n_layer)]
    w_out_load = pltpu.make_async_copy(w_out_hbm, w_out, in_sem.at[1 + n_layer])
    w_x_load = pltpu.make_async_copy(w_x_hbm, w_x, in_sem.at[2 + n_layer])
    w_dt_load = pltpu.make_async_copy(w_dt_hbm, w_dt, in_sem.at[3 + n_layer])
    r_store = pltpu.make_async_copy(r_ref, r_out, in_sem.at[4 + n_layer])

    res_load.start()
    w_in_load[0].start()

    barrier = pltpu.get_barrier_semaphore()
    for dev in (y_peer, core_peer, x_peer, d_peer, st_peer):
        pl.semaphore_signal(barrier, inc=1, device_id=dev, device_id_type=MESH)
    pl.semaphore_wait(barrier, 5)

    def eye():
        n = 2 * blk
        return lax.broadcasted_iota(jnp.int32, (n, n), 0) == lax.broadcasted_iota(jnp.int32, (n, n), 1)

    def phase_a(i):
        sums = []
        for part in range(2):
            val = r_ref[pl.ds(part_rows(i, part), blk), :]
            sums.append(jnp.sum(val * val, axis=1, keepdims=True))
        col = jnp.concatenate(sums, axis=0)
        row = jnp.sum(jnp.where(eye(), col, 0.0), axis=0, keepdims=True)
        st_send[i] = jnp.broadcast_to(row, (8, 2 * blk))
        st_copy(i).start()

    def phase_b(i):
        l = layer_of(i)
        s = lax.rem(i, 2)
        st_copy(i).wait_recv()
        sq = st_send[i] + pltpu.roll(st_recv[i], blk, 1)
        inv = lax.rsqrt(sq / d_model + NORM_EPS)
        col = jnp.sum(jnp.where(eye(), jnp.broadcast_to(inv[0:1], (2 * blk, 2 * blk)), 0.0), axis=1, keepdims=True)
        nw = norm_w[l]
        for part in range(2):
            base = part_rows(i, part)
            for q in range(blk // 16):
                lo = part * blk + q * 16
                val = r_ref[pl.ds(base + q * 16, 16), :]
                h_buf[lo:lo + 16, :] = (val * col[lo:lo + 16] * nw).astype(BF)

        src = lax.broadcasted_iota(jnp.int32, (128, 256), 0)
        dst = lax.broadcasted_iota(jnp.int32, (128, 256), 1)
        for k in range(2):
            spread = jnp.where(dst == 2 * src + k, 1.0, 0.0).astype(BF)
            for t in range(d_loc // 128):
                wide = jnp.dot(h_buf[:, t * 128:(t + 1) * 128], spread, preferred_element_type=F32)
                hx_buf[k * 2 * blk:(k + 1) * 2 * blk, t * 256:(t + 1) * 256] = wide.astype(BF)

        @pl.when(i >= 2)
        def _():
            for k in range(len(U_PARTS)):
                u_copy(i - 2, k).wait_send()

        w_rows = w_in.at[l].reshape(2 * d_loc, e_loc)

        for t in range(n_tile):
            cols = slice(t * 256, (t + 1) * 256)
            u = jnp.dot(hx_buf[...], w_rows[:, cols], preferred_element_type=F32)
            for k in range(2):
                u_own[s, k, :, cols] = u[2 * k * blk:(2 * k + 1) * blk]
                u_send[s, k * n_tile + t] = u[(2 * k + 1) * blk:(2 * k + 2) * blk].astype(BF)
            for k, (lo, hi) in enumerate(U_PARTS):
                if (hi - 1 if hi <= n_tile else n_tile - 1) == t:
                    u_copy(i, k).start()

    def phase_c(i):
        l = layer_of(i)
        s = lax.rem(i, 2)

        @pl.when(i >= 1)
        def _():
            xi_store(i - 1).wait()
            x_store(i - 1).wait()

            @pl.when(i + 1 < total)
            def _():
                conv_load(i + 1).start()

        conv_load(i).wait()

        for t in range(n_tile):
            for k, (lo, hi) in enumerate(U_PARTS):
                if lo == t:
                    u_copy(i, k).wait_recv()
            cols = slice(t * 256, (t + 1) * 256)
            xi = (u_own[s, 0, :, cols] + u_recv[i, t].astype(F32)).astype(BF)
            conv_buf[s, 3, :, cols] = xi
            acc = conv_buf[s, 0, :, cols].astype(F32) * conv_w[l, 0:1, cols]
            acc = acc + conv_buf[s, 1, :, cols].astype(F32) * conv_w[l, 1:2, cols]
            acc = acc + conv_buf[s, 2, :, cols].astype(F32) * conv_w[l, 2:3, cols]
            acc = acc + xi.astype(F32) * conv_w[l, 3:4, cols]
            acc = acc + conv_b[l, :, cols]
            x_buf[:, cols] = (acc * jax.nn.sigmoid(acc)).astype(BF)
        xi_store(i).start()
        x_store(i).start()

        @pl.when(i >= 2)
        def _():
            for q in range(3):
                p_copy(i - 2, q).wait_send()

        pt = lax.dot_general(w_x[l], x_buf[...], (((1,), (1,)), ((), ())), preferred_element_type=F32)
        pt = jnp.concatenate([pt[:pt.shape[0] // 2], pt[pt.shape[0] // 2:]], axis=1)
        p_own[...] = pt
        p_send[s] = pt.astype(BF)
        for q in range(3):
            p_copy(i, q).start()

    def phase_d(i):
        l = layer_of(i)
        s = lax.rem(i, 2)

        for t in range(n_tile):
            for k, (lo, hi) in enumerate(U_PARTS):
                if lo == n_tile + t:
                    u_copy(i, k).wait_recv()
            cols = slice(t * 256, (t + 1) * 256)
            z = (u_own[s, 1, :, cols] + u_recv[i, n_tile + t].astype(F32)).astype(BF).astype(F32)
            z_buf[:, cols] = z * jax.nn.sigmoid(z)
        for q in range(3):
            p_copy(i, q).wait_recv()
        pt = p_own[...]
        for q in range(3):
            pt = pt + p_recv[i, q].astype(F32)
        pt = jnp.concatenate([pt, pltpu.roll(pt, blk, 1)], axis=0)

        def unit(v):
            return v * lax.rsqrt(jnp.mean(v * v, axis=0, keepdims=True) + INNER_EPS)

        low_buf[...] = jnp.transpose(unit(pt[:n_rank]))[:blk].astype(BF)
        bt = unit(pt[n_rank:n_rank + n_state])
        ct = unit(pt[n_rank + n_state:])
        bt_out[i] = bt
        for b in range(blk):
            b_bc[b] = jnp.broadcast_to(bt[:, b:b + 1], (n_state, 128))
            c_bc[b] = jnp.broadcast_to(ct[:, b:b + 1], (n_state, 128))

        @pl.when(i >= 1)
        def _():
            dt_store(i - 1).wait()

        def dt_tile(t, carry):
            cols = pl.ds(pl.multiple_of(t * 256, 256), 256)
            v = jnp.dot(low_buf[...], w_dt[l, :, cols], preferred_element_type=F32)
            v = v + dt_bias[l, :, cols]
            dt = jnp.maximum(v, 0.0) + jnp.log1p(jnp.exp(-jnp.abs(v)))
            dt_buf[:, :, cols] = dt.reshape(blk // 8, 8, 256)
            dtx_buf[:, :, cols] = (dt * x_buf[:, cols].astype(F32)).reshape(blk // 8, 8, 256)
            return carry

        lax.fori_loop(0, e_loc // 256, dt_tile, 0, unroll=True)
        dt_store(i).start()
        ssm_load(i).wait()

        def group(g, carry):
            for j in range(e_loc // 128):
                cols = slice(j * 128, (j + 1) * 128)
                a = a_neg[l, :, cols]
                out = []
                for p in range(2):
                    parts = []
                    for b in range(8):
                        row = g * 16 + p * 8 + b
                        decay = jnp.exp2(jnp.broadcast_to(dt_buf[g * 2 + p, b:b + 1, cols], (n_state, 128)) * a)
                        new = decay * ssm_buf[s, row, :, cols] + jnp.broadcast_to(dtx_buf[g * 2 + p, b:b + 1, cols], (n_state, 128)) * b_bc[row]
                        term = new * c_bc[row]
                        parts.append(term[:8] + term[8:])
                    out.append(fold_rows(parts))
                rws = pl.ds(pl.multiple_of(g * 16, 16), 16)
                y = jnp.concatenate(out, axis=0) + d_skip[l, :, cols] * x_buf[rws, cols].astype(F32)
                g_all[i, rws, cols] = (y * z_buf[rws, cols]).astype(BF)
            return carry

        lax.fori_loop(0, blk // 16, group, 0)

        @pl.when(i < total - n_chunk)
        def _():
            g_copy(i).start()

        @pl.when(i >= total - n_chunk)
        def _():
            g_store(i).start()

    def phase_e(i):
        l = layer_of(i)
        g_copy(i).wait_recv()

        def tile(t, carry):
            cols = pl.ds(pl.multiple_of(t * 256, 256), 256)
            cr_send[i, :, cols] = jnp.dot(g_all[i], w_out[l, :, cols], preferred_element_type=F32).astype(BF)
            return carry

        lax.fori_loop(0, d_loc // 256, tile, 0, unroll=True)
        cr_copy(i).start()

    def phase_f(i):
        cr_copy(i).wait_recv()
        xs_send[i] = (cr_send[i].astype(F32) + cr_recv[i].astype(F32)).astype(BF)
        xs_copy(i).start()

    def phase_g(i):
        def add(h):
            rws = pl.ds(part_rows(i, h), blk)
            r_ref[rws, :] = r_ref[rws, :] + (xs_send[i, half_rows(h), :].astype(F32) + xs_recv[i, half_rows(h), :].astype(F32))

        xs_copy(i).wait_recv()
        fw_copy(i).start()
        add(core)
        fw_copy(i).wait_recv()
        add(1 - core)
        phase_a(i + n_chunk)

    for l in range(n_layer):
        for vec, src in ((norm_w, norm_w_in), (conv_b, conv_b_in), (dt_bias, dt_bias_in), (d_skip, d_skip_in)):
            vec[l] = src[l:l + 1, :]
        a_neg[l] = jnp.exp(a_log[l]) * (-LOG2E)
    res_load.wait()

    def first_a(i, carry):
        phase_a(i)
        return carry

    lax.fori_loop(0, n_chunk, first_a, 0)
    w_in_load[0].wait()

    def run(phase, i, stop=total):
        ok = (i >= 0) & (i < stop)

        @pl.when(ok)
        def _():
            phase(i)

    def step(s, carry):
        last = total - n_chunk

        @pl.when((s >= 2) & (s < total))
        def _():
            ssm_load(s).start()

        @pl.when(s == 1)
        def _():
            w_x_load.wait()
            w_dt_load.wait()

        run(phase_c, s - 1)
        run(phase_f, s - 3, last)

        @pl.when(s == n_chunk)
        def _():
            w_in_load[1].wait()

        run(phase_b, s)

        @pl.when(s == 0)
        def _():
            conv_load(0).start()
            w_x_load.start()
            w_dt_load.start()
            conv_load(1).start()
            ssm_load(0).start()
            ssm_load(1).start()
            w_out_load.start()
            w_in_load[1].start()

        run(phase_d, s - 1)
        run(phase_g, s - 3, last)

        @pl.when(s == n_chunk + 2)
        def _():
            r_store.start()

        @pl.when(s == 2)
        def _():
            w_out_load.wait()

        run(phase_e, s - 2, last)
        return carry

    lax.fori_loop(0, total + 1, step, 0)

    r_store.wait()
    xi_store(total - 1).wait()
    x_store(total - 1).wait()
    dt_store(total - 1).wait()
    for i in range(total - 2, total):
        for k in range(len(U_PARTS)):
            u_copy(i, k).wait_send()
        for q in range(3):
            p_copy(i, q).wait_send()

    def drain(i, carry):
        st_copy(i).wait_send()
        st_copy(i + n_chunk).wait_send()
        g_copy(i).wait_send()
        cr_copy(i).wait_send()
        xs_copy(i).wait_send()
        fw_copy(i).wait_send()
        g_store(i + total - n_chunk).wait()
        return carry

    lax.fori_loop(0, n_chunk, drain, 0)


def state_kernel(n_carry, blk, ssm_in, dt, x, bt, a_log, conv_in, xi, *refs):
    ssm_out, conv_out, a_neg, b_bc = refs[n_carry:]
    n_state, e_loc = a_log.shape[1:]

    @pl.when(pl.program_id(0) == 0)
    def _():
        a_neg[...] = jnp.exp(a_log[0]) * (-LOG2E)

    for b in range(blk):
        b_bc[b] = jnp.broadcast_to(bt[0, :, b:b + 1], (n_state, 128))
    conv_out[0, 0] = conv_in[0, 1]
    conv_out[0, 1] = conv_in[0, 2]
    conv_out[0, 2] = xi[0]

    def group(g, carry):
        rws16 = pl.ds(pl.multiple_of(g * 16, 16), 16)
        for j in range(e_loc // 128):
            cols = slice(j * 128, (j + 1) * 128)
            a = a_neg[:, cols]
            x16 = x[0, rws16, cols].astype(F32)
            for p in range(2):
                dt8 = dt[0, g * 2 + p, :, cols]
                dtx = dt8 * x16[p * 8:p * 8 + 8]
                rws = pl.ds(pl.multiple_of(g * 16 + p * 8, 8), 8)
                decay = jnp.exp2(dt8[:, None, :] * a[None])
                ssm_out[0, rws, :, cols] = decay * ssm_in[0, rws, :, cols] + dtx[:, None, :] * b_bc[rws]
        return carry

    lax.fori_loop(0, blk // 16, group, 0)


def state_pass(l, ssm_t, dt, x, bt, a_log_t, conv_t, xi, carried):
    _, half, n_state, e_loc = ssm_t.shape
    blk = half // N_CHUNK

    def rows_spec(*tail):
        return pl.BlockSpec((1, blk) + tail, lambda g: (l, g) + (0,) * len(tail))

    conv_spec = pl.BlockSpec((1, 3, blk, e_loc), lambda g: (l, 0, g, 0))
    in_specs = [rows_spec(n_state, e_loc), pl.BlockSpec((1, blk // 8, 8, e_loc), lambda g: (l, g, 0, 0)), rows_spec(e_loc),
                pl.BlockSpec((1, n_state, 128), lambda g: (l * N_CHUNK + g, 0, 0)),
                pl.BlockSpec((1, n_state, e_loc), lambda g: (l, 0, 0)), conv_spec, rows_spec(e_loc)]
    in_specs += [pl.BlockSpec(memory_space=pl.ANY)] * len(carried)
    n_elem = half * n_state * e_loc
    return pl.pallas_call(
        functools.partial(state_kernel, len(carried), blk),
        grid=(half // blk,),
        out_shape=(jax.ShapeDtypeStruct(ssm_t.shape, F32), jax.ShapeDtypeStruct(conv_t.shape, BF)),
        in_specs=in_specs,
        out_specs=(rows_spec(n_state, e_loc), conv_spec),
        scratch_shapes=[pltpu.VMEM((n_state, e_loc), F32), pltpu.VMEM((blk, n_state, 128), F32)],
        input_output_aliases={7 + k: k for k in range(len(carried))},
        compiler_params=pltpu.CompilerParams(vmem_limit_bytes=67043328),
        cost_estimate=pl.CostEstimate(flops=n_elem * 1000, bytes_accessed=n_elem * 8, transcendentals=n_elem),
    )(ssm_t, dt, x, bt, a_log_t, conv_t, xi, *carried)


def out_kernel(l, g_ref, w_hbm, own_hbm, kept_ref, sent_ref, w_buf, own_buf, sem, own_sem):
    first = lax.rem(lax.axis_index("ty"), 2) == 0
    n_tile = kept_ref.shape[1] // 256
    loads = [pltpu.make_async_copy(w_hbm.at[l, :, pl.ds(t * 256, 256)], w_buf.at[t], sem.at[t]) for t in range(n_tile)]
    own_load = pltpu.make_async_copy(own_hbm, own_buf, own_sem)
    loads[0].start()
    own_load.start()
    for load in loads[1:]:
        load.start()
    for t in range(n_tile):
        loads[t].wait()
        if t == 0:
            own_load.wait()
        cols = slice(t * 256, (t + 1) * 256)
        peer = jnp.dot(g_ref[...], w_buf[t], preferred_element_type=F32)
        own = jnp.dot(own_buf[...], w_buf[t], preferred_element_type=F32)
        kept_ref[:, cols] = jnp.where(first, own, peer)
        sent_ref[:, cols] = jnp.where(first, peer, own).astype(BF)


def out_proj(g, w_out, g_own, l):
    vmem = pl.BlockSpec(memory_space=pltpu.VMEM)
    hbm = pl.BlockSpec(memory_space=pltpu.HBM)
    n_rows, d_loc = g.shape[0], w_out.shape[2]
    n_tile = d_loc // 256
    return pl.pallas_call(
        functools.partial(out_kernel, l),
        out_shape=(jax.ShapeDtypeStruct((n_rows, d_loc), F32), jax.ShapeDtypeStruct((n_rows, d_loc), BF)),
        in_specs=[vmem, hbm, hbm],
        out_specs=(vmem, vmem),
        scratch_shapes=[pltpu.VMEM((n_tile, w_out.shape[1], 256), BF), pltpu.VMEM(g_own.shape, BF), pltpu.SemaphoreType.DMA((n_tile,)), pltpu.SemaphoreType.DMA],
        compiler_params=pltpu.CompilerParams(vmem_limit_bytes=24 * 2 ** 20),
        name="out_proj",
    )(g, w_out, g_own)


def solution(mesh):
    def local_step(residual, norm_w, w_in, conv_w, conv_b, w_x, w_dt, dt_bias, a_log, d_skip, w_out, conv_state, ssm_state):
        n_layer = norm_w.shape[0]
        rows, d_loc = residual.shape
        e_loc = w_x.shape[1]
        n_state = a_log.shape[-1]
        n_rank = w_dt.shape[1]
        n_proj = w_x.shape[2]
        d_model = d_loc * mesh.shape["tx"]
        total = n_layer * N_CHUNK
        blk = rows // 2 // N_CHUNK
        dims = (n_layer, rows, d_loc, e_loc, n_state, n_rank, d_model)
        conv_t = jnp.transpose(conv_state, (0, 3, 1, 2))
        ssm_t = jnp.transpose(ssm_state, (0, 1, 3, 2))
        a_log_t = jnp.transpose(a_log, (0, 2, 1))
        args = (residual, norm_w, w_in, jnp.transpose(conv_w, (0, 2, 1)), conv_b, jnp.transpose(w_x, (0, 2, 1)), w_dt, dt_bias, a_log_t, d_skip, w_out, conv_t, ssm_t)
        hbm = pl.BlockSpec(memory_space=pl.ANY)
        vmem = pl.BlockSpec(memory_space=pltpu.VMEM)
        in_specs = [hbm, vmem, hbm, vmem, vmem, hbm, hbm, vmem, vmem, vmem, hbm, hbm, hbm]
        dma = pltpu.SemaphoreType.DMA
        scratch = [pltpu.VMEM((rows, d_loc), F32), pltpu.VMEM((n_layer, n_proj, e_loc), BF), pltpu.VMEM((n_layer, n_rank, e_loc), BF), pltpu.VMEM((n_layer, 1, d_loc), F32)] + [pltpu.VMEM((n_layer, 1, e_loc), F32)] * 3 + [
            pltpu.VMEM((n_layer, d_loc, 2, e_loc), BF),
            pltpu.VMEM((n_layer, e_loc, d_loc), BF),
            pltpu.VMEM((n_layer, n_state, e_loc), F32),
            pltpu.VMEM((2, blk, n_state, e_loc), F32),
            pltpu.VMEM((2, 4, blk, e_loc), BF),
            pltpu.VMEM((2 * blk, d_loc), BF),
            pltpu.VMEM((2, 2, blk, e_loc), F32),
            pltpu.VMEM((blk, e_loc), F32),
            pltpu.VMEM((blk, e_loc), BF),
            pltpu.VMEM((blk, n_rank), BF),
            pltpu.VMEM((blk // 8, 8, e_loc), F32),
            pltpu.VMEM((blk // 8, 8, e_loc), F32),
            pltpu.VMEM((blk, n_state, 128), F32),
            pltpu.VMEM((blk, n_state, 128), F32),
            pltpu.VMEM((4 * blk, 2 * d_loc), BF),
            pltpu.VMEM((total, 8, 2 * blk), F32),
            pltpu.VMEM((total, 8, 2 * blk), F32),
            pltpu.VMEM((2, 2 * (e_loc // 256), blk, 256), BF),
            pltpu.VMEM((total, 2 * (e_loc // 256), blk, 256), BF),
            pltpu.VMEM((n_proj // 2, 2 * blk), F32),
            pltpu.VMEM((2, n_proj // 2, 2 * blk), BF),
            pltpu.VMEM((total, 3, n_proj // 2, 2 * blk), BF),
            pltpu.VMEM((total, 2 * blk, e_loc), BF),
        ] + [pltpu.VMEM((N_CHUNK, 2 * blk, d_loc), BF)] * 4 + [
            dma((5 + n_layer,)), dma((2,)), dma((2,)), dma(()), dma(()), dma((2,)), dma((N_CHUNK,)),
            dma((total,)), dma((total,)), dma((2, len(U_PARTS))), dma((total, len(U_PARTS))), dma((2, 3)), dma((total, 3)),
            dma((total,)), dma((total,)), dma((N_CHUNK,)), dma((N_CHUNK,)), dma((N_CHUNK,)), dma((N_CHUNK,)), dma((N_CHUNK,)), dma((N_CHUNK,)),
        ]
        half = rows // 2
        r_mid, bt, g_own, dt, x_act, xi = pl.pallas_call(
            functools.partial(step_kernel, dims),
            out_shape=(jax.ShapeDtypeStruct((rows, d_loc), F32), jax.ShapeDtypeStruct((total, n_state, 128), F32), jax.ShapeDtypeStruct((half, e_loc), BF),
                       jax.ShapeDtypeStruct((n_layer, half // 8, 8, e_loc), F32), jax.ShapeDtypeStruct((n_layer, half, e_loc), BF), jax.ShapeDtypeStruct((n_layer, half, e_loc), BF)),
            in_specs=in_specs,
            out_specs=(hbm, vmem, hbm, hbm, hbm, hbm),
            scratch_shapes=scratch,
            compiler_params=pltpu.CompilerParams(collective_id=0, has_side_effects=True, vmem_limit_bytes=67043328),
            name="mamba_step",
        )(*args)

        core = lax.rem(lax.axis_index("ty"), 2)
        tx = lax.axis_index("tx")
        core_swap = [(0, 1), (1, 0), (2, 3), (3, 2)]
        g_peer = lax.ppermute(g_own, "tx", [(0, 1), (1, 0)])
        caches = state_pass(0, ssm_t, dt, x_act, bt, a_log_t, conv_t, xi, ())
        kept, sent = out_proj(g_peer, pltpu.with_memory_space_constraint(w_out, pltpu.HBM), pltpu.with_memory_space_constraint(g_own, pltpu.HBM), n_layer - 1)
        part = (kept + lax.ppermute(sent, "ty", core_swap).astype(F32)).astype(BF)
        other = lax.ppermute(part, "ty", [(0, 2), (2, 0), (1, 3), (3, 1)])
        part_peer = lax.ppermute(part, "ty", core_swap)
        caches = state_pass(1, ssm_t, dt, x_act, bt, a_log_t, conv_t, xi, caches)
        other_peer = lax.ppermute(other, "ty", core_swap)
        mine = part.astype(F32) + other.astype(F32)
        theirs = part_peer.astype(F32) + other_peer.astype(F32)
        same = core == tx
        r_out = r_mid + jnp.concatenate([jnp.where(same, mine, theirs), jnp.where(same, theirs, mine)], axis=0)
        return r_out, jnp.transpose(caches[1], (0, 2, 3, 1)), jnp.transpose(caches[0], (0, 1, 3, 2))

    cache_spec = P(None, ("dp", "tx"), "ty", None)
    in_specs = (P("dp", "tx"), P(None, "tx"), P(None, "tx", None, "ty"), P(None, "ty", None), P(None, "ty"), P(None, "ty", None), P(None, None, "ty"), P(None, "ty"), P(None, "ty", None), P(None, "ty"), P(None, "ty", "tx"), cache_spec, cache_spec)
    out_specs = (P("dp", "tx"), cache_spec, cache_spec)
    return jax.shard_map(local_step, mesh=mesh, in_specs=in_specs, out_specs=out_specs, check_vma=False)
```

```python
import functools
import jax
import jax.numpy as jnp
from jax import lax
from jax.experimental import pallas as pl
from jax.experimental.pallas import tpu as pltpu
from jax.sharding import PartitionSpec as P


NORM_EPS = 1e-5
INNER_EPS = 1e-6
N_CHUNK = 4
U_PARTS = ((0, 3), (3, 5), (5, 10))
BF = jnp.bfloat16
F32 = jnp.float32
MESH = pl.DeviceIdType.MESH


def fold_rows(parts):
    sub = lax.broadcasted_iota(jnp.int32, (8, 128), 0)

    def pair(a, b, shift):
        low = (sub & shift) == 0
        p = jnp.where(low, a, b)
        q = jnp.where(low, b, a)
        if shift == 4:
            return p + pltpu.roll(q, 4, 0)
        return p + jnp.where(low, pltpu.roll(q, 8 - shift, 0), pltpu.roll(q, shift, 0))

    for shift in (4, 2, 1):
        parts = [pair(parts[b], parts[b + shift], shift) for b in range(shift)]
    return parts[0]


def step_kernel(dims, res_hbm, norm_w_in, w_in_hbm, conv_w, conv_b_in, w_x_hbm, w_dt_hbm, dt_bias_in, a_log, d_skip_in, w_out_hbm, conv_hbm, ssm_hbm,
                r_out, bt_out, g_out, dt_out, x_out, xi_out,
                r_ref, w_x, w_dt, norm_w, conv_b, dt_bias, d_skip, w_in, w_out, a_neg, ssm_buf, conv_buf, h_buf, u_own, z_buf, x_buf, low_buf, dt_buf, dtx_buf, b_bc, c_bc, hx_buf,
                st_send, st_recv, u_send, u_recv, p_own, p_send, p_recv, g_all, cr_send, cr_recv, xs_send, xs_recv,
                in_sem, ssm_in_sem, conv_in_sem, dt_sem, x_sem, xi_sem, go_sem,
                st_s, st_r, u_s, u_r, p_s, p_r, g_s, g_r, cr_s, cr_r, xs_s, xs_r, fw_s, fw_r):
    n_layer, rows, d_loc, e_loc, n_state, n_rank, d_model = dims
    half = rows // 2
    n_chunk = N_CHUNK
    blk = half // n_chunk
    total = n_layer * n_chunk
    n_tile = e_loc // 256
    tx = lax.axis_index("tx")
    ty = lax.axis_index("ty")
    core = lax.rem(ty, 2)
    chip = lax.div(ty, 2)
    y_peer = {"tx": 1 - tx, "ty": ty}
    core_peer = {"tx": tx, "ty": chip * 2 + (1 - core)}
    x_peer = {"tx": tx, "ty": (1 - chip) * 2 + core}
    d_peer = {"tx": tx, "ty": (1 - chip) * 2 + (1 - core)}
    st_peer = {"tx": 1 - tx, "ty": (1 - chip) * 2 + core}

    def layer_of(i):
        return lax.div(i, n_chunk)

    def chunk_of(i):
        return lax.rem(i, n_chunk)

    def part_rows(i, part):
        side = jnp.where(part == 0, tx, 1 - tx)
        return pl.multiple_of(side * half + chunk_of(i) * blk, blk)

    def remote(src, dst, s_sem, r_sem, dev):
        return pltpu.make_async_remote_copy(src_ref=src, dst_ref=dst, send_sem=s_sem, recv_sem=r_sem, device_id=dev, device_id_type=MESH)

    def st_copy(i):
        return remote(st_send.at[i], st_recv.at[i], st_s.at[i], st_r.at[i], st_peer)

    def u_copy(i, k):
        s = lax.rem(i, 2)
        part = pl.ds(U_PARTS[k][0], U_PARTS[k][1] - U_PARTS[k][0])
        return remote(u_send.at[s, part], u_recv.at[i, part], u_s.at[s, k], u_r.at[i, k], y_peer)

    def p_copy(i, q):
        s = lax.rem(i, 2)
        dev = (core_peer, x_peer, d_peer)[q]
        return remote(p_send.at[s], p_recv.at[i, q], p_s.at[s, q], p_r.at[i, q], dev)

    def g_copy(i):
        return remote(g_all.at[i, pl.ds(0, blk)], g_all.at[i, pl.ds(blk, blk)], g_s.at[i], g_r.at[i], y_peer)

    def cr_copy(i):
        return remote(cr_send.at[i], cr_recv.at[i], cr_s.at[i], cr_r.at[i], core_peer)

    def half_rows(h):
        return pl.ds(pl.multiple_of(h * blk, blk), blk)

    def xs_copy(i):
        return remote(xs_send.at[i, half_rows(core)], xs_recv.at[i, half_rows(core)], xs_s.at[i], xs_r.at[i], x_peer)

    def fw_copy(i):
        return remote(xs_recv.at[i, half_rows(core)], xs_recv.at[i, half_rows(core)], fw_s.at[i], fw_r.at[i], core_peer)

    def cache_rows(i):
        return pl.ds(pl.multiple_of(chunk_of(i) * blk, blk), blk)

    def ssm_load(i):
        s = lax.rem(i, 2)
        return pltpu.make_async_copy(ssm_hbm.at[layer_of(i), cache_rows(i)], ssm_buf.at[s], ssm_in_sem.at[s])

    def conv_load(i):
        s = lax.rem(i, 2)
        return pltpu.make_async_copy(conv_hbm.at[layer_of(i), :, cache_rows(i)], conv_buf.at[s, pl.ds(0, 3)], conv_in_sem.at[s])

    def dt_store(i):
        n = blk // 8
        return pltpu.make_async_copy(dt_buf, dt_out.at[layer_of(i), pl.ds(chunk_of(i) * n, n)], dt_sem)

    def x_store(i):
        return pltpu.make_async_copy(x_buf, x_out.at[layer_of(i), cache_rows(i)], x_sem)

    def xi_store(i):
        s = lax.rem(i, 2)
        return pltpu.make_async_copy(conv_buf.at[s, 3], xi_out.at[layer_of(i), cache_rows(i)], xi_sem.at[s])

    def g_store(i):
        return pltpu.make_async_copy(g_all.at[i, pl.ds(0, blk)], g_out.at[cache_rows(i)], go_sem.at[chunk_of(i)])

    res_load = pltpu.make_async_copy(res_hbm, r_ref, in_sem.at[0])
    w_in_load = [pltpu.make_async_copy(w_in_hbm.at[l], w_in.at[l], in_sem.at[1 + l]) for l in range(n_layer)]
    w_out_load = pltpu.make_async_copy(w_out_hbm, w_out, in_sem.at[1 + n_layer])
    w_x_load = pltpu.make_async_copy(w_x_hbm, w_x, in_sem.at[2 + n_layer])
    w_dt_load = pltpu.make_async_copy(w_dt_hbm, w_dt, in_sem.at[3 + n_layer])
    r_store = pltpu.make_async_copy(r_ref, r_out, in_sem.at[4 + n_layer])

    res_load.start()
    w_in_load[0].start()

    barrier = pltpu.get_barrier_semaphore()
    for dev in (y_peer, core_peer, x_peer, d_peer, st_peer):
        pl.semaphore_signal(barrier, inc=1, device_id=dev, device_id_type=MESH)
    pl.semaphore_wait(barrier, 5)

    def eye():
        n = 2 * blk
        return lax.broadcasted_iota(jnp.int32, (n, n), 0) == lax.broadcasted_iota(jnp.int32, (n, n), 1)

    def phase_a(i):
        sums = []
        for part in range(2):
            val = r_ref[pl.ds(part_rows(i, part), blk), :]
            sums.append(jnp.sum(val * val, axis=1, keepdims=True))
        col = jnp.concatenate(sums, axis=0)
        row = jnp.sum(jnp.where(eye(), col, 0.0), axis=0, keepdims=True)
        st_send[i] = jnp.broadcast_to(row, (8, 2 * blk))
        st_copy(i).start()

    def phase_b(i):
        l = layer_of(i)
        s = lax.rem(i, 2)
        st_copy(i).wait_recv()
        sq = st_send[i] + pltpu.roll(st_recv[i], blk, 1)
        inv = lax.rsqrt(sq / d_model + NORM_EPS)
        col = jnp.sum(jnp.where(eye(), jnp.broadcast_to(inv[0:1], (2 * blk, 2 * blk)), 0.0), axis=1, keepdims=True)
        nw = norm_w[l]
        for part in range(2):
            base = part_rows(i, part)
            for q in range(blk // 16):
                lo = part * blk + q * 16
                val = r_ref[pl.ds(base + q * 16, 16), :]
                h_buf[lo:lo + 16, :] = (val * col[lo:lo + 16] * nw).astype(BF)

        src = lax.broadcasted_iota(jnp.int32, (128, 256), 0)
        dst = lax.broadcasted_iota(jnp.int32, (128, 256), 1)
        for k in range(2):
            spread = jnp.where(dst == 2 * src + k, 1.0, 0.0).astype(BF)
            for t in range(d_loc // 128):
                wide = jnp.dot(h_buf[:, t * 128:(t + 1) * 128], spread, preferred_element_type=F32)
                hx_buf[k * 2 * blk:(k + 1) * 2 * blk, t * 256:(t + 1) * 256] = wide.astype(BF)

        @pl.when(i >= 2)
        def _():
            for k in range(len(U_PARTS)):
                u_copy(i - 2, k).wait_send()

        w_rows = w_in.at[l].reshape(2 * d_loc, e_loc)

        for t in range(n_tile):
            cols = slice(t * 256, (t + 1) * 256)
            u = jnp.dot(hx_buf[...], w_rows[:, cols], preferred_element_type=F32)
            for k in range(2):
                u_own[s, k, :, cols] = u[2 * k * blk:(2 * k + 1) * blk]
                u_send[s, k * n_tile + t] = u[(2 * k + 1) * blk:(2 * k + 2) * blk].astype(BF)
            for k, (lo, hi) in enumerate(U_PARTS):
                if (hi - 1 if hi <= n_tile else n_tile - 1) == t:
                    u_copy(i, k).start()

    def phase_c(i):
        l = layer_of(i)
        s = lax.rem(i, 2)

        @pl.when(i >= 1)
        def _():
            xi_store(i - 1).wait()
            x_store(i - 1).wait()

            @pl.when(i + 1 < total)
            def _():
                conv_load(i + 1).start()

        conv_load(i).wait()

        for t in range(n_tile):
            for k, (lo, hi) in enumerate(U_PARTS):
                if lo == t:
                    u_copy(i, k).wait_recv()
            cols = slice(t * 256, (t + 1) * 256)
            xi = (u_own[s, 0, :, cols] + u_recv[i, t].astype(F32)).astype(BF)
            conv_buf[s, 3, :, cols] = xi
            acc = conv_buf[s, 0, :, cols].astype(F32) * conv_w[l, 0:1, cols]
            acc = acc + conv_buf[s, 1, :, cols].astype(F32) * conv_w[l, 1:2, cols]
            acc = acc + conv_buf[s, 2, :, cols].astype(F32) * conv_w[l, 2:3, cols]
            acc = acc + xi.astype(F32) * conv_w[l, 3:4, cols]
            acc = acc + conv_b[l, :, cols]
            x_buf[:, cols] = (acc * jax.nn.sigmoid(acc)).astype(BF)
        xi_store(i).start()
        x_store(i).start()

        @pl.when(i >= 2)
        def _():
            for q in range(3):
                p_copy(i - 2, q).wait_send()

        pt = lax.dot_general(w_x[l], x_buf[...], (((1,), (1,)), ((), ())), preferred_element_type=F32)
        pt = jnp.concatenate([pt[:pt.shape[0] // 2], pt[pt.shape[0] // 2:]], axis=1)
        p_own[...] = pt
        p_send[s] = pt.astype(BF)
        for q in range(3):
            p_copy(i, q).start()

    def phase_d(i):
        l = layer_of(i)
        s = lax.rem(i, 2)

        for t in range(n_tile):
            for k, (lo, hi) in enumerate(U_PARTS):
                if lo == n_tile + t:
                    u_copy(i, k).wait_recv()
            cols = slice(t * 256, (t + 1) * 256)
            z = (u_own[s, 1, :, cols] + u_recv[i, n_tile + t].astype(F32)).astype(BF).astype(F32)
            z_buf[:, cols] = z * jax.nn.sigmoid(z)
        for q in range(3):
            p_copy(i, q).wait_recv()
        pt = p_own[...]
        for q in range(3):
            pt = pt + p_recv[i, q].astype(F32)
        pt = jnp.concatenate([pt, pltpu.roll(pt, blk, 1)], axis=0)

        def unit(v):
            return v * lax.rsqrt(jnp.mean(v * v, axis=0, keepdims=True) + INNER_EPS)

        low_buf[...] = jnp.transpose(unit(pt[:n_rank]))[:blk].astype(BF)
        bt = unit(pt[n_rank:n_rank + n_state])
        ct = unit(pt[n_rank + n_state:])
        bt_out[i] = bt
        for b in range(blk):
            b_bc[b] = jnp.broadcast_to(bt[:, b:b + 1], (n_state, 128))
            c_bc[b] = jnp.broadcast_to(ct[:, b:b + 1], (n_state, 128))

        @pl.when(i >= 1)
        def _():
            dt_store(i - 1).wait()

        def dt_tile(t, carry):
            cols = pl.ds(pl.multiple_of(t * 256, 256), 256)
            v = jnp.dot(low_buf[...], w_dt[l, :, cols], preferred_element_type=F32)
            v = v + dt_bias[l, :, cols]
            dt = jnp.maximum(v, 0.0) + jnp.log1p(jnp.exp(-jnp.abs(v)))
            dt_buf[:, :, cols] = dt.reshape(blk // 8, 8, 256)
            dtx_buf[:, :, cols] = (dt * x_buf[:, cols].astype(F32)).reshape(blk // 8, 8, 256)
            return carry

        lax.fori_loop(0, e_loc // 256, dt_tile, 0, unroll=True)
        dt_store(i).start()
        ssm_load(i).wait()

        def group(g, carry):
            for j in range(e_loc // 128):
                cols = slice(j * 128, (j + 1) * 128)
                a = a_neg[l, :, cols]
                out = []
                for p in range(2):
                    parts = []
                    for b in range(8):
                        row = g * 16 + p * 8 + b
                        decay = jnp.exp(jnp.broadcast_to(dt_buf[g * 2 + p, b:b + 1, cols], (n_state, 128)) * a)
                        new = decay * ssm_buf[s, row, :, cols] + jnp.broadcast_to(dtx_buf[g * 2 + p, b:b + 1, cols], (n_state, 128)) * b_bc[row]
                        term = new * c_bc[row]
                        parts.append(term[:8] + term[8:])
                    out.append(fold_rows(parts))
                rws = pl.ds(pl.multiple_of(g * 16, 16), 16)
                y = jnp.concatenate(out, axis=0) + d_skip[l, :, cols] * x_buf[rws, cols].astype(F32)
                g_all[i, rws, cols] = (y * z_buf[rws, cols]).astype(BF)
            return carry

        lax.fori_loop(0, blk // 16, group, 0)

        @pl.when(i < total - n_chunk)
        def _():
            g_copy(i).start()

        @pl.when(i >= total - n_chunk)
        def _():
            g_store(i).start()

    def phase_e(i):
        l = layer_of(i)
        g_copy(i).wait_recv()

        def tile(t, carry):
            cols = pl.ds(pl.multiple_of(t * 256, 256), 256)
            cr_send[i, :, cols] = jnp.dot(g_all[i], w_out[l, :, cols], preferred_element_type=F32).astype(BF)
            return carry

        lax.fori_loop(0, d_loc // 256, tile, 0, unroll=True)
        cr_copy(i).start()

    def phase_f(i):
        cr_copy(i).wait_recv()
        xs_send[i] = (cr_send[i].astype(F32) + cr_recv[i].astype(F32)).astype(BF)
        xs_copy(i).start()

    def phase_g(i):
        def add(h):
            rws = pl.ds(part_rows(i, h), blk)
            r_ref[rws, :] = r_ref[rws, :] + (xs_send[i, half_rows(h), :].astype(F32) + xs_recv[i, half_rows(h), :].astype(F32))

        xs_copy(i).wait_recv()
        fw_copy(i).start()
        add(core)
        fw_copy(i).wait_recv()
        add(1 - core)
        phase_a(i + n_chunk)

    for l in range(n_layer):
        for vec, src in ((norm_w, norm_w_in), (conv_b, conv_b_in), (dt_bias, dt_bias_in), (d_skip, d_skip_in)):
            vec[l] = src[l:l + 1, :]
        a_neg[l] = -jnp.exp(a_log[l])
    res_load.wait()

    def first_a(i, carry):
        phase_a(i)
        return carry

    lax.fori_loop(0, n_chunk, first_a, 0)
    w_in_load[0].wait()

    def run(phase, i, stop=total):
        ok = (i >= 0) & (i < stop)

        @pl.when(ok)
        def _():
            phase(i)

    def step(s, carry):
        last = total - n_chunk

        @pl.when((s >= 2) & (s < total))
        def _():
            ssm_load(s).start()

        @pl.when(s == 1)
        def _():
            w_x_load.wait()
            w_dt_load.wait()

        run(phase_c, s - 1)
        run(phase_f, s - 3, last)

        @pl.when(s == n_chunk)
        def _():
            w_in_load[1].wait()

        run(phase_b, s)

        @pl.when(s == 0)
        def _():
            conv_load(0).start()
            w_x_load.start()
            w_dt_load.start()
            conv_load(1).start()
            ssm_load(0).start()
            ssm_load(1).start()
            w_out_load.start()
            w_in_load[1].start()

        run(phase_d, s - 1)
        run(phase_g, s - 3, last)

        @pl.when(s == n_chunk + 2)
        def _():
            r_store.start()

        @pl.when(s == 2)
        def _():
            w_out_load.wait()

        run(phase_e, s - 2, last)
        return carry

    lax.fori_loop(0, total + 1, step, 0)

    r_store.wait()
    xi_store(total - 1).wait()
    x_store(total - 1).wait()
    dt_store(total - 1).wait()
    for i in range(total - 2, total):
        for k in range(len(U_PARTS)):
            u_copy(i, k).wait_send()
        for q in range(3):
            p_copy(i, q).wait_send()

    def drain(i, carry):
        st_copy(i).wait_send()
        st_copy(i + n_chunk).wait_send()
        g_copy(i).wait_send()
        cr_copy(i).wait_send()
        xs_copy(i).wait_send()
        fw_copy(i).wait_send()
        g_store(i + total - n_chunk).wait()
        return carry

    lax.fori_loop(0, n_chunk, drain, 0)


def state_kernel(n_carry, blk, ssm_in, dt, x, bt, a_log, conv_in, xi, *refs):
    ssm_out, conv_out, a_neg, b_bc = refs[n_carry:]
    n_state, e_loc = a_log.shape[1:]

    @pl.when(pl.program_id(0) == 0)
    def _():
        a_neg[...] = -jnp.exp(a_log[0])

    for b in range(blk):
        b_bc[b] = jnp.broadcast_to(bt[0, :, b:b + 1], (n_state, 128))
    conv_out[0, 0] = conv_in[0, 1]
    conv_out[0, 1] = conv_in[0, 2]
    conv_out[0, 2] = xi[0]

    def group(g, carry):
        rws16 = pl.ds(pl.multiple_of(g * 16, 16), 16)
        for j in range(e_loc // 128):
            cols = slice(j * 128, (j + 1) * 128)
            a = a_neg[:, cols]
            x16 = x[0, rws16, cols].astype(F32)
            for p in range(2):
                dt8 = dt[0, g * 2 + p, :, cols]
                dtx = dt8 * x16[p * 8:p * 8 + 8]
                rws = pl.ds(pl.multiple_of(g * 16 + p * 8, 8), 8)
                decay = jnp.exp(dt8[:, None, :] * a[None])
                ssm_out[0, rws, :, cols] = decay * ssm_in[0, rws, :, cols] + dtx[:, None, :] * b_bc[rws]
        return carry

    lax.fori_loop(0, blk // 16, group, 0)


def state_pass(l, ssm_t, dt, x, bt, a_log_t, conv_t, xi, carried):
    _, half, n_state, e_loc = ssm_t.shape
    blk = half // N_CHUNK

    def rows_spec(*tail):
        return pl.BlockSpec((1, blk) + tail, lambda g: (l, g) + (0,) * len(tail))

    conv_spec = pl.BlockSpec((1, 3, blk, e_loc), lambda g: (l, 0, g, 0))
    in_specs = [rows_spec(n_state, e_loc), pl.BlockSpec((1, blk // 8, 8, e_loc), lambda g: (l, g, 0, 0)), rows_spec(e_loc),
                pl.BlockSpec((1, n_state, 128), lambda g: (l * N_CHUNK + g, 0, 0)),
                pl.BlockSpec((1, n_state, e_loc), lambda g: (l, 0, 0)), conv_spec, rows_spec(e_loc)]
    in_specs += [pl.BlockSpec(memory_space=pl.ANY)] * len(carried)
    n_elem = half * n_state * e_loc
    return pl.pallas_call(
        functools.partial(state_kernel, len(carried), blk),
        grid=(half // blk,),
        out_shape=(jax.ShapeDtypeStruct(ssm_t.shape, F32), jax.ShapeDtypeStruct(conv_t.shape, BF)),
        in_specs=in_specs,
        out_specs=(rows_spec(n_state, e_loc), conv_spec),
        scratch_shapes=[pltpu.VMEM((n_state, e_loc), F32), pltpu.VMEM((blk, n_state, 128), F32)],
        input_output_aliases={7 + k: k for k in range(len(carried))},
        compiler_params=pltpu.CompilerParams(vmem_limit_bytes=67043328),
        cost_estimate=pl.CostEstimate(flops=n_elem * 1000, bytes_accessed=n_elem * 8, transcendentals=n_elem),
    )(ssm_t, dt, x, bt, a_log_t, conv_t, xi, *carried)


def out_kernel(l, g_ref, w_hbm, own_hbm, kept_ref, sent_ref, w_buf, own_buf, sem, own_sem):
    first = lax.rem(lax.axis_index("ty"), 2) == 0
    n_tile = kept_ref.shape[1] // 256
    loads = [pltpu.make_async_copy(w_hbm.at[l, :, pl.ds(t * 256, 256)], w_buf.at[t], sem.at[t]) for t in range(n_tile)]
    own_load = pltpu.make_async_copy(own_hbm, own_buf, own_sem)
    loads[0].start()
    own_load.start()
    for load in loads[1:]:
        load.start()
    for t in range(n_tile):
        loads[t].wait()
        if t == 0:
            own_load.wait()
        cols = slice(t * 256, (t + 1) * 256)
        peer = jnp.dot(g_ref[...], w_buf[t], preferred_element_type=F32)
        own = jnp.dot(own_buf[...], w_buf[t], preferred_element_type=F32)
        kept_ref[:, cols] = jnp.where(first, own, peer)
        sent_ref[:, cols] = jnp.where(first, peer, own).astype(BF)


def out_proj(g, w_out, g_own, l):
    vmem = pl.BlockSpec(memory_space=pltpu.VMEM)
    hbm = pl.BlockSpec(memory_space=pltpu.HBM)
    n_rows, d_loc = g.shape[0], w_out.shape[2]
    n_tile = d_loc // 256
    return pl.pallas_call(
        functools.partial(out_kernel, l),
        out_shape=(jax.ShapeDtypeStruct((n_rows, d_loc), F32), jax.ShapeDtypeStruct((n_rows, d_loc), BF)),
        in_specs=[vmem, hbm, hbm],
        out_specs=(vmem, vmem),
        scratch_shapes=[pltpu.VMEM((n_tile, w_out.shape[1], 256), BF), pltpu.VMEM(g_own.shape, BF), pltpu.SemaphoreType.DMA((n_tile,)), pltpu.SemaphoreType.DMA],
        compiler_params=pltpu.CompilerParams(vmem_limit_bytes=24 * 2 ** 20),
        name="out_proj",
    )(g, w_out, g_own)


def solution(mesh):
    def local_step(residual, norm_w, w_in, conv_w, conv_b, w_x, w_dt, dt_bias, a_log, d_skip, w_out, conv_state, ssm_state):
        n_layer = norm_w.shape[0]
        rows, d_loc = residual.shape
        e_loc = w_x.shape[1]
        n_state = a_log.shape[-1]
        n_rank = w_dt.shape[1]
        n_proj = w_x.shape[2]
        d_model = d_loc * mesh.shape["tx"]
        total = n_layer * N_CHUNK
        blk = rows // 2 // N_CHUNK
        dims = (n_layer, rows, d_loc, e_loc, n_state, n_rank, d_model)
        conv_t = jnp.transpose(conv_state, (0, 3, 1, 2))
        ssm_t = jnp.transpose(ssm_state, (0, 1, 3, 2))
        a_log_t = jnp.transpose(a_log, (0, 2, 1))
        args = (residual, norm_w, w_in, jnp.transpose(conv_w, (0, 2, 1)), conv_b, jnp.transpose(w_x, (0, 2, 1)), w_dt, dt_bias, a_log_t, d_skip, w_out, conv_t, ssm_t)
        hbm = pl.BlockSpec(memory_space=pl.ANY)
        vmem = pl.BlockSpec(memory_space=pltpu.VMEM)
        in_specs = [hbm, vmem, hbm, vmem, vmem, hbm, hbm, vmem, vmem, vmem, hbm, hbm, hbm]
        dma = pltpu.SemaphoreType.DMA
        scratch = [pltpu.VMEM((rows, d_loc), F32), pltpu.VMEM((n_layer, n_proj, e_loc), BF), pltpu.VMEM((n_layer, n_rank, e_loc), BF), pltpu.VMEM((n_layer, 1, d_loc), F32)] + [pltpu.VMEM((n_layer, 1, e_loc), F32)] * 3 + [
            pltpu.VMEM((n_layer, d_loc, 2, e_loc), BF),
            pltpu.VMEM((n_layer, e_loc, d_loc), BF),
            pltpu.VMEM((n_layer, n_state, e_loc), F32),
            pltpu.VMEM((2, blk, n_state, e_loc), F32),
            pltpu.VMEM((2, 4, blk, e_loc), BF),
            pltpu.VMEM((2 * blk, d_loc), BF),
            pltpu.VMEM((2, 2, blk, e_loc), F32),
            pltpu.VMEM((blk, e_loc), F32),
            pltpu.VMEM((blk, e_loc), BF),
            pltpu.VMEM((blk, n_rank), BF),
            pltpu.VMEM((blk // 8, 8, e_loc), F32),
            pltpu.VMEM((blk // 8, 8, e_loc), F32),
            pltpu.VMEM((blk, n_state, 128), F32),
            pltpu.VMEM((blk, n_state, 128), F32),
            pltpu.VMEM((4 * blk, 2 * d_loc), BF),
            pltpu.VMEM((total, 8, 2 * blk), F32),
            pltpu.VMEM((total, 8, 2 * blk), F32),
            pltpu.VMEM((2, 2 * (e_loc // 256), blk, 256), BF),
            pltpu.VMEM((total, 2 * (e_loc // 256), blk, 256), BF),
            pltpu.VMEM((n_proj // 2, 2 * blk), F32),
            pltpu.VMEM((2, n_proj // 2, 2 * blk), BF),
            pltpu.VMEM((total, 3, n_proj // 2, 2 * blk), BF),
            pltpu.VMEM((total, 2 * blk, e_loc), BF),
        ] + [pltpu.VMEM((N_CHUNK, 2 * blk, d_loc), BF)] * 4 + [
            dma((5 + n_layer,)), dma((2,)), dma((2,)), dma(()), dma(()), dma((2,)), dma((N_CHUNK,)),
            dma((total,)), dma((total,)), dma((2, len(U_PARTS))), dma((total, len(U_PARTS))), dma((2, 3)), dma((total, 3)),
            dma((total,)), dma((total,)), dma((N_CHUNK,)), dma((N_CHUNK,)), dma((N_CHUNK,)), dma((N_CHUNK,)), dma((N_CHUNK,)), dma((N_CHUNK,)),
        ]
        half = rows // 2
        r_mid, bt, g_own, dt, x_act, xi = pl.pallas_call(
            functools.partial(step_kernel, dims),
            out_shape=(jax.ShapeDtypeStruct((rows, d_loc), F32), jax.ShapeDtypeStruct((total, n_state, 128), F32), jax.ShapeDtypeStruct((half, e_loc), BF),
                       jax.ShapeDtypeStruct((n_layer, half // 8, 8, e_loc), F32), jax.ShapeDtypeStruct((n_layer, half, e_loc), BF), jax.ShapeDtypeStruct((n_layer, half, e_loc), BF)),
            in_specs=in_specs,
            out_specs=(hbm, vmem, hbm, hbm, hbm, hbm),
            scratch_shapes=scratch,
            compiler_params=pltpu.CompilerParams(collective_id=0, has_side_effects=True, vmem_limit_bytes=67043328),
            name="mamba_step",
        )(*args)

        core = lax.rem(lax.axis_index("ty"), 2)
        tx = lax.axis_index("tx")
        core_swap = [(0, 1), (1, 0), (2, 3), (3, 2)]
        g_peer = lax.ppermute(g_own, "tx", [(0, 1), (1, 0)])
        caches = state_pass(0, ssm_t, dt, x_act, bt, a_log_t, conv_t, xi, ())
        kept, sent = out_proj(g_peer, pltpu.with_memory_space_constraint(w_out, pltpu.HBM), pltpu.with_memory_space_constraint(g_own, pltpu.HBM), n_layer - 1)
        part = (kept + lax.ppermute(sent, "ty", core_swap).astype(F32)).astype(BF)
        other = lax.ppermute(part, "ty", [(0, 2), (2, 0), (1, 3), (3, 1)])
        part_peer = lax.ppermute(part, "ty", core_swap)
        caches = state_pass(1, ssm_t, dt, x_act, bt, a_log_t, conv_t, xi, caches)
        other_peer = lax.ppermute(other, "ty", core_swap)
        mine = part.astype(F32) + other.astype(F32)
        theirs = part_peer.astype(F32) + other_peer.astype(F32)
        same = core == tx
        r_out = r_mid + jnp.concatenate([jnp.where(same, mine, theirs), jnp.where(same, theirs, mine)], axis=0)
        return r_out, jnp.transpose(caches[1], (0, 2, 3, 1)), jnp.transpose(caches[0], (0, 1, 3, 2))

    cache_spec = P(None, ("dp", "tx"), "ty", None)
    in_specs = (P("dp", "tx"), P(None, "tx"), P(None, "tx", None, "ty"), P(None, "ty", None), P(None, "ty"), P(None, "ty", None), P(None, None, "ty"), P(None, "ty"), P(None, "ty", None), P(None, "ty"), P(None, "ty", "tx"), cache_spec, cache_spec)
    out_specs = (P("dp", "tx"), cache_spec, cache_spec)
    return jax.shard_map(local_step, mesh=mesh, in_specs=in_specs, out_specs=out_specs, check_vma=False)
```
